512 devices in a mesh: groups: 2 (over y), gx: 32 (over z), gy: 4 (over x), gz: 2 (over core).
Axes of the slice: x: 4, y: 2, z: 32, core: 2. Of those that a mesh axis runs over, the one named last changes fastest.
The devices are a block of a 4x8x32 slice.
Arguments:
- pair: float32 [256, 384, 384], P(('groups', 'gz'), 'gx', 'gy'), parts along dimension 0, may hold values from -6 to 6
- residue_mask: int32 [768], P('groups'), parts along dimension 0, may hold values 0 or 1
- norm_in_gain: float32 [2, 128], P(None, 'gz'), may hold values from 0.25 to 1.75
- proj_weight: bfloat16 [2, 4, 128, 128], P(None, None, None, 'gz'), may hold values from -0.5 to 0.5
- gate_weight: bfloat16 [2, 128, 128], P(None, None, 'gz'), may hold values from -0.5 to 0.5
- norm_out_gain: float32 [2, 128], P(None, 'gz'), may hold values from 0.25 to 1.75
- out_weight: bfloat16 [2, 128, 128], P(None, None, 'gz'), may hold values from -0.5 to 0.5
Outputs:
- pair_out: float32 [256, 384, 384], P(('groups', 'gz'), 'gx', 'gy'), parts along dimension 0
The draws below stay inside these ranges and needn't reach their ends.
There are 2 independent parts, one for each index of `groups`. The reference program is written for one: setup_inputs(seed, part) draws one part's arguments, and reference() takes and returns one part's arrays. A program takes and returns all parts, laid end to end along the dimension named above; an argument that names none is the same for every part. Nothing has to cross between parts.
All inputs are finite; a program needn't handle non-finite values.
Results may differ from the reference program's by a relative error of at most 0.006.
Values may be sent and summed in bfloat16 or wider, within the bound.
A program may use at most 64 MiB of HBM per device.

```python
import jax
import jax.numpy as jnp
from jax import lax

CHANNELS = 128
HIDDEN_SIZE = 128
RES = 384


def with_ends(entries, stream_key, smallest, top_value):
    extent = entries.shape
    index_at = [jax.random.randint(jax.random.fold_in(stream_key, axis), (), 0, extent[axis]) for axis in range(len(extent))]
    entries = entries.at[tuple(index_at)].set(smallest)
    longest = extent.index(max(extent))
    index_at[longest] = (index_at[longest] + 1) % extent[longest]
    return entries.at[tuple(index_at)].set(top_value)


def block_levels(rng, dims, split, least, largest):
    loudness = 1.0
    for dim, shards_of in split:
        heights = jax.random.uniform(jax.random.fold_in(jax.random.fold_in(rng, 6), dim), (shards_of,), jnp.float32, least / len(split), largest / len(split))
        loudness = loudness * jnp.repeat(jnp.exp(heights), dims[dim] // shards_of).reshape((-1,) + (1,) * (len(dims) - 1 - dim))
    return loudness


def gaussian(stream_key, shape, deviation, bound, cuts=(), dtype=jnp.bfloat16):
    result = jax.random.normal(stream_key, shape, jnp.float32) * deviation
    if len(cuts) > 0:
        result = block_levels(stream_key, shape, cuts, -0.22, 0.18) * result
    return jnp.clip(result, min=-bound, max=bound).astype(dtype)


def setup_inputs(seed: int = 0, part: int = 0) -> dict:
    key_of = jax.random.split(jax.random.key(seed), 8)
    own_keys = jax.random.split(jax.random.fold_in(key_of[7], part), 8)
    return {
        "pair": gaussian(own_keys[0], (CHANNELS, RES, RES), 1.0, 6.0, ((0, 2), (1, 32), (2, 4)), jnp.float32),
        "residue_mask": with_ends((jax.random.randint(own_keys[1], (RES,), 0, 4) < 3).astype(jnp.int32), jax.random.fold_in(own_keys[1], 1), 0, 1),
        "norm_in_gain": jnp.clip(1.0 + 0.15 * jax.random.normal(key_of[2], (2, CHANNELS), jnp.float32), 0.25, 1.75),
        "proj_weight": gaussian(key_of[3], (2, 4, CHANNELS, HIDDEN_SIZE), CHANNELS ** -0.5, 0.5, ((3, 2),)),
        "gate_weight": gaussian(key_of[4], (2, CHANNELS, CHANNELS), CHANNELS ** -0.5, 0.5, ((2, 2),)),
        "norm_out_gain": jnp.clip(1.0 + 0.15 * jax.random.normal(key_of[5], (2, HIDDEN_SIZE), jnp.float32), 0.25, 1.75),
        "out_weight": gaussian(key_of[6], (2, HIDDEN_SIZE, CHANNELS), HIDDEN_SIZE ** -0.5, 0.5, ((2, 2),)),
    }


EPSILON = 1e-05

def layer_norm(values, gain_row):
    mean_val = lax.optimization_barrier(jnp.mean(values, axis=0))
    centred = values - mean_val
    spread = lax.optimization_barrier(jnp.mean(centred * centred, axis=0))
    normed = (centred * lax.rsqrt(spread + EPSILON) * gain_row[:, None, None]).astype(jnp.bfloat16)
    return lax.optimization_barrier(normed).astype(jnp.float32)

def reference(pair, residue_mask, norm_in_gain, proj_weight, gate_weight, norm_out_gain, out_weight):
    residue_flags = residue_mask.astype(jnp.float32)
    pair_mask = residue_flags[:, None] * residue_flags[None, :]
    current = pair
    for update in range(2):
        normed = layer_norm(current, norm_in_gain[update])

        def project(which_one):
            return jnp.einsum('cij,ch->hij', normed, proj_weight[update, which_one].astype(jnp.float32))
        left = (jax.nn.sigmoid(project(0)) * project(1) * pair_mask).astype(jnp.bfloat16)
        left = lax.optimization_barrier(left).astype(jnp.float32)
        right = (jax.nn.sigmoid(project(2)) * project(3) * pair_mask).astype(jnp.bfloat16)
        right = lax.optimization_barrier(right).astype(jnp.float32)
        gate_values = jax.nn.sigmoid(jnp.einsum('cij,cd->dij', normed, gate_weight[update].astype(jnp.float32)))
        if update == 0:
            triangle = jnp.einsum('hik,hjk->hij', left, right)
        else:
            triangle = jnp.einsum('hki,hkj->hij', left, right)
        tri_normed = layer_norm(triangle, norm_out_gain[update])
        current = current + gate_values * jnp.einsum('hij,hd->dij', tri_normed, out_weight[update].astype(jnp.float32))
    return current
```

```python
import functools

import jax
import jax.numpy as jnp
from jax import lax
from jax.experimental import pallas as pl
from jax.experimental.pallas import tpu as pltpu
from jax.sharding import PartitionSpec as P

EPSILON = 1e-05
LANES = 128
MESH = pl.DeviceIdType.MESH
F32 = jnp.float32
BF16 = jnp.bfloat16


class Geometry:
    def __init__(self, rows, cols, nz, nx):
        self.rows, self.cols, self.nz, self.nx = rows, cols, nz, nx
        self.spare = LANES - cols
        self.blocks = rows * cols // LANES
        self.extra = rows - self.blocks
        self.pieces = cols // self.spare
        self.width = self.blocks * LANES
        self.res = nz * rows
        self.near = cols // rows
        assert self.blocks * LANES == rows * cols
        assert self.extra * self.pieces == self.blocks
        assert nz * rows == nx * cols and self.near * rows == cols


def packed(geo, x):
    lead = x.shape[:-2]
    main = x[..., : geo.blocks, :]
    rest = x[..., geo.blocks :, :].reshape(*lead, geo.blocks, geo.spare)
    return jnp.concatenate([main, rest], axis=-1).reshape(*lead, geo.width)


def unpacked(geo, x):
    lead = x.shape[:-1]
    x = x.reshape(*lead, geo.blocks, LANES)
    rest = x[..., geo.cols :].reshape(*lead, geo.extra, geo.cols)
    return jnp.concatenate([x[..., : geo.cols], rest], axis=-2)


def lane_block(v, k):
    return v[:, k * LANES : (k + 1) * LANES]


def rows_of(geo, v):
    lane = lax.broadcasted_iota(jnp.int32, (v.shape[0], LANES), 1)
    rows = [jnp.where(lane < geo.cols, lane_block(v, r), 0.0) for r in range(geo.blocks)]
    for e in range(geo.extra):
        row = jnp.zeros((v.shape[0], LANES), F32)
        for q in range(geo.pieces):
            low = geo.spare * q
            piece = pltpu.roll(lane_block(v, e * geo.pieces + q), (low - geo.cols) % LANES, 1)
            row = jnp.where((lane >= low) & (lane < low + geo.spare), piece, row)
        rows.append(row)
    return rows


def block_of(geo, get_row, k):
    row = get_row(k)
    lane = lax.broadcasted_iota(jnp.int32, row.shape, 1)
    extra, q = divmod(k, geo.pieces)
    piece = pltpu.roll(get_row(geo.blocks + extra), geo.cols - geo.spare * q, 1)
    return jnp.where(lane < geo.cols, row, piece)


def normed(values, gain):
    mean = jnp.mean(values, axis=0, keepdims=True)
    centred = values - mean
    spread = jnp.mean(centred * centred, axis=0, keepdims=True)
    return (centred * lax.rsqrt(spread + EPSILON) * gain).astype(BF16)


def kernel(
    geo,
    half,
    z_ref,
    mask_ref,
    weight_ref,
    out_ref,
    z_next,
    zn,
    tmp,
    gate,
    left_out,
    right_out,
    left_all,
    right_in,
    right_all,
    left_mat,
    right_mat,
    product,
    back_out,
    back_in,
    back_other,
    triangle,
    left_sem,
    right_sem,
    right_x_sem,
    back_sem,
    other_sem,
    z_sem,
    sent_sem,
):
    nz, nx = geo.nz, geo.nx
    me_z = lax.axis_index("gx")
    me_x = lax.axis_index("gy")
    me_c = lax.axis_index("gz")
    other_c = 1 - me_c
    chunk = 3 * LANES
    chunks = [slice(k, k + chunk) for k in range(0, geo.width, chunk)]

    barrier = pltpu.get_barrier_semaphore()

    def signal_z(k, _):
        pl.semaphore_signal(
            barrier, inc=1, device_id={"gx": lax.rem(me_z + 1 + k, nz)}, device_id_type=MESH
        )
        return _

    lax.fori_loop(0, nz - 1, signal_z, 0)
    for k in range(1, nx):
        pl.semaphore_signal(
            barrier, inc=1, device_id={"gy": lax.rem(me_x + k, nx)}, device_id_type=MESH
        )
    pl.semaphore_signal(barrier, inc=1, device_id={"gz": other_c}, device_id_type=MESH)

    def far_first(k):
        m = (k + 1) // 2
        return lax.rem(me_z + nz // 2 + m * (1 - 2 * (k % 2)), nz)

    def copy_z(src, dst, send, recv, to):
        return pltpu.make_async_remote_copy(
            src_ref=src, dst_ref=dst, send_sem=send, recv_sem=recv, device_id={"gx": to}, device_id_type=MESH
        )

    def copy_x(src, dst, send, recv, to):
        return pltpu.make_async_remote_copy(
            src_ref=src, dst_ref=dst, send_sem=send, recv_sem=recv, device_id={"gy": to}, device_id_type=MESH
        )

    def copy_c(src, dst, send, recv):
        return pltpu.make_async_remote_copy(
            src_ref=src, dst_ref=dst, send_sem=send, recv_sem=recv, device_id={"gz": other_c}, device_id_type=MESH
        )

    def store_rows(mat, lead, base, value):
        for r, row in enumerate(rows_of(geo, value)):
            for h in range(2):
                mat[lead, h, pl.ds(base + r, 1), :] = row[h : h + 1, :]

    for u in range(2):
        weights = weight_ref.at[u]
        left_u, right_u = left_out.at[u], right_out.at[u]

        if u == 1:
            copy_c(z_next.at[me_c], z_next.at[me_c], sent_sem.at[5, 0], z_sem).wait_recv()
        gain_in = z_ref[:, geo.width + u : geo.width + u + 1]
        for s in chunks:
            if u == 0:
                z = z_ref[:, s]
            else:
                z = jnp.concatenate([z_next[0, :, s], z_next[1, :, s]], axis=0)
            zn[:, s] = normed(z, gain_in)

        def project(first):
            for s in chunks:
                both = jnp.dot(
                    weights[first : first + 2 * half, :], zn[:, s], preferred_element_type=F32
                )
                tmp[:, s] = jax.nn.sigmoid(both[:half]) * both[half:] * mask_ref[:, s]

        def to_messages(out):
            for k in range(nz):
                out[k] = tmp[2 * k : 2 * k + 2, :].astype(BF16)

        project(0)
        to_messages(left_u)
        if u == 0:
            pl.semaphore_wait(barrier, nz - 1 + nx - 1 + 1)

        def send_left(k, _):
            to = far_first(k)
            copy_z(
                left_u.at[to],
                left_all.at[u, me_x, me_z],
                sent_sem.at[0, u],
                left_sem.at[u, me_x, me_z],
                to,
            ).start()
            return _

        lax.fori_loop(0, nz - 1, send_left, 0)

        def forward_left(src, s):
            for k in range(1, nx):
                copy_x(
                    src,
                    left_all.at[u, me_x, s],
                    sent_sem.at[2, u],
                    left_sem.at[u, me_x, s],
                    lax.rem(me_x + k, nx),
                ).start()

        forward_left(left_u.at[me_z], me_z)

        project(2 * half)
        to_messages(right_u)

        def send_right(k, _):
            to = far_first(k)
            copy_z(
                right_u.at[to],
                right_in.at[u, me_z],
                sent_sem.at[1, u],
                right_sem.at[u, me_z],
                to,
            ).start()
            return _

        lax.fori_loop(0, nz - 1, send_right, 0)

        def forward_right(src, s):
            target = s // geo.near

            @pl.when(target != me_x)
            def run():
                copy_x(
                    src,
                    right_all.at[me_x, s % geo.near],
                    sent_sem.at[3, 0],
                    right_x_sem.at[me_x, s % geo.near],
                    target,
                ).start()

        if u == 0:
            forward_right(right_u.at[me_z], me_z)

        for s in chunks:
            gate[:, s] = jax.nn.sigmoid(
                jnp.dot(weights[4 * half : 5 * half, :], zn[:, s], preferred_element_type=F32)
            )

        store_rows(left_mat, me_x, me_z * geo.rows, left_u[me_z].astype(F32))

        def take_left(k, _):
            s = far_first(k)
            slot = left_all.at[u, me_x, s]
            copy_z(slot, slot, sent_sem.at[0, u], left_sem.at[u, me_x, s], s).wait_recv()
            forward_left(slot, s)
            store_rows(left_mat, me_x, s * geo.rows, left_all[u, me_x, s].astype(F32))
            return _

        lax.fori_loop(0, nz - 1, take_left, 0)

        if u == 0:
            @pl.when(me_z // geo.near == me_x)
            def run():
                store_rows(
                    right_mat, me_x, (me_z % geo.near) * geo.rows, right_u[me_z].astype(F32)
                )
        else:
            store_rows(right_mat, 0, me_z * geo.rows, right_u[me_z].astype(F32))

        def take_right(k, _):
            s = far_first(k)
            slot = right_in.at[u, s]
            copy_z(slot, slot, sent_sem.at[1, u], right_sem.at[u, s], s).wait_recv()
            if u == 0:
                forward_right(slot, s)

                @pl.when(s // geo.near == me_x)
                def run():
                    store_rows(
                        right_mat, me_x, (s % geo.near) * geo.rows, right_in[u, s].astype(F32)
                    )
            else:
                store_rows(right_mat, 0, s * geo.rows, right_in[u, s].astype(F32))
            return _

        lax.fori_loop(0, nz - 1, take_right, 0)

        for d in range(1, nx):
            x = lax.rem(me_x + d, nx)

            def take_left_x(k, _):
                slot = left_all.at[u, x, k]
                copy_x(slot, slot, sent_sem.at[2, u], left_sem.at[u, x, k], x).wait_recv()
                store_rows(left_mat, x, k * geo.rows, left_all[u, x, k].astype(F32))
                return _

            lax.fori_loop(0, nz, take_left_x, 0)

            if u == 0:

                def take_right_x(k, _):
                    slot = right_all.at[x, k]
                    copy_x(slot, slot, sent_sem.at[3, 0], right_x_sem.at[x, k], x).wait_recv()
                    store_rows(right_mat, x, k * geo.rows, right_all[x, k].astype(F32))
                    return _

                lax.fori_loop(0, geo.near, take_right_x, 0)

        for h in range(2):
            if u == 0:
                total = jnp.zeros((geo.res, geo.cols), F32)
                for x in range(nx):
                    total += lax.dot_general(
                        left_mat[x, h].astype(BF16),
                        right_mat[x, h, : geo.cols, :].astype(BF16),
                        (((1,), (1,)), ((), ())),
                        preferred_element_type=F32,
                    )
                product[h, :, : geo.cols] = total
            else:
                right = right_mat[0, h].astype(BF16)
                for x in range(nx):
                    part = lax.dot_general(
                        left_mat[x, h].astype(BF16),
                        right,
                        (((0,), (0,)), ((), ())),
                        preferred_element_type=F32,
                    )
                    product[h, geo.cols * x : geo.cols * (x + 1), :] = part[: geo.cols, :]

        back_u = back_out.at[u]

        def block_row(base, r):
            return jnp.concatenate([product[h, pl.ds(base + r, 1), :] for h in range(2)], axis=0)

        def build_back(to):
            base = to * geo.rows
            for k in range(geo.blocks):
                value = block_of(geo, functools.partial(block_row, base), k)
                back_u[to, :, k * LANES : (k + 1) * LANES] = value.astype(BF16)

        def send_back(k, _):
            to = far_first(k)
            build_back(to)
            copy_z(
                back_u.at[to], back_in.at[u, me_z], sent_sem.at[4, u], back_sem.at[u, me_z], to
            ).start()
            return _

        lax.fori_loop(0, nz - 1, send_back, 0)
        build_back(me_z)

        def forward_back(src, s):
            copy_c(src, back_other.at[u, s], sent_sem.at[6, u], other_sem.at[u, s]).start()

        forward_back(back_u.at[me_z], me_z)
        triangle[me_c, me_z] = back_u[me_z].astype(F32)

        def take_back(k, _):
            s = far_first(k)
            slot = back_in.at[u, s]
            copy_z(slot, slot, sent_sem.at[4, u], back_sem.at[u, s], s).wait_recv()
            forward_back(slot, s)
            triangle[me_c, s] = back_in[u, s].astype(F32)
            return _

        lax.fori_loop(0, nz - 1, take_back, 0)

        def take_other(k, _):
            slot = back_other.at[u, k]
            copy_c(slot, slot, sent_sem.at[6, u], other_sem.at[u, k]).wait_recv()
            triangle[other_c, k] = back_other[u, k].astype(F32)
            return _

        lax.fori_loop(0, nz, take_other, 0)

        gain_out = z_ref[:, geo.width + 2 + u : geo.width + 3 + u]
        for s in chunks:
            values = jnp.concatenate(
                [triangle[c, k, :, s] for c in range(2) for k in range(nz)], axis=0
            )
            tn = normed(values, gain_out)
            change = jnp.dot(weights[5 * half :, :], tn, preferred_element_type=F32)
            if u == 0:
                mine = z_ref[pl.ds(pl.multiple_of(me_c * half, half), half), s]
                z_next[me_c, :, s] = mine + gate[:, s] * change
            else:
                out_ref[:, s] = z_next[me_c, :, s] + gate[:, s] * change
        if u == 0:
            copy_c(z_next.at[me_c], z_next.at[me_c], sent_sem.at[5, 0], z_sem).start()

    for u in range(2):
        many = left_out.at[u, pl.ds(0, nz - 1)]
        copy_z(many, many, sent_sem.at[0, u], z_sem, me_z).wait_send()
        copy_z(many, many, sent_sem.at[1, u], z_sem, me_z).wait_send()
        copy_z(many, many, sent_sem.at[4, u], z_sem, me_z).wait_send()
        for k in range(1, nx):
            all_slots = left_out.at[u]
            copy_x(all_slots, all_slots, sent_sem.at[2, u], z_sem, me_x).wait_send()
        every = left_out.at[u]
        copy_c(every, every, sent_sem.at[6, u], z_sem).wait_send()
    away = left_out.at[0, pl.ds(0, nz - geo.near)]
    copy_x(away, away, sent_sem.at[3, 0], z_sem, me_x).wait_send()
    copy_c(z_next.at[me_c], z_next.at[me_c], sent_sem.at[5, 0], z_sem).wait_send()


def per_device(
    geo, pair, residue_mask, norm_in_gain, proj_weight, gate_weight, norm_out_gain, out_weight
):
    half = pair.shape[0]
    full = 2 * half
    row_start = lax.axis_index("gx") * geo.rows
    col_start = lax.axis_index("gy") * geo.cols
    row_flags = lax.dynamic_slice_in_dim(residue_mask, row_start, geo.rows).astype(F32)
    col_flags = lax.dynamic_slice_in_dim(residue_mask, col_start, geo.cols).astype(F32)
    mask = packed(geo, row_flags[:, None] * col_flags[None, :])[None, :]
    gains = jnp.concatenate([norm_in_gain, norm_out_gain], axis=0).T
    gains = jnp.pad(gains, ((0, 0), (0, LANES - 4)))
    z = jnp.concatenate([packed(geo, pair), gains], axis=1)
    z = lax.all_gather(z, "gz", axis=0, tiled=True)
    weights = jnp.concatenate(
        [proj_weight, gate_weight[:, None], out_weight[:, None]], axis=1
    )
    weights = jnp.swapaxes(weights, 2, 3).reshape(2, 6 * half, full)

    nz, nx = geo.nz, geo.nx
    vmem = pltpu.VMEM
    message = (2, geo.width)
    dma = pltpu.SemaphoreType.DMA
    result = pl.pallas_call(
        functools.partial(kernel, geo, half),
        out_shape=jax.ShapeDtypeStruct((half, geo.width), F32),
        in_specs=[pl.BlockSpec(memory_space=vmem)] * 3,
        out_specs=pl.BlockSpec(memory_space=vmem),
        scratch_shapes=[
            vmem((2, half, geo.width), F32),
            vmem((full, geo.width), BF16),
            vmem((half, geo.width), F32),
            vmem((half, geo.width), F32),
            vmem((2, nz, *message), BF16),
            vmem((2, nz, *message), BF16),
            vmem((2, nx, nz, *message), BF16),
            vmem((2, nz, *message), BF16),
            vmem((nx, geo.near, *message), BF16),
            vmem((nx, 2, geo.res, LANES), F32),
            vmem((nx, 2, geo.res, LANES), F32),
            vmem((2, geo.res, LANES), F32),
            vmem((2, nz, *message), BF16),
            vmem((2, nz, *message), BF16),
            vmem((2, nz, *message), BF16),
            vmem((2, nz, *message), F32),
            dma((2, nx, nz)),
            dma((2, nz)),
            dma((nx, geo.near)),
            dma((2, nz)),
            dma((2, nz)),
            dma,
            dma((7, 2)),
        ],
        compiler_params=pltpu.CompilerParams(
            collective_id=0, has_side_effects=True, vmem_limit_bytes=60 * 1024 * 1024
        ),
        name="triangle_updates",
    )(z, mask, weights)
    return unpacked(geo, result)


def solution(mesh):
    def body(pair, *rest):
        geo = Geometry(pair.shape[1], pair.shape[2], mesh.shape["gx"], mesh.shape["gy"])
        return per_device(geo, pair, *rest)

    return jax.shard_map(
        body,
        mesh=mesh,
        in_specs=(
            P(("groups", "gz"), "gx", "gy"),
            P("groups"),
            P(None, "gz"),
            P(None, None, None, "gz"),
            P(None, None, "gz"),
            P(None, "gz"),
            P(None, None, "gz"),
        ),
        out_specs=P(("groups", "gz"), "gx", "gy"),
        check_vma=False,
    )
```

```python
import functools

import jax
import jax.numpy as jnp
from jax import lax
from jax.experimental import pallas as pl
from jax.experimental.pallas import tpu as pltpu
from jax.sharding import PartitionSpec as P

EPSILON = 1e-05
LANES = 128
MESH = pl.DeviceIdType.MESH
F32 = jnp.float32
BF16 = jnp.bfloat16


class Geometry:
    def __init__(self, rows, cols, nz, nx):
        self.rows, self.cols, self.nz, self.nx = rows, cols, nz, nx
        self.spare = LANES - cols
        self.blocks = rows * cols // LANES
        self.extra = rows - self.blocks
        self.pieces = cols // self.spare
        self.width = self.blocks * LANES
        self.res = nz * rows
        self.near = cols // rows
        assert self.blocks * LANES == rows * cols
        assert self.extra * self.pieces == self.blocks
        assert nz * rows == nx * cols and self.near * rows == cols


def packed(geo, x):
    lead = x.shape[:-2]
    main = x[..., : geo.blocks, :]
    rest = x[..., geo.blocks :, :].reshape(*lead, geo.blocks, geo.spare)
    return jnp.concatenate([main, rest], axis=-1).reshape(*lead, geo.width)


def lane_block(v, k):
    return v[:, k * LANES : (k + 1) * LANES]


def rows_of(geo, v):
    lane = lax.broadcasted_iota(jnp.int32, (v.shape[0], LANES), 1)
    rows = [jnp.where(lane < geo.cols, lane_block(v, r), 0.0) for r in range(geo.blocks)]
    for e in range(geo.extra):
        row = jnp.zeros((v.shape[0], LANES), F32)
        for q in range(geo.pieces):
            low = geo.spare * q
            piece = pltpu.roll(lane_block(v, e * geo.pieces + q), (low - geo.cols) % LANES, 1)
            row = jnp.where((lane >= low) & (lane < low + geo.spare), piece, row)
        rows.append(row)
    return rows


def block_of(geo, get_row, k):
    row = get_row(k)
    lane = lax.broadcasted_iota(jnp.int32, row.shape, 1)
    extra, q = divmod(k, geo.pieces)
    piece = pltpu.roll(get_row(geo.blocks + extra), geo.cols - geo.spare * q, 1)
    return jnp.where(lane < geo.cols, row, piece)


def normed(values, gain):
    mean = jnp.mean(values, axis=0, keepdims=True)
    centred = values - mean
    spread = jnp.mean(centred * centred, axis=0, keepdims=True)
    return (centred * lax.rsqrt(spread + EPSILON) * gain).astype(BF16)


def kernel(
    geo,
    half,
    z_ref,
    mask_ref,
    weight_ref,
    out_ref,
    z_next,
    zn,
    tmp,
    gate,
    left_out,
    right_out,
    left_all,
    right_in,
    right_all,
    left_mat,
    right_mat,
    product,
    back_out,
    back_in,
    back_other,
    triangle,
    left_sem,
    right_sem,
    right_x_sem,
    back_sem,
    other_sem,
    z_sem,
    sent_sem,
):
    nz, nx = geo.nz, geo.nx
    me_z = lax.axis_index("gx")
    me_x = lax.axis_index("gy")
    me_c = lax.axis_index("gz")
    other_c = 1 - me_c
    chunk = geo.pieces * LANES
    chunks = [slice(k, k + chunk) for k in range(0, geo.width, chunk)]

    barrier = pltpu.get_barrier_semaphore()

    def signal_z(k, _):
        pl.semaphore_signal(
            barrier, inc=1, device_id={"gx": lax.rem(me_z + 1 + k, nz)}, device_id_type=MESH
        )
        return _

    lax.fori_loop(0, nz - 1, signal_z, 0)
    for k in range(1, nx):
        pl.semaphore_signal(
            barrier, inc=1, device_id={"gy": lax.rem(me_x + k, nx)}, device_id_type=MESH
        )
    pl.semaphore_signal(barrier, inc=1, device_id={"gz": other_c}, device_id_type=MESH)

    def far_first(k):
        m = (k + 1) // 2
        return lax.rem(me_z + nz // 2 + m * (1 - 2 * (k % 2)), nz)

    def copy_z(src, dst, send, recv, to):
        return pltpu.make_async_remote_copy(
            src_ref=src, dst_ref=dst, send_sem=send, recv_sem=recv, device_id={"gx": to}, device_id_type=MESH
        )

    def copy_x(src, dst, send, recv, to):
        return pltpu.make_async_remote_copy(
            src_ref=src, dst_ref=dst, send_sem=send, recv_sem=recv, device_id={"gy": to}, device_id_type=MESH
        )

    def copy_c(src, dst, send, recv):
        return pltpu.make_async_remote_copy(
            src_ref=src, dst_ref=dst, send_sem=send, recv_sem=recv, device_id={"gz": other_c}, device_id_type=MESH
        )

    def store_rows(mat, lead, base, value):
        for r, row in enumerate(rows_of(geo, value)):
            for h in range(2):
                mat[lead, h, pl.ds(base + r, 1), :] = row[h : h + 1, :]

    group = 4
    lag = 8

    for u in range(2):
        weights = weight_ref.at[u]
        left_u, right_u, back_u = left_out.at[u], right_out.at[u], back_out.at[u]

        gain_in = z_ref[:, geo.width + u : geo.width + u + 1]
        for i, s in enumerate(chunks):
            if u == 0:
                z = z_ref[:, s]
            else:
                piece = z_next.at[me_c, :, s]
                copy_c(piece, piece, sent_sem.at[5, 0], z_sem.at[i]).wait_recv()
                z = jnp.concatenate([z_next[0, :, s], z_next[1, :, s]], axis=0)
            zn[:, s] = normed(z, gain_in)

        def project(first, out):
            for s in chunks:
                both = jnp.dot(
                    weights[first : first + 2 * half, :], zn[:, s], preferred_element_type=F32
                )
                tmp[:, s] = jax.nn.sigmoid(both[:half]) * both[half:] * mask_ref[:, s]
            for k in range(nz):
                out[k] = tmp[2 * k : 2 * k + 2, :].astype(BF16)

        def forward_left(src, s):
            for k in range(1, nx):
                copy_x(
                    src,
                    left_all.at[u, me_x, s],
                    sent_sem.at[2, u],
                    left_sem.at[u, me_x, s],
                    lax.rem(me_x + k, nx),
                ).start()

        def forward_right(src, s):
            target = s // geo.near

            @pl.when(target != me_x)
            def run():
                copy_x(
                    src,
                    right_all.at[me_x, s % geo.near],
                    sent_sem.at[3, 0],
                    right_x_sem.at[me_x, s % geo.near],
                    target,
                ).start()

        def send_left():
            def send(k, _):
                to = far_first(k)
                copy_z(
                    left_u.at[to],
                    left_all.at[u, me_x, me_z],
                    sent_sem.at[0, u],
                    left_sem.at[u, me_x, me_z],
                    to,
                ).start()
                return _

            lax.fori_loop(0, nz - 1, send, 0)
            forward_left(left_u.at[me_z], me_z)
            left_all[u, me_x, me_z] = left_u[me_z]

        def send_right():
            def send(k, _):
                to = far_first(k)
                copy_z(
                    right_u.at[to],
                    right_in.at[u, me_z],
                    sent_sem.at[1, u],
                    right_sem.at[u, me_z],
                    to,
                ).start()
                return _

            lax.fori_loop(0, nz - 1, send, 0)
            right_in[u, me_z] = right_u[me_z]

        def open_gate():
            for s in chunks:
                gate[:, s] = jax.nn.sigmoid(
                    jnp.dot(weights[4 * half : 5 * half, :], zn[:, s], preferred_element_type=F32)
                )

        def left_base(k, s):
            return (k if u == 0 else s) * geo.rows

        def take_left(k):
            s = far_first(k)
            slot = left_all.at[u, me_x, s]

            @pl.when(k < nz - 1)
            def run():
                copy_z(slot, slot, sent_sem.at[0, u], left_sem.at[u, me_x, s], s).wait_recv()
                forward_left(slot, s)

            store_rows(left_mat, me_x, left_base(k, s), left_all[u, me_x, s].astype(F32))

        def take_left_x(k):
            s = far_first(k)
            for d in range(1, nx):
                x = lax.rem(me_x + d, nx)
                slot = left_all.at[u, x, s]
                copy_x(slot, slot, sent_sem.at[2, u], left_sem.at[u, x, s], x).wait_recv()
                store_rows(left_mat, x, left_base(k, s), left_all[u, x, s].astype(F32))

        def wait_right(k, s):
            slot = right_in.at[u, s]

            @pl.when(k < nz - 1)
            def run():
                copy_z(slot, slot, sent_sem.at[1, u], right_sem.at[u, s], s).wait_recv()

        def block_row(base, r):
            return jnp.concatenate([product[h, pl.ds(base + r, 1), :] for h in range(2)], axis=0)

        def send_back(k):
            to = far_first(k)
            base = left_base(k, to)
            for b in range(geo.blocks):
                value = block_of(geo, functools.partial(block_row, base), b)
                back_u[to, :, b * LANES : (b + 1) * LANES] = value.astype(BF16)

            @pl.when(k < nz - 1)
            def run():
                copy_z(
                    back_u.at[to], back_in.at[u, me_z], sent_sem.at[4, u], back_sem.at[u, me_z], to
                ).start()

        if u == 0:
            project(2 * half, right_u)
            pl.semaphore_wait(barrier, nz - 1 + nx - 1 + 1)
            send_right()
            forward_right(right_u.at[me_z], me_z)
            project(0, left_u)
            send_left()
            open_gate()

            def take_right(k, _):
                s = far_first(k)
                wait_right(k, s)

                @pl.when(k < nz - 1)
                def run():
                    forward_right(right_in.at[0, s], s)

                @pl.when(s // geo.near == me_x)
                def run_own():
                    store_rows(
                        right_mat, me_x, (s % geo.near) * geo.rows, right_in[0, s].astype(F32)
                    )

                return _

            lax.fori_loop(0, nz, take_right, 0)

            def take_group(g):
                def take(i, _):
                    take_left(g * group + i)
                    return _

                lax.fori_loop(0, group, take, 0)

            take_group(0)

            for d in range(1, nx):
                x = lax.rem(me_x + d, nx)

                def take_right_x(k, _):
                    slot = right_all.at[x, k]
                    copy_x(slot, slot, sent_sem.at[3, 0], right_x_sem.at[x, k], x).wait_recv()
                    store_rows(right_mat, x, k * geo.rows, right_all[x, k].astype(F32))
                    return _

                lax.fori_loop(0, geo.near, take_right_x, 0)
            take_group(1)

            tall = group * geo.rows

            def work(g, _):
                @pl.when(g < nz // group - 2)
                def run():
                    take_group(g + 2)

                def take_x(i, _):
                    take_left_x(g * group + i)
                    return _

                lax.fori_loop(0, group, take_x, 0)
                rows = pl.ds(pl.multiple_of(g * tall, tall), tall)
                for h in range(2):
                    total = jnp.zeros((tall, geo.cols), F32)
                    for x in range(nx):
                        total += lax.dot_general(
                            left_mat[x, h, rows, :].astype(BF16),
                            right_mat[x, h, : geo.cols, :].astype(BF16),
                            (((1,), (1,)), ((), ())),
                            preferred_element_type=F32,
                        )
                    product[h, rows, : geo.cols] = total

                def send(i, _):
                    send_back(g * group + i)
                    return _

                lax.fori_loop(0, group, send, 0)
                return _

            lax.fori_loop(0, nz // group, work, 0)
        else:
            project(0, left_u)
            send_left()
            project(2 * half, right_u)
            send_right()
            open_gate()

            def take_lefts(k, _):
                take_left(k)

                @pl.when(k >= lag)
                def run():
                    take_left_x(k - lag)

                return _

            lax.fori_loop(0, nz, take_lefts, 0)

            def take_right(k, _):
                s = far_first(k)
                wait_right(k, s)
                store_rows(right_mat, 0, s * geo.rows, right_in[1, s].astype(F32))

                @pl.when(k < lag)
                def run():
                    take_left_x(nz - lag + k)

                return _

            lax.fori_loop(0, nz, take_right, 0)

            for h in range(2):
                right = right_mat[0, h].astype(BF16)
                for x in range(nx):
                    part = lax.dot_general(
                        left_mat[x, h].astype(BF16),
                        right,
                        (((0,), (0,)), ((), ())),
                        preferred_element_type=F32,
                    )
                    product[h, geo.cols * x : geo.cols * (x + 1), :] = part[: geo.cols, :]

            def send(k, _):
                send_back(k)
                return _

            lax.fori_loop(0, nz, send, 0)

        def take_back(k, _):
            s = far_first(k)
            slot = back_in.at[u, s]
            copy_z(slot, slot, sent_sem.at[4, u], back_sem.at[u, s], s).wait_recv()
            copy_c(slot, back_other.at[u, s], sent_sem.at[6, u], other_sem.at[u, s]).start()
            triangle[me_c, s] = back_in[u, s].astype(F32)
            return _

        copy_c(
            back_u.at[me_z], back_other.at[u, me_z], sent_sem.at[6, u], other_sem.at[u, me_z]
        ).start()
        triangle[me_c, me_z] = back_u[me_z].astype(F32)
        lax.fori_loop(0, nz - 1, take_back, 0)

        def take_other(k, _):
            slot = back_other.at[u, k]
            copy_c(slot, slot, sent_sem.at[6, u], other_sem.at[u, k]).wait_recv()
            triangle[other_c, k] = back_other[u, k].astype(F32)
            return _

        lax.fori_loop(0, nz, take_other, 0)

        gain_out = z_ref[:, geo.width + 2 + u : geo.width + 3 + u]
        for i, s in enumerate(chunks):
            values = jnp.concatenate(
                [triangle[c, k, :, s] for c in range(2) for k in range(nz)], axis=0
            )
            tn = normed(values, gain_out)
            change = jnp.dot(weights[5 * half :, :], tn, preferred_element_type=F32)
            if u == 0:
                mine = z_ref[pl.ds(pl.multiple_of(me_c * half, half), half), s]
                z_next[me_c, :, s] = mine + gate[:, s] * change
                piece = z_next.at[me_c, :, s]
                copy_c(piece, piece, sent_sem.at[5, 0], z_sem.at[i]).start()
            else:
                value = z_next[me_c, :, s] + gate[:, s] * change
                lane = lax.broadcasted_iota(jnp.int32, (half, LANES), 1)
                row = jnp.zeros((half, LANES), F32)
                for q in range(geo.pieces):
                    block = lane_block(value, q)
                    out_ref[:, i * geo.pieces + q, :] = block[:, : geo.cols]
                    low = geo.spare * q
                    moved = pltpu.roll(block, (low - geo.cols) % LANES, 1)
                    row = jnp.where((lane >= low) & (lane < low + geo.spare), moved, row)
                out_ref[:, geo.blocks + i, :] = row[:, : geo.cols]

    any_sem = z_sem.at[0]
    for u in range(2):
        many = left_out.at[u, pl.ds(0, nz - 1)]
        copy_z(many, many, sent_sem.at[0, u], any_sem, me_z).wait_send()
        copy_z(many, many, sent_sem.at[1, u], any_sem, me_z).wait_send()
        copy_z(many, many, sent_sem.at[4, u], any_sem, me_z).wait_send()
        for k in range(1, nx):
            all_slots = left_out.at[u]
            copy_x(all_slots, all_slots, sent_sem.at[2, u], any_sem, me_x).wait_send()
        every = left_out.at[u]
        copy_c(every, every, sent_sem.at[6, u], any_sem).wait_send()
    away = left_out.at[0, pl.ds(0, nz - geo.near)]
    copy_x(away, away, sent_sem.at[3, 0], any_sem, me_x).wait_send()
    copy_c(z_next.at[me_c], z_next.at[me_c], sent_sem.at[5, 0], any_sem).wait_send()


def per_device(
    geo, pair, residue_mask, norm_in_gain, proj_weight, gate_weight, norm_out_gain, out_weight
):
    half = pair.shape[0]
    full = 2 * half
    row_start = lax.axis_index("gx") * geo.rows
    col_start = lax.axis_index("gy") * geo.cols
    row_flags = lax.dynamic_slice_in_dim(residue_mask, row_start, geo.rows).astype(F32)
    col_flags = lax.dynamic_slice_in_dim(residue_mask, col_start, geo.cols).astype(F32)
    mask = packed(geo, row_flags[:, None] * col_flags[None, :])[None, :]
    gains = jnp.concatenate([norm_in_gain, norm_out_gain], axis=0).T
    gains = jnp.pad(gains, ((0, 0), (0, LANES - 4)))
    z = jnp.concatenate([packed(geo, pair), gains], axis=1)
    z = lax.all_gather(z, "gz", axis=0, tiled=True)
    weights = jnp.concatenate(
        [proj_weight, gate_weight[:, None], out_weight[:, None]], axis=1
    )
    weights = jnp.swapaxes(weights, 2, 3).reshape(2, 6 * half, full)

    nz, nx = geo.nz, geo.nx
    vmem = pltpu.VMEM
    message = (2, geo.width)
    dma = pltpu.SemaphoreType.DMA
    return pl.pallas_call(
        functools.partial(kernel, geo, half),
        out_shape=jax.ShapeDtypeStruct(pair.shape, F32),
        in_specs=[pl.BlockSpec(memory_space=vmem)] * 3,
        out_specs=pl.BlockSpec(memory_space=vmem),
        scratch_shapes=[
            vmem((2, half, geo.width), F32),
            vmem((full, geo.width), BF16),
            vmem((half, geo.width), F32),
            vmem((half, geo.width), F32),
            vmem((2, nz, *message), BF16),
            vmem((2, nz, *message), BF16),
            vmem((2, nx, nz, *message), BF16),
            vmem((2, nz, *message), BF16),
            vmem((nx, geo.near, *message), BF16),
            vmem((nx, 2, geo.res, LANES), F32),
            vmem((nx, 2, geo.res, LANES), F32),
            vmem((2, geo.res, LANES), F32),
            vmem((2, nz, *message), BF16),
            vmem((2, nz, *message), BF16),
            vmem((2, nz, *message), BF16),
            vmem((2, nz, *message), F32),
            dma((2, nx, nz)),
            dma((2, nz)),
            dma((nx, geo.near)),
            dma((2, nz)),
            dma((2, nz)),
            dma((geo.extra,)),
            dma((7, 2)),
        ],
        compiler_params=pltpu.CompilerParams(
            collective_id=0, has_side_effects=True, vmem_limit_bytes=60 * 1024 * 1024
        ),
        name="triangle_updates",
    )(z, mask, weights)


def solution(mesh):
    def body(pair, *rest):
        geo = Geometry(pair.shape[1], pair.shape[2], mesh.shape["gx"], mesh.shape["gy"])
        return per_device(geo, pair, *rest)

    return jax.shard_map(
        body,
        mesh=mesh,
        in_specs=(
            P(("groups", "gz"), "gx", "gy"),
            P("groups"),
            P(None, "gz"),
            P(None, None, None, "gz"),
            P(None, None, "gz"),
            P(None, "gz"),
            P(None, None, "gz"),
        ),
        out_specs=P(("groups", "gz"), "gx", "gy"),
        check_vma=False,
    )
```

```python
import functools

import jax
import jax.numpy as jnp
from jax import lax
from jax.experimental import pallas as pl
from jax.experimental.pallas import tpu as pltpu
from jax.sharding import PartitionSpec as P

EPSILON = 1e-05
LANES = 128
MESH = pl.DeviceIdType.MESH
F32 = jnp.float32
BF16 = jnp.bfloat16


class Geometry:
    def __init__(self, rows, cols, nz, nx):
        self.rows, self.cols, self.nz, self.nx = rows, cols, nz, nx
        self.spare = LANES - cols
        self.blocks = rows * cols // LANES
        self.extra = rows - self.blocks
        self.pieces = cols // self.spare
        self.width = self.blocks * LANES
        self.res = nz * rows
        self.near = cols // rows
        assert self.blocks * LANES == rows * cols
        assert self.extra * self.pieces == self.blocks
        assert nz * rows == nx * cols and self.near * rows == cols


def lane_block(v, k):
    return v[:, k * LANES : (k + 1) * LANES]


def rows_of(geo, v):
    lane = lax.broadcasted_iota(jnp.int32, (v.shape[0], LANES), 1)
    rows = [jnp.where(lane < geo.cols, lane_block(v, r), 0.0) for r in range(geo.blocks)]
    for e in range(geo.extra):
        row = jnp.zeros((v.shape[0], LANES), F32)
        for q in range(geo.pieces):
            low = geo.spare * q
            piece = pltpu.roll(lane_block(v, e * geo.pieces + q), (low - geo.cols) % LANES, 1)
            row = jnp.where((lane >= low) & (lane < low + geo.spare), piece, row)
        rows.append(row)
    return rows


def block_of(geo, get_row, k):
    row = get_row(k)
    lane = lax.broadcasted_iota(jnp.int32, row.shape, 1)
    extra, q = divmod(k, geo.pieces)
    piece = pltpu.roll(get_row(geo.blocks + extra), geo.cols - geo.spare * q, 1)
    return jnp.where(lane < geo.cols, row, piece)


def normed(values, gain):
    mean = jnp.mean(values, axis=0, keepdims=True)
    centred = values - mean
    spread = jnp.mean(centred * centred, axis=0, keepdims=True)
    return (centred * lax.rsqrt(spread + EPSILON) * gain).astype(BF16)


def kernel(
    geo,
    half,
    pair_hbm,
    flag_ref,
    flags_ref,
    gain_in_hbm,
    proj_hbm,
    gate_hbm,
    gain_out_hbm,
    out_hbm,
    out_ref,
    pair_ref,
    gains,
    proj_raw,
    gate_raw,
    out_raw,
    weight_ref,
    mask_ref,
    z_all,
    zn,
    tmp,
    gate,
    left_out,
    right_out,
    left_all,
    right_in,
    right_all,
    left_mat,
    right_mat,
    product,
    back_out,
    back_in,
    back_other,
    triangle,
    left_sem,
    right_sem,
    right_x_sem,
    back_sem,
    other_sem,
    z_sem,
    sent_sem,
    load_sem,
):
    nz, nx = geo.nz, geo.nx
    me_z = lax.axis_index("gx")
    me_x = lax.axis_index("gy")
    me_c = lax.axis_index("gz")
    other_c = 1 - me_c
    chunk = geo.pieces * LANES
    chunks = [slice(k, k + chunk) for k in range(0, geo.width, chunk)]

    barrier = pltpu.get_barrier_semaphore()

    def signal_z(k, _):
        pl.semaphore_signal(
            barrier, inc=1, device_id={"gx": lax.rem(me_z + 1 + k, nz)}, device_id_type=MESH
        )
        return _

    lax.fori_loop(0, nz - 1, signal_z, 0)
    for k in range(1, nx):
        pl.semaphore_signal(
            barrier, inc=1, device_id={"gy": lax.rem(me_x + k, nx)}, device_id_type=MESH
        )
    pl.semaphore_signal(barrier, inc=1, device_id={"gz": other_c}, device_id_type=MESH)

    def far_first(k):
        m = (k + 1) // 2
        return lax.rem(me_z + nz // 2 + m * (1 - 2 * (k % 2)), nz)

    def copy_z(src, dst, send, recv, to):
        return pltpu.make_async_remote_copy(
            src_ref=src, dst_ref=dst, send_sem=send, recv_sem=recv, device_id={"gx": to}, device_id_type=MESH
        )

    def copy_x(src, dst, send, recv, to):
        return pltpu.make_async_remote_copy(
            src_ref=src, dst_ref=dst, send_sem=send, recv_sem=recv, device_id={"gy": to}, device_id_type=MESH
        )

    def copy_c(src, dst, send, recv):
        return pltpu.make_async_remote_copy(
            src_ref=src, dst_ref=dst, send_sem=send, recv_sem=recv, device_id={"gz": other_c}, device_id_type=MESH
        )

    def store_rows(mat, lead, base, value):
        for r, row in enumerate(rows_of(geo, value)):
            for h in range(2):
                mat[lead, h, pl.ds(base + r, 1), :] = row[h : h + 1, :]

    lag = 8
    wide = geo.width

    loads = [
        pltpu.make_async_copy(src, dst, load_sem.at[i])
        for i, (src, dst) in enumerate(
            [
                (pair_hbm, pair_ref),
                (gain_in_hbm, gains.at[0]),
                (gain_out_hbm, gains.at[1]),
                (proj_hbm, proj_raw),
                (gate_hbm, gate_raw),
                (out_hbm, out_raw),
            ]
        )
    ]
    for load in loads:
        load.start()
    for load in loads[:3]:
        load.wait()
    for k in range(geo.blocks):
        e, q = divmod(k, geo.pieces)
        low = geo.spare * q
        z_all[0, me_c, :, k * LANES : (k + 1) * LANES] = jnp.concatenate(
            [pair_ref[:, k, :], pair_ref[:, geo.blocks + e, low : low + geo.spare]], axis=1
        )
    diagonal = lax.broadcasted_iota(jnp.int32, (half, half), 0) == lax.broadcasted_iota(
        jnp.int32, (half, half), 1
    )
    columns = [
        jnp.sum(jnp.where(diagonal, gains[kind, u : u + 1, :], 0.0), axis=1, keepdims=True)
        for kind in range(2)
        for u in range(2)
    ]
    lane = lax.broadcasted_iota(jnp.int32, (half, LANES), 1)
    last = jnp.zeros((half, LANES), F32)
    for i, column in enumerate(columns):
        last = jnp.where(lane == i, column, last)
    z_all[0, me_c, :, wide:] = last

    flags = flags_ref[...].astype(F32)
    near_flags = jnp.zeros((1, LANES), F32)
    for x in range(nx):
        own = jnp.where(me_x == x, 1.0, 0.0)
        part = flags[:, geo.cols * x : geo.cols * (x + 1)]
        near_flags += own * jnp.concatenate([part, jnp.zeros((1, geo.spare), F32)], axis=1)
    row_flag = [flag_ref[me_z * geo.rows + r].astype(F32) for r in range(geo.rows)]
    for k in range(geo.blocks):
        mask_ref[:, k * LANES : (k + 1) * LANES] = block_of(
            geo, lambda r: near_flags * row_flag[r], k
        )

    for load in loads[3:]:
        load.wait()
    for u in range(2):
        raw = [proj_raw.at[u, p] for p in range(4)] + [gate_raw.at[u], out_raw.at[u]]
        for p, ref in enumerate(raw):
            weight_ref[u, p * half : (p + 1) * half, :] = ref[...].astype(F32).T.astype(BF16)

    pl.semaphore_wait(barrier, nz - 1 + nx - 1 + 1)

    def z_piece(u, i):
        low = i * chunk
        high = low + chunk + (LANES if u == 0 and i == geo.extra - 1 else 0)
        part = z_all.at[u, me_c, :, low:high]
        return copy_c(part, part, sent_sem.at[5, u], z_sem.at[u, i])

    for i in reversed(range(geo.extra)):
        z_piece(0, i).start()

    for u in range(2):
        weights = weight_ref.at[u]
        left_u, right_u, back_u = left_out.at[u], right_out.at[u], back_out.at[u]

        for i in reversed(range(geo.extra)):
            z_piece(u, i).wait_recv()
            s = chunks[i]
            if i == geo.extra - 1:
                gain_in = jnp.concatenate(
                    [z_all[0, c, :, wide + u : wide + u + 1] for c in range(2)], axis=0
                )
            z = jnp.concatenate([z_all[u, 0, :, s], z_all[u, 1, :, s]], axis=0)
            zn[:, s] = normed(z, gain_in)

        def project(first, out):
            for s in chunks:
                both = jnp.dot(
                    weights[first : first + 2 * half, :], zn[:, s], preferred_element_type=F32
                )
                tmp[:, s] = jax.nn.sigmoid(both[:half]) * both[half:] * mask_ref[:, s]
            for k in range(nz):
                out[k] = tmp[2 * k : 2 * k + 2, :].astype(BF16)

        def forward_left(src, s):
            for k in range(1, nx):
                copy_x(
                    src,
                    left_all.at[u, me_x, s],
                    sent_sem.at[2, u],
                    left_sem.at[u, me_x, s],
                    lax.rem(me_x + k, nx),
                ).start()

        def forward_right(src, s):
            target = s // geo.near

            @pl.when(target != me_x)
            def run():
                copy_x(
                    src,
                    right_all.at[me_x, s % geo.near],
                    sent_sem.at[3, 0],
                    right_x_sem.at[me_x, s % geo.near],
                    target,
                ).start()

        def send_left():
            def send(k, _):
                to = far_first(k)
                copy_z(
                    left_u.at[to],
                    left_all.at[u, me_x, me_z],
                    sent_sem.at[0, u],
                    left_sem.at[u, me_x, me_z],
                    to,
                ).start()
                return _

            lax.fori_loop(0, nz - 1, send, 0)
            forward_left(left_u.at[me_z], me_z)
            left_all[u, me_x, me_z] = left_u[me_z]

        def send_right():
            def send(k, _):
                to = far_first(k)
                copy_z(
                    right_u.at[to],
                    right_in.at[u, me_z],
                    sent_sem.at[1, u],
                    right_sem.at[u, me_z],
                    to,
                ).start()
                return _

            lax.fori_loop(0, nz - 1, send, 0)
            right_in[u, me_z] = right_u[me_z]

        def open_gate():
            for s in chunks:
                gate[:, s] = jax.nn.sigmoid(
                    jnp.dot(weights[4 * half : 5 * half, :], zn[:, s], preferred_element_type=F32)
                )

        def take_left(k):
            s = far_first(k)
            slot = left_all.at[u, me_x, s]

            @pl.when(k < nz - 1)
            def run():
                copy_z(slot, slot, sent_sem.at[0, u], left_sem.at[u, me_x, s], s).wait_recv()
                forward_left(slot, s)

            store_rows(left_mat, me_x, s * geo.rows, left_all[u, me_x, s].astype(F32))

        def take_left_x(k):
            s = far_first(k)
            for d in range(1, nx):
                x = lax.rem(me_x + d, nx)
                slot = left_all.at[u, x, s]
                copy_x(slot, slot, sent_sem.at[2, u], left_sem.at[u, x, s], x).wait_recv()
                store_rows(left_mat, x, s * geo.rows, left_all[u, x, s].astype(F32))

        def wait_right(k, s):
            slot = right_in.at[u, s]

            @pl.when(k < nz - 1)
            def run():
                copy_z(slot, slot, sent_sem.at[1, u], right_sem.at[u, s], s).wait_recv()

        def block_row(base, r):
            return jnp.concatenate([product[h, pl.ds(base + r, 1), :] for h in range(2)], axis=0)

        def send_back(k):
            to = far_first(k)
            base = to * geo.rows
            for b in range(geo.blocks):
                value = block_of(geo, functools.partial(block_row, base), b)
                back_u[to, :, b * LANES : (b + 1) * LANES] = value.astype(BF16)

            @pl.when(k < nz - 1)
            def run():
                copy_z(
                    back_u.at[to], back_in.at[u, me_z], sent_sem.at[4, u], back_sem.at[u, me_z], to
                ).start()

        project(0, left_u)
        send_left()
        project(2 * half, right_u)
        send_right()
        if u == 0:
            forward_right(right_u.at[me_z], me_z)
        open_gate()

        def take_lefts(k, _):
            take_left(k)

            @pl.when(k >= lag)
            def run():
                take_left_x(k - lag)

            return _

        lax.fori_loop(0, nz, take_lefts, 0)

        def take_right_x(k):
            s = far_first(k)
            at = s % geo.near

            @pl.when(s // geo.near == me_x)
            def run():
                for d in range(1, nx):
                    x = lax.rem(me_x + d, nx)
                    slot = right_all.at[x, at]
                    copy_x(slot, slot, sent_sem.at[3, 0], right_x_sem.at[x, at], x).wait_recv()
                    store_rows(right_mat, x, at * geo.rows, right_all[x, at].astype(F32))

        def take_right(k, _):
            s = far_first(k)
            wait_right(k, s)
            if u == 0:

                @pl.when(k < nz - 1)
                def run():
                    forward_right(right_in.at[0, s], s)

                @pl.when(s // geo.near == me_x)
                def run_own():
                    store_rows(
                        right_mat, me_x, (s % geo.near) * geo.rows, right_in[0, s].astype(F32)
                    )

                @pl.when(k >= lag)
                def run_x():
                    take_right_x(k - lag)

            else:
                store_rows(right_mat, 0, s * geo.rows, right_in[1, s].astype(F32))

            @pl.when(k < lag)
            def run_left():
                take_left_x(nz - lag + k)

            return _

        lax.fori_loop(0, nz, take_right, 0)

        if u == 0:

            def take_last(k, _):
                take_right_x(k)
                return _

            lax.fori_loop(nz - lag, nz, take_last, 0)

            for h in range(2):
                total = jnp.zeros((geo.res, geo.cols), F32)
                for x in range(nx):
                    total += lax.dot_general(
                        left_mat[x, h].astype(BF16),
                        right_mat[x, h, : geo.cols, :].astype(BF16),
                        (((1,), (1,)), ((), ())),
                        preferred_element_type=F32,
                    )
                product[h, :, : geo.cols] = total
        else:
            for h in range(2):
                right = right_mat[0, h].astype(BF16)
                for x in range(nx):
                    part = lax.dot_general(
                        left_mat[x, h].astype(BF16),
                        right,
                        (((0,), (0,)), ((), ())),
                        preferred_element_type=F32,
                    )
                    product[h, geo.cols * x : geo.cols * (x + 1), :] = part[: geo.cols, :]

        def send(k, _):
            send_back(k)
            return _

        lax.fori_loop(0, nz, send, 0)

        def take_back(k, _):
            s = far_first(k)
            slot = back_in.at[u, s]
            copy_z(slot, slot, sent_sem.at[4, u], back_sem.at[u, s], s).wait_recv()
            copy_c(slot, back_other.at[u, s], sent_sem.at[6, u], other_sem.at[u, s]).start()
            triangle[me_c, s] = back_in[u, s].astype(F32)
            return _

        copy_c(
            back_u.at[me_z], back_other.at[u, me_z], sent_sem.at[6, u], other_sem.at[u, me_z]
        ).start()
        triangle[me_c, me_z] = back_u[me_z].astype(F32)
        lax.fori_loop(0, nz - 1, take_back, 0)

        def take_other(k, _):
            slot = back_other.at[u, k]
            copy_c(slot, slot, sent_sem.at[6, u], other_sem.at[u, k]).wait_recv()
            triangle[other_c, k] = back_other[u, k].astype(F32)
            return _

        lax.fori_loop(0, nz, take_other, 0)

        at = wide + 2 + u
        gain_out = jnp.concatenate([z_all[0, c, :, at : at + 1] for c in range(2)], axis=0)
        for i in reversed(range(geo.extra)):
            s = chunks[i]
            values = jnp.concatenate(
                [triangle[c, k, :, s] for c in range(2) for k in range(nz)], axis=0
            )
            tn = normed(values, gain_out)
            change = jnp.dot(weights[5 * half :, :], tn, preferred_element_type=F32)
            value = z_all[u, me_c, :, s] + gate[:, s] * change
            if u == 0:
                z_all[1, me_c, :, s] = value
                z_piece(1, i).start()
            else:
                lane = lax.broadcasted_iota(jnp.int32, (half, LANES), 1)
                row = jnp.zeros((half, LANES), F32)
                for q in range(geo.pieces):
                    block = lane_block(value, q)
                    out_ref[:, i * geo.pieces + q, :] = block[:, : geo.cols]
                    low = geo.spare * q
                    moved = pltpu.roll(block, (low - geo.cols) % LANES, 1)
                    row = jnp.where((lane >= low) & (lane < low + geo.spare), moved, row)
                out_ref[:, geo.blocks + i, :] = row[:, : geo.cols]

    any_sem = z_sem.at[0, 0]
    for u in range(2):
        many = left_out.at[u, pl.ds(0, nz - 1)]
        copy_z(many, many, sent_sem.at[0, u], any_sem, me_z).wait_send()
        copy_z(many, many, sent_sem.at[1, u], any_sem, me_z).wait_send()
        copy_z(many, many, sent_sem.at[4, u], any_sem, me_z).wait_send()
        for k in range(1, nx):
            all_slots = left_out.at[u]
            copy_x(all_slots, all_slots, sent_sem.at[2, u], any_sem, me_x).wait_send()
        every = left_out.at[u]
        copy_c(every, every, sent_sem.at[6, u], any_sem).wait_send()
    away = left_out.at[0, pl.ds(0, nz - geo.near)]
    copy_x(away, away, sent_sem.at[3, 0], any_sem, me_x).wait_send()
    for u in range(2):
        part = z_all.at[u, me_c, :, : wide + (LANES if u == 0 else 0)]
        copy_c(part, part, sent_sem.at[5, u], any_sem).wait_send()


def per_device(
    geo, pair, residue_mask, norm_in_gain, proj_weight, gate_weight, norm_out_gain, out_weight
):
    half = pair.shape[0]
    full = 2 * half
    nz, nx = geo.nz, geo.nx
    vmem = pltpu.VMEM
    message = (2, geo.width)
    dma = pltpu.SemaphoreType.DMA
    hbm = pl.BlockSpec(memory_space=pl.ANY)
    return pl.pallas_call(
        functools.partial(kernel, geo, half),
        out_shape=jax.ShapeDtypeStruct(pair.shape, F32),
        in_specs=[
            hbm,
            pl.BlockSpec(memory_space=pltpu.SMEM),
            pl.BlockSpec(memory_space=vmem),
            hbm,
            hbm,
            hbm,
            hbm,
            hbm,
        ],
        out_specs=pl.BlockSpec(memory_space=vmem),
        scratch_shapes=[
            vmem(pair.shape, F32),
            vmem((2, *norm_in_gain.shape), F32),
            vmem(proj_weight.shape, BF16),
            vmem(gate_weight.shape, BF16),
            vmem(out_weight.shape, BF16),
            vmem((2, 6 * half, full), BF16),
            vmem((1, geo.width), F32),
            vmem((2, 2, half, geo.width + LANES), F32),
            vmem((full, geo.width), BF16),
            vmem((half, geo.width), F32),
            vmem((half, geo.width), F32),
            vmem((2, nz, *message), BF16),
            vmem((2, nz, *message), BF16),
            vmem((2, nx, nz, *message), BF16),
            vmem((2, nz, *message), BF16),
            vmem((nx, geo.near, *message), BF16),
            vmem((nx, 2, geo.res, LANES), F32),
            vmem((nx, 2, geo.res, LANES), F32),
            vmem((2, geo.res, LANES), F32),
            vmem((2, nz, *message), BF16),
            vmem((2, nz, *message), BF16),
            vmem((2, nz, *message), BF16),
            vmem((2, nz, *message), F32),
            dma((2, nx, nz)),
            dma((2, nz)),
            dma((nx, geo.near)),
            dma((2, nz)),
            dma((2, nz)),
            dma((2, geo.extra)),
            dma((7, 2)),
            dma((6,)),
        ],
        compiler_params=pltpu.CompilerParams(
            collective_id=0, has_side_effects=True, vmem_limit_bytes=60 * 1024 * 1024
        ),
        name="triangle_updates",
    )(
        pair,
        residue_mask,
        residue_mask[None, :],
        norm_in_gain,
        proj_weight,
        gate_weight,
        norm_out_gain,
        out_weight,
    )


def solution(mesh):
    def body(pair, *rest):
        geo = Geometry(pair.shape[1], pair.shape[2], mesh.shape["gx"], mesh.shape["gy"])
        return per_device(geo, pair, *rest)

    return jax.shard_map(
        body,
        mesh=mesh,
        in_specs=(
            P(("groups", "gz"), "gx", "gy"),
            P("groups"),
            P(None, "gz"),
            P(None, None, None, "gz"),
            P(None, None, "gz"),
            P(None, "gz"),
            P(None, None, "gz"),
        ),
        out_specs=P(("groups", "gz"), "gx", "gy"),
        check_vma=False,
    )
```

```python
import functools

import jax
import jax.numpy as jnp
from jax import lax
from jax.experimental import pallas as pl
from jax.experimental.pallas import tpu as pltpu
from jax.sharding import PartitionSpec as P

EPSILON = 1e-05
LANES = 128
MESH = pl.DeviceIdType.MESH
F32 = jnp.float32
BF16 = jnp.bfloat16


class Geometry:
    def __init__(self, rows, cols, nz, nx):
        self.rows, self.cols, self.nz, self.nx = rows, cols, nz, nx
        self.spare = LANES - cols
        self.blocks = rows * cols // LANES
        self.extra = rows - self.blocks
        self.pieces = cols // self.spare
        self.width = self.blocks * LANES
        self.res = nz * rows
        self.near = cols // rows
        assert self.blocks * LANES == rows * cols
        assert self.extra * self.pieces == self.blocks
        assert nz * rows == nx * cols and self.near * rows == cols


def lane_block(v, k):
    return v[:, k * LANES : (k + 1) * LANES]


def rows_of(geo, v):
    lane = lax.broadcasted_iota(jnp.int32, (v.shape[0], LANES), 1)
    rows = [jnp.where(lane < geo.cols, lane_block(v, r), 0.0) for r in range(geo.blocks)]
    for e in range(geo.extra):
        row = jnp.zeros((v.shape[0], LANES), F32)
        for q in range(geo.pieces):
            low = geo.spare * q
            piece = pltpu.roll(lane_block(v, e * geo.pieces + q), (low - geo.cols) % LANES, 1)
            row = jnp.where((lane >= low) & (lane < low + geo.spare), piece, row)
        rows.append(row)
    return rows


def block_of(geo, get_row, k):
    row = get_row(k)
    lane = lax.broadcasted_iota(jnp.int32, row.shape, 1)
    extra, q = divmod(k, geo.pieces)
    piece = pltpu.roll(get_row(geo.blocks + extra), geo.cols - geo.spare * q, 1)
    return jnp.where(lane < geo.cols, row, piece)


def normed(values, gain):
    mean = jnp.mean(values, axis=0, keepdims=True)
    centred = values - mean
    spread = jnp.mean(centred * centred, axis=0, keepdims=True)
    return (centred * lax.rsqrt(spread + EPSILON) * gain).astype(BF16)


def kernel(
    geo,
    half,
    pair_hbm,
    flag_ref,
    gain_in_hbm,
    proj_hbm,
    gate_hbm,
    gain_out_hbm,
    out_hbm,
    out_ref,
    pair_ref,
    gains,
    proj_ref,
    gate_ref,
    out_weight_ref,
    mask_ref,
    z_all,
    zn,
    tmp,
    gate,
    left_out,
    right_out,
    left_all,
    right_in,
    right_all,
    left_mat,
    right_mat,
    product,
    back_out,
    back_in,
    back_other,
    triangle,
    left_sem,
    right_sem,
    right_x_sem,
    back_sem,
    other_sem,
    z_sem,
    sent_sem,
    load_sem,
):
    nz, nx = geo.nz, geo.nx
    me_z = lax.axis_index("gx")
    me_x = lax.axis_index("gy")
    me_c = lax.axis_index("gz")
    other_c = 1 - me_c
    chunk = geo.pieces * LANES
    chunks = [slice(k, k + chunk) for k in range(0, geo.width, chunk)]

    barrier = pltpu.get_barrier_semaphore()

    def signal_z(k, _):
        pl.semaphore_signal(
            barrier, inc=1, device_id={"gx": lax.rem(me_z + 1 + k, nz)}, device_id_type=MESH
        )
        return _

    lax.fori_loop(0, nz - 1, signal_z, 0)
    for k in range(1, nx):
        pl.semaphore_signal(
            barrier, inc=1, device_id={"gy": lax.rem(me_x + k, nx)}, device_id_type=MESH
        )
    pl.semaphore_signal(barrier, inc=1, device_id={"gz": other_c}, device_id_type=MESH)

    def far_first(k):
        m = (k + 1) // 2
        return lax.rem(me_z + nz // 2 + m * (1 - 2 * (k % 2)), nz)

    def copy_z(src, dst, send, recv, to):
        return pltpu.make_async_remote_copy(
            src_ref=src, dst_ref=dst, send_sem=send, recv_sem=recv, device_id={"gx": to}, device_id_type=MESH
        )

    def copy_x(src, dst, send, recv, to):
        return pltpu.make_async_remote_copy(
            src_ref=src, dst_ref=dst, send_sem=send, recv_sem=recv, device_id={"gy": to}, device_id_type=MESH
        )

    def copy_c(src, dst, send, recv):
        return pltpu.make_async_remote_copy(
            src_ref=src, dst_ref=dst, send_sem=send, recv_sem=recv, device_id={"gz": other_c}, device_id_type=MESH
        )

    def store_rows(mat, lead, base, value):
        for r, row in enumerate(rows_of(geo, value)):
            for h in range(2):
                mat[lead, h, pl.ds(base + r, 1), :] = row[h : h + 1, :]

    lag = 8
    wide = geo.width

    loads = [
        pltpu.make_async_copy(src, dst, load_sem.at[i])
        for i, (src, dst) in enumerate(
            [
                (pair_hbm, pair_ref),
                (gain_in_hbm, gains.at[0]),
                (gain_out_hbm, gains.at[1]),
                (proj_hbm, proj_ref),
                (gate_hbm, gate_ref),
                (out_hbm, out_weight_ref),
            ]
        )
    ]
    for load in loads:
        load.start()
    for load in loads[:3]:
        load.wait()
    for k in range(geo.blocks):
        e, q = divmod(k, geo.pieces)
        low = geo.spare * q
        z_all[0, me_c, :, k * LANES : (k + 1) * LANES] = jnp.concatenate(
            [pair_ref[k], pair_ref[geo.blocks + e, :, low : low + geo.spare]], axis=1
        )
    diagonal = lax.broadcasted_iota(jnp.int32, (half, half), 0) == lax.broadcasted_iota(
        jnp.int32, (half, half), 1
    )
    columns = [
        jnp.sum(jnp.where(diagonal, gains[kind, u : u + 1, :], 0.0), axis=1, keepdims=True)
        for kind in range(2)
        for u in range(2)
    ]
    lane = lax.broadcasted_iota(jnp.int32, (half, LANES), 1)
    last = jnp.zeros((half, LANES), F32)
    for i, column in enumerate(columns):
        last = jnp.where(lane == i, column, last)
    z_all[0, me_c, :, wide:] = last

    near_lane = lax.broadcasted_iota(jnp.int32, (1, LANES), 1)
    near_flags = jnp.zeros((1, LANES), F32)
    for t in range(geo.cols):
        flag = flag_ref[me_x * geo.cols + t].astype(F32)
        near_flags = jnp.where(near_lane == t, flag, near_flags)
    row_flag = [flag_ref[me_z * geo.rows + r].astype(F32) for r in range(geo.rows)]
    for k in range(geo.blocks):
        mask_ref[:, k * LANES : (k + 1) * LANES] = block_of(
            geo, lambda r: near_flags * row_flag[r], k
        )

    for load in loads[3:]:
        load.wait()

    pl.semaphore_wait(barrier, nz - 1 + nx - 1 + 1)

    def z_piece(u, i):
        low = i * chunk
        high = low + chunk + (LANES if u == 0 and i == geo.extra - 1 else 0)
        part = z_all.at[u, me_c, :, low:high]
        return copy_c(part, part, sent_sem.at[5, u], z_sem.at[u, i])

    for i in reversed(range(geo.extra)):
        z_piece(0, i).start()

    for u in range(2):
        left_u, right_u, back_u = left_out.at[u], right_out.at[u], back_out.at[u]

        for i in reversed(range(geo.extra)):
            z_piece(u, i).wait_recv()
            s = chunks[i]
            if i == geo.extra - 1:
                gain_in = jnp.concatenate(
                    [z_all[0, c, :, wide + u : wide + u + 1] for c in range(2)], axis=0
                )
            z = jnp.concatenate([z_all[u, 0, :, s], z_all[u, 1, :, s]], axis=0)
            zn[:, s] = normed(z, gain_in)

        def project(first, out):
            for s in chunks:
                opening, value = (
                    jnp.dot(proj_ref[u, first + i], zn[:, s], preferred_element_type=F32)
                    for i in range(2)
                )
                tmp[:, s] = jax.nn.sigmoid(opening) * value * mask_ref[:, s]
            for k in range(nz):
                out[k] = tmp[2 * k : 2 * k + 2, :].astype(BF16)

        def forward_left(src, s):
            for k in range(1, nx):
                copy_x(
                    src,
                    left_all.at[u, me_x, s],
                    sent_sem.at[2, u],
                    left_sem.at[u, me_x, s],
                    lax.rem(me_x + k, nx),
                ).start()

        def forward_right(src, s):
            target = s // geo.near

            @pl.when(target != me_x)
            def run():
                copy_x(
                    src,
                    right_all.at[me_x, s % geo.near],
                    sent_sem.at[3, 0],
                    right_x_sem.at[me_x, s % geo.near],
                    target,
                ).start()

        def send_left():
            def send(k, _):
                to = far_first(k)
                copy_z(
                    left_u.at[to],
                    left_all.at[u, me_x, me_z],
                    sent_sem.at[0, u],
                    left_sem.at[u, me_x, me_z],
                    to,
                ).start()
                return _

            lax.fori_loop(0, nz - 1, send, 0)
            forward_left(left_u.at[me_z], me_z)
            left_all[u, me_x, me_z] = left_u[me_z]

        def send_right():
            def send(k, _):
                to = far_first(k)
                copy_z(
                    right_u.at[to],
                    right_in.at[u, me_z],
                    sent_sem.at[1, u],
                    right_sem.at[u, me_z],
                    to,
                ).start()
                return _

            lax.fori_loop(0, nz - 1, send, 0)
            right_in[u, me_z] = right_u[me_z]

        def open_gate():
            for s in chunks:
                gate[:, s] = jax.nn.sigmoid(
                    jnp.dot(gate_ref[u], zn[:, s], preferred_element_type=F32)
                )

        def take_left(k):
            s = far_first(k)
            slot = left_all.at[u, me_x, s]

            @pl.when(k < nz - 1)
            def run():
                copy_z(slot, slot, sent_sem.at[0, u], left_sem.at[u, me_x, s], s).wait_recv()
                forward_left(slot, s)

            store_rows(left_mat, me_x, s * geo.rows, left_all[u, me_x, s].astype(F32))

        def take_left_x(k):
            s = far_first(k)
            for d in range(1, nx):
                x = lax.rem(me_x + d, nx)
                slot = left_all.at[u, x, s]
                copy_x(slot, slot, sent_sem.at[2, u], left_sem.at[u, x, s], x).wait_recv()
                store_rows(left_mat, x, s * geo.rows, left_all[u, x, s].astype(F32))

        def wait_right(k, s):
            slot = right_in.at[u, s]

            @pl.when(k < nz - 1)
            def run():
                copy_z(slot, slot, sent_sem.at[1, u], right_sem.at[u, s], s).wait_recv()

        def block_row(base, r):
            return jnp.concatenate([product[h, pl.ds(base + r, 1), :] for h in range(2)], axis=0)

        def send_back(k):
            to = far_first(k)
            base = to * geo.rows
            for b in range(geo.blocks):
                value = block_of(geo, functools.partial(block_row, base), b)
                back_u[to, :, b * LANES : (b + 1) * LANES] = value.astype(BF16)

            @pl.when(k < nz - 1)
            def run():
                copy_z(
                    back_u.at[to], back_in.at[u, me_z], sent_sem.at[4, u], back_sem.at[u, me_z], to
                ).start()

        project(0, left_u)
        send_left()
        project(2, right_u)
        send_right()
        if u == 0:
            forward_right(right_u.at[me_z], me_z)
        open_gate()

        def take_lefts(k, _):
            take_left(k)

            @pl.when(k >= lag)
            def run():
                take_left_x(k - lag)

            return _

        lax.fori_loop(0, nz, take_lefts, 0)

        def take_right_x(k):
            s = far_first(k)
            at = s % geo.near

            @pl.when(s // geo.near == me_x)
            def run():
                for d in range(1, nx):
                    x = lax.rem(me_x + d, nx)
                    slot = right_all.at[x, at]
                    copy_x(slot, slot, sent_sem.at[3, 0], right_x_sem.at[x, at], x).wait_recv()
                    store_rows(right_mat, x, at * geo.rows, right_all[x, at].astype(F32))

        def take_right(k, _):
            s = far_first(k)
            wait_right(k, s)
            if u == 0:

                @pl.when(k < nz - 1)
                def run():
                    forward_right(right_in.at[0, s], s)

                @pl.when(s // geo.near == me_x)
                def run_own():
                    store_rows(
                        right_mat, me_x, (s % geo.near) * geo.rows, right_in[0, s].astype(F32)
                    )

                @pl.when(k >= lag)
                def run_x():
                    take_right_x(k - lag)

            else:
                store_rows(right_mat, 0, s * geo.rows, right_in[1, s].astype(F32))

            @pl.when(k < lag)
            def run_left():
                take_left_x(nz - lag + k)

            return _

        lax.fori_loop(0, nz, take_right, 0)

        if u == 0:

            def take_last(k, _):
                take_right_x(k)
                return _

            lax.fori_loop(nz - lag, nz, take_last, 0)

            for h in range(2):
                total = jnp.zeros((geo.res, geo.cols), F32)
                for x in range(nx):
                    total += lax.dot_general(
                        left_mat[x, h].astype(BF16),
                        right_mat[x, h, : geo.cols, :].astype(BF16),
                        (((1,), (1,)), ((), ())),
                        preferred_element_type=F32,
                    )
                product[h, :, : geo.cols] = total
        else:
            for h in range(2):
                right = right_mat[0, h].astype(BF16)
                for x in range(nx):
                    part = lax.dot_general(
                        left_mat[x, h].astype(BF16),
                        right,
                        (((0,), (0,)), ((), ())),
                        preferred_element_type=F32,
                    )
                    product[h, geo.cols * x : geo.cols * (x + 1), :] = part[: geo.cols, :]

        def send(k, _):
            send_back(k)
            return _

        lax.fori_loop(0, nz, send, 0)

        def take_back(k, _):
            s = far_first(k)
            slot = back_in.at[u, s]
            copy_z(slot, slot, sent_sem.at[4, u], back_sem.at[u, s], s).wait_recv()
            copy_c(slot, back_other.at[u, s], sent_sem.at[6, u], other_sem.at[u, s]).start()
            triangle[me_c, s] = back_in[u, s].astype(F32)
            return _

        copy_c(
            back_u.at[me_z], back_other.at[u, me_z], sent_sem.at[6, u], other_sem.at[u, me_z]
        ).start()
        triangle[me_c, me_z] = back_u[me_z].astype(F32)
        lax.fori_loop(0, nz - 1, take_back, 0)

        def take_other(k, _):
            slot = back_other.at[u, k]
            copy_c(slot, slot, sent_sem.at[6, u], other_sem.at[u, k]).wait_recv()
            triangle[other_c, k] = back_other[u, k].astype(F32)
            return _

        lax.fori_loop(0, nz, take_other, 0)

        at = wide + 2 + u
        gain_out = jnp.concatenate([z_all[0, c, :, at : at + 1] for c in range(2)], axis=0)
        for i in reversed(range(geo.extra)):
            s = chunks[i]
            values = jnp.concatenate(
                [triangle[c, k, :, s] for c in range(2) for k in range(nz)], axis=0
            )
            tn = normed(values, gain_out)
            change = jnp.dot(out_weight_ref[u], tn, preferred_element_type=F32)
            value = z_all[u, me_c, :, s] + gate[:, s] * change
            if u == 0:
                z_all[1, me_c, :, s] = value
                z_piece(1, i).start()
            else:
                lane = lax.broadcasted_iota(jnp.int32, (half, LANES), 1)
                row = jnp.zeros((half, LANES), F32)
                for q in range(geo.pieces):
                    block = lane_block(value, q)
                    out_ref[i * geo.pieces + q] = block[:, : geo.cols]
                    low = geo.spare * q
                    moved = pltpu.roll(block, (low - geo.cols) % LANES, 1)
                    row = jnp.where((lane >= low) & (lane < low + geo.spare), moved, row)
                out_ref[geo.blocks + i] = row[:, : geo.cols]

    any_sem = z_sem.at[0, 0]
    for u in range(2):
        many = left_out.at[u, pl.ds(0, nz - 1)]
        copy_z(many, many, sent_sem.at[0, u], any_sem, me_z).wait_send()
        copy_z(many, many, sent_sem.at[1, u], any_sem, me_z).wait_send()
        copy_z(many, many, sent_sem.at[4, u], any_sem, me_z).wait_send()
        for k in range(1, nx):
            all_slots = left_out.at[u]
            copy_x(all_slots, all_slots, sent_sem.at[2, u], any_sem, me_x).wait_send()
        every = left_out.at[u]
        copy_c(every, every, sent_sem.at[6, u], any_sem).wait_send()
    away = left_out.at[0, pl.ds(0, nz - geo.near)]
    copy_x(away, away, sent_sem.at[3, 0], any_sem, me_x).wait_send()
    for u in range(2):
        part = z_all.at[u, me_c, :, : wide + (LANES if u == 0 else 0)]
        copy_c(part, part, sent_sem.at[5, u], any_sem).wait_send()


def per_device(
    geo, pair, residue_mask, norm_in_gain, proj_weight, gate_weight, norm_out_gain, out_weight
):
    half = pair.shape[0]
    full = 2 * half
    nz, nx = geo.nz, geo.nx
    vmem = pltpu.VMEM
    message = (2, geo.width)
    dma = pltpu.SemaphoreType.DMA
    hbm = pl.BlockSpec(memory_space=pl.ANY)
    pair = jnp.swapaxes(pair, 0, 1)
    proj_weight = jnp.swapaxes(proj_weight, 2, 3)
    gate_weight = jnp.swapaxes(gate_weight, 1, 2)
    out_weight = jnp.swapaxes(out_weight, 1, 2)
    result = pl.pallas_call(
        functools.partial(kernel, geo, half),
        out_shape=jax.ShapeDtypeStruct(pair.shape, F32),
        in_specs=[
            hbm,
            pl.BlockSpec(memory_space=pltpu.SMEM),
            hbm,
            hbm,
            hbm,
            hbm,
            hbm,
        ],
        out_specs=pl.BlockSpec(memory_space=vmem),
        scratch_shapes=[
            vmem(pair.shape, F32),
            vmem((2, *norm_in_gain.shape), F32),
            vmem(proj_weight.shape, BF16),
            vmem(gate_weight.shape, BF16),
            vmem(out_weight.shape, BF16),
            vmem((1, geo.width), F32),
            vmem((2, 2, half, geo.width + LANES), F32),
            vmem((full, geo.width), BF16),
            vmem((half, geo.width), F32),
            vmem((half, geo.width), F32),
            vmem((2, nz, *message), BF16),
            vmem((2, nz, *message), BF16),
            vmem((2, nx, nz, *message), BF16),
            vmem((2, nz, *message), BF16),
            vmem((nx, geo.near, *message), BF16),
            vmem((nx, 2, geo.res, LANES), F32),
            vmem((nx, 2, geo.res, LANES), F32),
            vmem((2, geo.res, LANES), F32),
            vmem((2, nz, *message), BF16),
            vmem((2, nz, *message), BF16),
            vmem((2, nz, *message), BF16),
            vmem((2, nz, *message), F32),
            dma((2, nx, nz)),
            dma((2, nz)),
            dma((nx, geo.near)),
            dma((2, nz)),
            dma((2, nz)),
            dma((2, geo.extra)),
            dma((7, 2)),
            dma((6,)),
        ],
        compiler_params=pltpu.CompilerParams(
            collective_id=0, has_side_effects=True, vmem_limit_bytes=60 * 1024 * 1024
        ),
        name="triangle_updates",
    )(
        pair,
        residue_mask,
        norm_in_gain,
        proj_weight,
        gate_weight,
        norm_out_gain,
        out_weight,
    )
    return jnp.swapaxes(result, 0, 1)


def solution(mesh):
    def body(pair, *rest):
        geo = Geometry(pair.shape[1], pair.shape[2], mesh.shape["gx"], mesh.shape["gy"])
        return per_device(geo, pair, *rest)

    return jax.shard_map(
        body,
        mesh=mesh,
        in_specs=(
            P(("groups", "gz"), "gx", "gy"),
            P("groups"),
            P(None, "gz"),
            P(None, None, None, "gz"),
            P(None, None, "gz"),
            P(None, "gz"),
            P(None, None, "gz"),
        ),
        out_specs=P(("groups", "gz"), "gx", "gy"),
        check_vma=False,
    )
```

```python
import functools

import jax
import jax.numpy as jnp
from jax import lax
from jax.experimental import pallas as pl
from jax.experimental.pallas import tpu as pltpu
from jax.sharding import PartitionSpec as P

EPSILON = 1e-05
LANES = 128
MESH = pl.DeviceIdType.MESH
F32 = jnp.float32
BF16 = jnp.bfloat16


class Geometry:
    def __init__(self, rows, cols, nz, nx):
        self.rows, self.cols, self.nz, self.nx = rows, cols, nz, nx
        self.spare = LANES - cols
        self.blocks = rows * cols // LANES
        self.extra = rows - self.blocks
        self.pieces = cols // self.spare
        self.width = self.blocks * LANES
        self.res = nz * rows
        self.near = cols // rows
        assert self.blocks * LANES == rows * cols
        assert self.extra * self.pieces == self.blocks
        assert nz * rows == nx * cols and self.near * rows == cols


def lane_block(v, k):
    return v[:, k * LANES : (k + 1) * LANES]


def rows_of(geo, v):
    lane = lax.broadcasted_iota(jnp.int32, (v.shape[0], LANES), 1)
    rows = [jnp.where(lane < geo.cols, lane_block(v, r), 0.0) for r in range(geo.blocks)]
    for e in range(geo.extra):
        row = jnp.zeros((v.shape[0], LANES), F32)
        for q in range(geo.pieces):
            low = geo.spare * q
            piece = pltpu.roll(lane_block(v, e * geo.pieces + q), (low - geo.cols) % LANES, 1)
            row = jnp.where((lane >= low) & (lane < low + geo.spare), piece, row)
        rows.append(row)
    return rows


def block_of(geo, get_row, k):
    row = get_row(k)
    lane = lax.broadcasted_iota(jnp.int32, row.shape, 1)
    extra, q = divmod(k, geo.pieces)
    piece = pltpu.roll(get_row(geo.blocks + extra), geo.cols - geo.spare * q, 1)
    return jnp.where(lane < geo.cols, row, piece)


def normed(values, gain):
    mean = jnp.mean(values, axis=0, keepdims=True)
    centred = values - mean
    spread = jnp.mean(centred * centred, axis=0, keepdims=True)
    return (centred * lax.rsqrt(spread + EPSILON) * gain).astype(BF16)


def kernel(
    geo,
    half,
    pair_hbm,
    flag_ref,
    gain_in_hbm,
    proj_hbm,
    gate_hbm,
    gain_out_hbm,
    out_hbm,
    out_ref,
    pair_ref,
    gains,
    proj_ref,
    gate_ref,
    out_weight_ref,
    mask_ref,
    z_all,
    zn,
    tmp,
    gate,
    left_out,
    right_out,
    left_all,
    right_in,
    right_all,
    left_mat,
    right_mat,
    product,
    back_out,
    back_in,
    back_other,
    triangle,
    left_sem,
    right_sem,
    right_x_sem,
    back_sem,
    other_sem,
    z_sem,
    sent_sem,
    load_sem,
    up_sem,
    down_sem,
):
    nz, nx = geo.nz, geo.nx
    me_z = lax.axis_index("gx")
    me_x = lax.axis_index("gy")
    me_c = lax.axis_index("gz")
    other_c = 1 - me_c
    chunk = geo.pieces * LANES
    chunks = [slice(k, k + chunk) for k in range(0, geo.width, chunk)]

    barrier = pltpu.get_barrier_semaphore()

    after = lax.rem(me_z + 1, nz)
    before = lax.rem(me_z + nz - 1, nz)
    for neighbour in (before, after):
        pl.semaphore_signal(barrier, inc=1, device_id={"gx": neighbour}, device_id_type=MESH)
    for k in range(1, nx):
        pl.semaphore_signal(
            barrier, inc=1, device_id={"gy": lax.rem(me_x + k, nx)}, device_id_type=MESH
        )
    pl.semaphore_signal(barrier, inc=1, device_id={"gz": other_c}, device_id_type=MESH)

    def far_first(k):
        m = (k + 1) // 2
        return lax.rem(me_z + nz // 2 + m * (1 - 2 * (k % 2)), nz)

    def copy_z(src, dst, send, recv, to):
        return pltpu.make_async_remote_copy(
            src_ref=src, dst_ref=dst, send_sem=send, recv_sem=recv, device_id={"gx": to}, device_id_type=MESH
        )

    def copy_x(src, dst, send, recv, to):
        return pltpu.make_async_remote_copy(
            src_ref=src, dst_ref=dst, send_sem=send, recv_sem=recv, device_id={"gy": to}, device_id_type=MESH
        )

    def copy_c(src, dst, send, recv):
        return pltpu.make_async_remote_copy(
            src_ref=src, dst_ref=dst, send_sem=send, recv_sem=recv, device_id={"gz": other_c}, device_id_type=MESH
        )

    def store_rows(mat, lead, base, value):
        for r, row in enumerate(rows_of(geo, value)):
            for h in range(2):
                mat[lead, h, pl.ds(base + r, 1), :] = row[h : h + 1, :]

    lag = 6
    wide = geo.width

    loads = [
        pltpu.make_async_copy(src, dst, load_sem.at[i])
        for i, (src, dst) in enumerate(
            [
                (pair_hbm, pair_ref),
                (gain_in_hbm, gains.at[0]),
                (gain_out_hbm, gains.at[1]),
                (proj_hbm, proj_ref),
                (gate_hbm, gate_ref),
                (out_hbm, out_weight_ref),
            ]
        )
    ]
    for load in loads:
        load.start()
    for load in loads[:3]:
        load.wait()
    for k in range(geo.blocks):
        e, q = divmod(k, geo.pieces)
        low = geo.spare * q
        z_all[0, me_c, :, k * LANES : (k + 1) * LANES] = jnp.concatenate(
            [pair_ref[k], pair_ref[geo.blocks + e, :, low : low + geo.spare]], axis=1
        )
    diagonal = lax.broadcasted_iota(jnp.int32, (half, half), 0) == lax.broadcasted_iota(
        jnp.int32, (half, half), 1
    )
    columns = [
        jnp.sum(jnp.where(diagonal, gains[kind, u : u + 1, :], 0.0), axis=1, keepdims=True)
        for kind in range(2)
        for u in range(2)
    ]
    lane = lax.broadcasted_iota(jnp.int32, (half, LANES), 1)
    last = jnp.zeros((half, LANES), F32)
    for i, column in enumerate(columns):
        last = jnp.where(lane == i, column, last)
    z_all[0, me_c, :, wide:] = last

    near_lane = lax.broadcasted_iota(jnp.int32, (1, LANES), 1)
    near_flags = jnp.zeros((1, LANES), F32)
    for t in range(geo.cols):
        flag = flag_ref[me_x * geo.cols + t].astype(F32)
        near_flags = jnp.where(near_lane == t, flag, near_flags)
    row_flag = [flag_ref[me_z * geo.rows + r].astype(F32) for r in range(geo.rows)]
    for k in range(geo.blocks):
        mask_ref[:, k * LANES : (k + 1) * LANES] = block_of(
            geo, lambda r: near_flags * row_flag[r], k
        )

    for load in loads[3:]:
        load.wait()

    pl.semaphore_wait(barrier, 2 + nx - 1 + 1)

    def z_piece(u, i):
        low = i * chunk
        high = low + chunk + (LANES if u == 0 and i == geo.extra - 1 else 0)
        part = z_all.at[u, me_c, :, low:high]
        return copy_c(part, part, sent_sem.at[5, u], z_sem.at[u, i])

    for i in reversed(range(geo.extra)):
        z_piece(0, i).start()

    middle = nz // 2
    early = jnp.where(me_z >= middle, middle, jnp.where(me_z == 0, middle - 1, me_z))
    later = jnp.where(me_z < middle, middle, nz - 1 - me_z)
    up_limit = jnp.where(after >= middle, middle, middle - 1)
    down_limit = jnp.where(before < middle, middle, middle - 1)
    below = me_z < middle

    def hear_up(j):
        @pl.when(j > 1)
        def run():
            pl.semaphore_wait(up_sem.at[j], 1)

        @pl.when(j < up_limit)
        def relay():
            pl.semaphore_signal(up_sem.at[j + 1], inc=1, device_id={"gx": after}, device_id_type=MESH)

    def hear_down(j):
        @pl.when(j > 1)
        def run():
            pl.semaphore_wait(down_sem.at[j], 1)

        @pl.when(j < down_limit)
        def relay():
            pl.semaphore_signal(
                down_sem.at[j + 1], inc=1, device_id={"gx": before}, device_id_type=MESH
            )

    def hear_early(j, _):
        hear_up(j)
        return _

    lax.fori_loop(1, early + 1, hear_early, 0)

    def by_word(n):
        crossed = n - early - later
        s = jnp.where(
            n < early,
            me_z - 1 - n,
            jnp.where(
                n < early + later,
                me_z + 1 + n - early,
                jnp.where(below, me_z - early - 1 - crossed, me_z + later + 1 + crossed),
            ),
        )
        return jnp.where(n == nz - 1, me_z, lax.rem(s + nz, nz))

    for u in range(2):
        left_u, right_u, back_u = left_out.at[u], right_out.at[u], back_out.at[u]

        for i in reversed(range(geo.extra)):
            z_piece(u, i).wait_recv()
            s = chunks[i]
            if i == geo.extra - 1:
                gain_in = jnp.concatenate(
                    [z_all[0, c, :, wide + u : wide + u + 1] for c in range(2)], axis=0
                )
            z = jnp.concatenate([z_all[u, 0, :, s], z_all[u, 1, :, s]], axis=0)
            zn[:, s] = normed(z, gain_in)

        def project(first, out):
            for s in chunks:
                opening, value = (
                    jnp.dot(proj_ref[u, first + i], zn[:, s], preferred_element_type=F32)
                    for i in range(2)
                )
                tmp[:, s] = jax.nn.sigmoid(opening) * value * mask_ref[:, s]
            for k in range(nz):
                out[k] = tmp[2 * k : 2 * k + 2, :].astype(BF16)

        def forward_left(src, s):
            for k in range(1, nx):
                copy_x(
                    src,
                    left_all.at[u, me_x, s],
                    sent_sem.at[2, u],
                    left_sem.at[u, me_x, s],
                    lax.rem(me_x + k, nx),
                ).start()

        def forward_right(src, s):
            target = s // geo.near

            @pl.when(target != me_x)
            def run():
                copy_x(
                    src,
                    right_all.at[me_x, s % geo.near],
                    sent_sem.at[3, 0],
                    right_x_sem.at[me_x, s % geo.near],
                    target,
                ).start()

        def send_left(to):
            copy_z(
                left_u.at[to],
                left_all.at[u, me_x, me_z],
                sent_sem.at[0, u],
                left_sem.at[u, me_x, me_z],
                to,
            ).start()

        def send_right(to):
            copy_z(
                right_u.at[to],
                right_in.at[u, me_z],
                sent_sem.at[1, u],
                right_sem.at[u, me_z],
                to,
            ).start()

        def open_gate():
            for s in chunks:
                gate[:, s] = jax.nn.sigmoid(
                    jnp.dot(gate_ref[u], zn[:, s], preferred_element_type=F32)
                )

        source = by_word if u == 0 else far_first

        def take_left(k):
            s = source(k)
            slot = left_all.at[u, me_x, s]

            @pl.when(k < nz - 1)
            def run():
                copy_z(slot, slot, sent_sem.at[0, u], left_sem.at[u, me_x, s], s).wait_recv()
                forward_left(slot, s)

            store_rows(left_mat, me_x, s * geo.rows, left_all[u, me_x, s].astype(F32))

        def take_left_x(k):
            s = source(k)
            for d in range(1, nx):
                x = lax.rem(me_x + d, nx)
                slot = left_all.at[u, x, s]
                copy_x(slot, slot, sent_sem.at[2, u], left_sem.at[u, x, s], x).wait_recv()
                store_rows(left_mat, x, s * geo.rows, left_all[u, x, s].astype(F32))

        def wait_right(k, s):
            slot = right_in.at[u, s]

            @pl.when(k < nz - 1)
            def run():
                copy_z(slot, slot, sent_sem.at[1, u], right_sem.at[u, s], s).wait_recv()

        def block_row(base, r):
            return jnp.concatenate([product[h, pl.ds(base + r, 1), :] for h in range(2)], axis=0)

        def send_back(k):
            to = far_first(k)
            base = to * geo.rows
            for b in range(geo.blocks):
                value = block_of(geo, functools.partial(block_row, base), b)
                back_u[to, :, b * LANES : (b + 1) * LANES] = value.astype(BF16)

            @pl.when(k < nz - 1)
            def run():
                copy_z(
                    back_u.at[to], back_in.at[u, me_z], sent_sem.at[4, u], back_sem.at[u, me_z], to
                ).start()

        def take_right_x(k):
            s = source(k)
            at = s % geo.near

            @pl.when(s // geo.near == me_x)
            def run():
                for d in range(1, nx):
                    x = lax.rem(me_x + d, nx)
                    slot = right_all.at[x, at]
                    copy_x(slot, slot, sent_sem.at[3, 0], right_x_sem.at[x, at], x).wait_recv()
                    store_rows(right_mat, x, at * geo.rows, right_all[x, at].astype(F32))

        project(0, left_u)
        forward_left(left_u.at[me_z], me_z)
        left_all[u, me_x, me_z] = left_u[me_z]
        if u == 0:
            project(2, right_u)
            forward_right(right_u.at[me_z], me_z)
            right_in[u, me_z] = right_u[me_z]

            def send_both(to):
                to = lax.rem(to + nz, nz)
                send_left(to)
                send_right(to)

            def send_early(n, _):
                send_both(me_z - early + n)
                return _

            def send_down(j, _):
                hear_down(j)
                send_both(me_z + j)
                return _

            def send_up(j, _):
                hear_up(j)
                send_both(me_z - j)
                return _

            lax.fori_loop(0, early, send_early, 0)
            open_gate()
            lax.fori_loop(1, later + 1, send_down, 0)
            lax.fori_loop(jnp.where(below, early + 1, middle), middle, send_up, 0)
            lax.fori_loop(jnp.where(below, middle, later + 1), middle, send_down, 0)

            def take_both(k, _):
                s = source(k)
                take_left(k)
                wait_right(k, s)

                @pl.when(k < nz - 1)
                def run():
                    forward_right(right_in.at[0, s], s)

                @pl.when(s // geo.near == me_x)
                def run_own():
                    store_rows(
                        right_mat, me_x, (s % geo.near) * geo.rows, right_in[0, s].astype(F32)
                    )

                @pl.when(k >= lag)
                def run_x():
                    take_left_x(k - lag)
                    take_right_x(k - lag)

                return _

            lax.fori_loop(0, nz, take_both, 0)
        else:

            def send_lefts(k, _):
                send_left(far_first(k))
                return _

            def send_rights(k, _):
                send_right(far_first(k))
                return _

            lax.fori_loop(0, nz - 1, send_lefts, 0)
            project(2, right_u)
            lax.fori_loop(0, nz - 1, send_rights, 0)
            right_in[u, me_z] = right_u[me_z]
            open_gate()

            def take_lefts(k, _):
                take_left(k)

                @pl.when(k >= lag)
                def run():
                    take_left_x(k - lag)

                return _

            lax.fori_loop(0, nz, take_lefts, 0)

            def take_rights(k, _):
                s = source(k)
                wait_right(k, s)
                store_rows(right_mat, 0, s * geo.rows, right_in[1, s].astype(F32))

                @pl.when(k < lag)
                def run_left():
                    take_left_x(nz - lag + k)

                return _

            lax.fori_loop(0, nz, take_rights, 0)

        if u == 0:

            def take_last(k, _):
                take_left_x(k)
                take_right_x(k)
                return _

            lax.fori_loop(nz - lag, nz, take_last, 0)

            for h in range(2):
                total = jnp.zeros((geo.res, geo.cols), F32)
                for x in range(nx):
                    total += lax.dot_general(
                        left_mat[x, h].astype(BF16),
                        right_mat[x, h, : geo.cols, :].astype(BF16),
                        (((1,), (1,)), ((), ())),
                        preferred_element_type=F32,
                    )
                product[h, :, : geo.cols] = total
        else:
            for h in range(2):
                right = right_mat[0, h].astype(BF16)
                for x in range(nx):
                    part = lax.dot_general(
                        left_mat[x, h].astype(BF16),
                        right,
                        (((0,), (0,)), ((), ())),
                        preferred_element_type=F32,
                    )
                    product[h, geo.cols * x : geo.cols * (x + 1), :] = part[: geo.cols, :]

        def send(k, _):
            send_back(k)
            return _

        lax.fori_loop(0, nz, send, 0)

        def take_back(k, _):
            s = far_first(k)
            slot = back_in.at[u, s]
            copy_z(slot, slot, sent_sem.at[4, u], back_sem.at[u, s], s).wait_recv()
            copy_c(slot, back_other.at[u, s], sent_sem.at[6, u], other_sem.at[u, s]).start()
            triangle[me_c, s] = back_in[u, s].astype(F32)
            return _

        copy_c(
            back_u.at[me_z], back_other.at[u, me_z], sent_sem.at[6, u], other_sem.at[u, me_z]
        ).start()
        triangle[me_c, me_z] = back_u[me_z].astype(F32)
        lax.fori_loop(0, nz - 1, take_back, 0)

        def take_other(k, _):
            slot = back_other.at[u, k]
            copy_c(slot, slot, sent_sem.at[6, u], other_sem.at[u, k]).wait_recv()
            triangle[other_c, k] = back_other[u, k].astype(F32)
            return _

        lax.fori_loop(0, nz, take_other, 0)

        at = wide + 2 + u
        gain_out = jnp.concatenate([z_all[0, c, :, at : at + 1] for c in range(2)], axis=0)
        for i in reversed(range(geo.extra)):
            s = chunks[i]
            values = jnp.concatenate(
                [triangle[c, k, :, s] for c in range(2) for k in range(nz)], axis=0
            )
            tn = normed(values, gain_out)
            change = jnp.dot(out_weight_ref[u], tn, preferred_element_type=F32)
            value = z_all[u, me_c, :, s] + gate[:, s] * change
            if u == 0:
                z_all[1, me_c, :, s] = value
                z_piece(1, i).start()
            else:
                lane = lax.broadcasted_iota(jnp.int32, (half, LANES), 1)
                row = jnp.zeros((half, LANES), F32)
                for q in range(geo.pieces):
                    block = lane_block(value, q)
                    out_ref[i * geo.pieces + q] = block[:, : geo.cols]
                    low = geo.spare * q
                    moved = pltpu.roll(block, (low - geo.cols) % LANES, 1)
                    row = jnp.where((lane >= low) & (lane < low + geo.spare), moved, row)
                out_ref[geo.blocks + i] = row[:, : geo.cols]

    any_sem = z_sem.at[0, 0]
    for u in range(2):
        many = left_out.at[u, pl.ds(0, nz - 1)]
        copy_z(many, many, sent_sem.at[0, u], any_sem, me_z).wait_send()
        copy_z(many, many, sent_sem.at[1, u], any_sem, me_z).wait_send()
        copy_z(many, many, sent_sem.at[4, u], any_sem, me_z).wait_send()
        for k in range(1, nx):
            all_slots = left_out.at[u]
            copy_x(all_slots, all_slots, sent_sem.at[2, u], any_sem, me_x).wait_send()
        every = left_out.at[u]
        copy_c(every, every, sent_sem.at[6, u], any_sem).wait_send()
    away = left_out.at[0, pl.ds(0, nz - geo.near)]
    copy_x(away, away, sent_sem.at[3, 0], any_sem, me_x).wait_send()
    for u in range(2):
        part = z_all.at[u, me_c, :, : wide + (LANES if u == 0 else 0)]
        copy_c(part, part, sent_sem.at[5, u], any_sem).wait_send()


def per_device(
    geo, pair, residue_mask, norm_in_gain, proj_weight, gate_weight, norm_out_gain, out_weight
):
    half = pair.shape[0]
    full = 2 * half
    nz, nx = geo.nz, geo.nx
    vmem = pltpu.VMEM
    message = (2, geo.width)
    dma = pltpu.SemaphoreType.DMA
    hbm = pl.BlockSpec(memory_space=pl.ANY)
    pair = jnp.swapaxes(pair, 0, 1)
    proj_weight = jnp.swapaxes(proj_weight, 2, 3)
    gate_weight = jnp.swapaxes(gate_weight, 1, 2)
    out_weight = jnp.swapaxes(out_weight, 1, 2)
    result = pl.pallas_call(
        functools.partial(kernel, geo, half),
        out_shape=jax.ShapeDtypeStruct(pair.shape, F32),
        in_specs=[
            hbm,
            pl.BlockSpec(memory_space=pltpu.SMEM),
            hbm,
            hbm,
            hbm,
            hbm,
            hbm,
        ],
        out_specs=pl.BlockSpec(memory_space=vmem),
        scratch_shapes=[
            vmem(pair.shape, F32),
            vmem((2, *norm_in_gain.shape), F32),
            vmem(proj_weight.shape, BF16),
            vmem(gate_weight.shape, BF16),
            vmem(out_weight.shape, BF16),
            vmem((1, geo.width), F32),
            vmem((2, 2, half, geo.width + LANES), F32),
            vmem((full, geo.width), BF16),
            vmem((half, geo.width), F32),
            vmem((half, geo.width), F32),
            vmem((2, nz, *message), BF16),
            vmem((2, nz, *message), BF16),
            vmem((2, nx, nz, *message), BF16),
            vmem((2, nz, *message), BF16),
            vmem((nx, geo.near, *message), BF16),
            vmem((nx, 2, geo.res, LANES), F32),
            vmem((nx, 2, geo.res, LANES), F32),
            vmem((2, geo.res, LANES), F32),
            vmem((2, nz, *message), BF16),
            vmem((2, nz, *message), BF16),
            vmem((2, nz, *message), BF16),
            vmem((2, nz, *message), F32),
            dma((2, nx, nz)),
            dma((2, nz)),
            dma((nx, geo.near)),
            dma((2, nz)),
            dma((2, nz)),
            dma((2, geo.extra)),
            dma((7, 2)),
            dma((6,)),
            pltpu.SemaphoreType.REGULAR((nz // 2 + 1,)),
            pltpu.SemaphoreType.REGULAR((nz // 2 + 1,)),
        ],
        compiler_params=pltpu.CompilerParams(
            collective_id=0, has_side_effects=True, vmem_limit_bytes=60 * 1024 * 1024
        ),
        name="triangle_updates",
    )(
        pair,
        residue_mask,
        norm_in_gain,
        proj_weight,
        gate_weight,
        norm_out_gain,
        out_weight,
    )
    return jnp.swapaxes(result, 0, 1)


def solution(mesh):
    def body(pair, *rest):
        geo = Geometry(pair.shape[1], pair.shape[2], mesh.shape["gx"], mesh.shape["gy"])
        return per_device(geo, pair, *rest)

    return jax.shard_map(
        body,
        mesh=mesh,
        in_specs=(
            P(("groups", "gz"), "gx", "gy"),
            P("groups"),
            P(None, "gz"),
            P(None, None, None, "gz"),
            P(None, None, "gz"),
            P(None, "gz"),
            P(None, None, "gz"),
        ),
        out_specs=P(("groups", "gz"), "gx", "gy"),
        check_vma=False,
    )
```

```python
import functools

import jax
import jax.numpy as jnp
from jax import lax
from jax.experimental import pallas as pl
from jax.experimental.pallas import tpu as pltpu
from jax.sharding import PartitionSpec as P

EPSILON = 1e-05
LANES = 128
MESH = pl.DeviceIdType.MESH
F32 = jnp.float32
BF16 = jnp.bfloat16


class Geometry:
    def __init__(self, rows, cols, nz, nx):
        self.rows, self.cols, self.nz, self.nx = rows, cols, nz, nx
        self.spare = LANES - cols
        self.blocks = rows * cols // LANES
        self.extra = rows - self.blocks
        self.pieces = cols // self.spare
        self.width = self.blocks * LANES
        self.res = nz * rows
        self.near = cols // rows
        assert self.blocks * LANES == rows * cols
        assert self.extra * self.pieces == self.blocks
        assert nz * rows == nx * cols and self.near * rows == cols


def lane_block(v, k):
    return v[:, k * LANES : (k + 1) * LANES]


def rows_of(geo, v):
    lane = lax.broadcasted_iota(jnp.int32, (v.shape[0], LANES), 1)
    rows = [jnp.where(lane < geo.cols, lane_block(v, r), 0.0) for r in range(geo.blocks)]
    for e in range(geo.extra):
        row = jnp.zeros((v.shape[0], LANES), F32)
        for q in range(geo.pieces):
            low = geo.spare * q
            piece = pltpu.roll(lane_block(v, e * geo.pieces + q), (low - geo.cols) % LANES, 1)
            row = jnp.where((lane >= low) & (lane < low + geo.spare), piece, row)
        rows.append(row)
    return rows


def block_of(geo, get_row, k):
    row = get_row(k)
    lane = lax.broadcasted_iota(jnp.int32, row.shape, 1)
    extra, q = divmod(k, geo.pieces)
    piece = pltpu.roll(get_row(geo.blocks + extra), geo.cols - geo.spare * q, 1)
    return jnp.where(lane < geo.cols, row, piece)


def normed(values, gain):
    mean = jnp.mean(values, axis=0, keepdims=True)
    centred = values - mean
    spread = jnp.mean(centred * centred, axis=0, keepdims=True)
    return (centred * lax.rsqrt(spread + EPSILON) * gain).astype(BF16)


def kernel(
    geo,
    half,
    pair_hbm,
    flag_ref,
    gain_in_hbm,
    proj_hbm,
    gate_hbm,
    gain_out_hbm,
    out_hbm,
    out_ref,
    pair_ref,
    gains,
    proj_ref,
    gate_ref,
    out_weight_ref,
    mask_ref,
    z_all,
    zn,
    tmp,
    gate,
    left_out,
    right_out,
    left_all,
    right_in,
    right_all,
    left_mat,
    right_mat,
    product,
    back_out,
    back_in,
    back_other,
    triangle,
    left_sem,
    right_sem,
    right_x_sem,
    back_sem,
    other_sem,
    z_sem,
    sent_sem,
    load_sem,
    up_sem,
    down_sem,
):
    nz, nx = geo.nz, geo.nx
    me_z = lax.axis_index("gx")
    me_x = lax.axis_index("gy")
    me_c = lax.axis_index("gz")
    other_c = 1 - me_c
    chunk = geo.pieces * LANES
    chunks = [slice(k, k + chunk) for k in range(0, geo.width, chunk)]

    barrier = pltpu.get_barrier_semaphore()

    after = lax.rem(me_z + 1, nz)
    before = lax.rem(me_z + nz - 1, nz)
    for neighbour in (before, after):
        pl.semaphore_signal(barrier, inc=1, device_id={"gx": neighbour}, device_id_type=MESH)
    for k in range(1, nx):
        pl.semaphore_signal(
            barrier, inc=1, device_id={"gy": lax.rem(me_x + k, nx)}, device_id_type=MESH
        )
    pl.semaphore_signal(barrier, inc=1, device_id={"gz": other_c}, device_id_type=MESH)

    def far_first(k):
        m = (k + 1) // 2
        return lax.rem(me_z + nz // 2 + m * (1 - 2 * (k % 2)), nz)

    def copy_z(src, dst, send, recv, to):
        return pltpu.make_async_remote_copy(
            src_ref=src, dst_ref=dst, send_sem=send, recv_sem=recv, device_id={"gx": to}, device_id_type=MESH
        )

    def copy_x(src, dst, send, recv, to):
        return pltpu.make_async_remote_copy(
            src_ref=src, dst_ref=dst, send_sem=send, recv_sem=recv, device_id={"gy": to}, device_id_type=MESH
        )

    def copy_c(src, dst, send, recv):
        return pltpu.make_async_remote_copy(
            src_ref=src, dst_ref=dst, send_sem=send, recv_sem=recv, device_id={"gz": other_c}, device_id_type=MESH
        )

    def store_rows(mat, lead, base, value):
        for r, row in enumerate(rows_of(geo, value)):
            for h in range(2):
                mat[lead, h, pl.ds(base + r, 1), :] = row[h : h + 1, :]

    lag = 6
    wide = geo.width

    loads = [
        pltpu.make_async_copy(src, dst, load_sem.at[i])
        for i, (src, dst) in enumerate(
            [
                (pair_hbm, pair_ref),
                (gain_in_hbm, gains.at[0]),
                (gain_out_hbm, gains.at[1]),
                (proj_hbm, proj_ref),
                (gate_hbm, gate_ref),
                (out_hbm, out_weight_ref),
            ]
        )
    ]
    for load in loads:
        load.start()
    for load in loads[:3]:
        load.wait()
    for k in range(geo.blocks):
        e, q = divmod(k, geo.pieces)
        low = geo.spare * q
        z_all[0, me_c, :, k * LANES : (k + 1) * LANES] = jnp.concatenate(
            [pair_ref[k], pair_ref[geo.blocks + e, :, low : low + geo.spare]], axis=1
        )
    diagonal = lax.broadcasted_iota(jnp.int32, (half, half), 0) == lax.broadcasted_iota(
        jnp.int32, (half, half), 1
    )
    columns = [
        jnp.sum(jnp.where(diagonal, gains[kind, u : u + 1, :], 0.0), axis=1, keepdims=True)
        for kind in range(2)
        for u in range(2)
    ]
    lane = lax.broadcasted_iota(jnp.int32, (half, LANES), 1)
    last = jnp.zeros((half, LANES), F32)
    for i, column in enumerate(columns):
        last = jnp.where(lane == i, column, last)
    z_all[0, me_c, :, wide:] = last

    near_lane = lax.broadcasted_iota(jnp.int32, (1, LANES), 1)
    near_flags = jnp.zeros((1, LANES), F32)
    for t in range(geo.cols):
        flag = flag_ref[me_x * geo.cols + t].astype(F32)
        near_flags = jnp.where(near_lane == t, flag, near_flags)
    row_flag = [flag_ref[me_z * geo.rows + r].astype(F32) for r in range(geo.rows)]
    for k in range(geo.blocks):
        mask_ref[:, k * LANES : (k + 1) * LANES] = block_of(
            geo, lambda r: near_flags * row_flag[r], k
        )

    for load in loads[3:]:
        load.wait()

    pl.semaphore_wait(barrier, 2 + nx - 1 + 1)

    def z_piece(u, i):
        low = i * chunk
        high = low + chunk + (LANES if u == 0 and i == geo.extra - 1 else 0)
        part = z_all.at[u, me_c, :, low:high]
        return copy_c(part, part, sent_sem.at[5, u], z_sem.at[u, i])

    for i in reversed(range(geo.extra)):
        z_piece(0, i).start()

    middle = nz // 2
    place = before
    early = jnp.where(place >= middle, middle, jnp.where(place == 0, middle - 1, place))
    later = jnp.where(place < middle, middle, nz - 1 - place)
    up_limit = jnp.where(me_z >= middle, middle, middle - 1)
    down_limit = jnp.where(lax.rem(place + nz - 1, nz) < middle, middle, middle - 1)
    below = place < middle
    at_end = later <= 4

    def hear_up(j):
        @pl.when(j > 1)
        def run():
            pl.semaphore_wait(up_sem.at[j], 1)

        @pl.when(j < up_limit)
        def relay():
            pl.semaphore_signal(up_sem.at[j + 1], inc=1, device_id={"gx": after}, device_id_type=MESH)

    def hear_down(j):
        @pl.when(j > 1)
        def run():
            pl.semaphore_wait(down_sem.at[j], 1)

        @pl.when(j < down_limit)
        def relay():
            pl.semaphore_signal(
                down_sem.at[j + 1], inc=1, device_id={"gx": before}, device_id_type=MESH
            )

    def hear_early(j, _):
        hear_up(j)
        return _

    def hear_later(j, _):
        hear_down(j)
        return _

    lax.fori_loop(1, early + 1, hear_early, 0)
    lax.fori_loop(1, jnp.where(at_end, later + 1, 1), hear_later, 0)

    def by_word(n):
        crossed = n - early - later
        s = jnp.where(
            n < early,
            me_z - 1 - n,
            jnp.where(
                n < early + later,
                me_z + 1 + n - early,
                jnp.where(below, me_z - early - 1 - crossed, me_z + later + 1 + crossed),
            ),
        )
        return jnp.where(n == nz - 1, me_z, lax.rem(s + nz, nz))

    for u in range(2):
        left_u, right_u, back_u = left_out.at[u], right_out.at[u], back_out.at[u]

        for i in reversed(range(geo.extra)):
            z_piece(u, i).wait_recv()
            s = chunks[i]
            if i == geo.extra - 1:
                gain_in = jnp.concatenate(
                    [z_all[0, c, :, wide + u : wide + u + 1] for c in range(2)], axis=0
                )
            z = jnp.concatenate([z_all[u, 0, :, s], z_all[u, 1, :, s]], axis=0)
            zn[:, s] = normed(z, gain_in)

        def project(first, out):
            for s in chunks:
                opening, value = (
                    jnp.dot(proj_ref[u, first + i], zn[:, s], preferred_element_type=F32)
                    for i in range(2)
                )
                tmp[:, s] = jax.nn.sigmoid(opening) * value * mask_ref[:, s]
            for k in range(nz):
                out[k] = tmp[2 * k : 2 * k + 2, :].astype(BF16)

        def forward_left(src, s):
            for k in range(1, nx):
                copy_x(
                    src,
                    left_all.at[u, me_x, s],
                    sent_sem.at[2, u],
                    left_sem.at[u, me_x, s],
                    lax.rem(me_x + k, nx),
                ).start()

        def forward_right(src, s):
            target = s // geo.near

            @pl.when(target != me_x)
            def run():
                copy_x(
                    src,
                    right_all.at[me_x, s % geo.near],
                    sent_sem.at[3, 0],
                    right_x_sem.at[me_x, s % geo.near],
                    target,
                ).start()

        def send_left(to):
            copy_z(
                left_u.at[to],
                left_all.at[u, me_x, me_z],
                sent_sem.at[0, u],
                left_sem.at[u, me_x, me_z],
                to,
            ).start()

        def send_right(to):
            copy_z(
                right_u.at[to],
                right_in.at[u, me_z],
                sent_sem.at[1, u],
                right_sem.at[u, me_z],
                to,
            ).start()

        def open_gate():
            for s in chunks:
                gate[:, s] = jax.nn.sigmoid(
                    jnp.dot(gate_ref[u], zn[:, s], preferred_element_type=F32)
                )

        source = by_word if u == 0 else far_first

        def take_left(k):
            s = source(k)
            slot = left_all.at[u, me_x, s]

            @pl.when(k < nz - 1)
            def run():
                copy_z(slot, slot, sent_sem.at[0, u], left_sem.at[u, me_x, s], s).wait_recv()
                forward_left(slot, s)

            store_rows(left_mat, me_x, s * geo.rows, left_all[u, me_x, s].astype(F32))

        def take_left_x(k):
            s = source(k)
            for d in range(1, nx):
                x = lax.rem(me_x + d, nx)
                slot = left_all.at[u, x, s]
                copy_x(slot, slot, sent_sem.at[2, u], left_sem.at[u, x, s], x).wait_recv()
                store_rows(left_mat, x, s * geo.rows, left_all[u, x, s].astype(F32))

        def wait_right(k, s):
            slot = right_in.at[u, s]

            @pl.when(k < nz - 1)
            def run():
                copy_z(slot, slot, sent_sem.at[1, u], right_sem.at[u, s], s).wait_recv()

        def block_row(base, r):
            return jnp.concatenate([product[h, pl.ds(base + r, 1), :] for h in range(2)], axis=0)

        def send_back(k):
            to = far_first(k)
            base = to * geo.rows
            for b in range(geo.blocks):
                value = block_of(geo, functools.partial(block_row, base), b)
                back_u[to, :, b * LANES : (b + 1) * LANES] = value.astype(BF16)

            @pl.when(k < nz - 1)
            def run():
                copy_z(
                    back_u.at[to], back_in.at[u, me_z], sent_sem.at[4, u], back_sem.at[u, me_z], to
                ).start()

        def take_right_x(k):
            s = source(k)
            at = s % geo.near

            @pl.when(s // geo.near == me_x)
            def run():
                for d in range(1, nx):
                    x = lax.rem(me_x + d, nx)
                    slot = right_all.at[x, at]
                    copy_x(slot, slot, sent_sem.at[3, 0], right_x_sem.at[x, at], x).wait_recv()
                    store_rows(right_mat, x, at * geo.rows, right_all[x, at].astype(F32))

        project(0, left_u)
        forward_left(left_u.at[me_z], me_z)
        left_all[u, me_x, me_z] = left_u[me_z]
        if u == 0:
            project(2, right_u)
            forward_right(right_u.at[me_z], me_z)
            right_in[u, me_z] = right_u[me_z]

            def send_both(to):
                to = lax.rem(to + nz, nz)
                send_left(to)
                send_right(to)

            def take_both(k, _):
                s = source(k)
                take_left(k)
                wait_right(k, s)

                @pl.when(k < nz - 1)
                def run():
                    forward_right(right_in.at[0, s], s)

                @pl.when(s // geo.near == me_x)
                def run_own():
                    store_rows(
                        right_mat, me_x, (s % geo.near) * geo.rows, right_in[0, s].astype(F32)
                    )

                @pl.when(k >= lag)
                def run_x():
                    take_left_x(k - lag)
                    take_right_x(k - lag)

                return _

            def send_early(n, _):
                send_both(me_z - early + n)
                return _

            between = jnp.maximum(jnp.minimum(later, early) - 2, 0) * jnp.minimum(place, 1)

            def send_later(j, _):
                @pl.when(jnp.logical_not(at_end))
                def run():
                    hear_down(j)

                send_both(me_z + j)

                @pl.when((j > 2) & (j - 3 < between))
                def run_take():
                    take_both(j - 3, 0)

                return _

            def send_down(j, _):
                hear_down(j)
                send_both(me_z + j)
                return _

            def send_up(j, _):
                hear_up(j)
                send_both(me_z - j)
                return _

            lax.fori_loop(0, early, send_early, 0)
            open_gate()
            lax.fori_loop(1, later + 1, send_later, 0)
            lax.fori_loop(jnp.where(below, early + 1, middle), middle, send_up, 0)
            lax.fori_loop(jnp.where(below, middle, later + 1), middle, send_down, 0)
            lax.fori_loop(between, nz, take_both, 0)
        else:

            def send_lefts(k, _):
                send_left(far_first(k))
                return _

            def send_rights(k, _):
                send_right(far_first(k))
                return _

            lax.fori_loop(0, nz - 1, send_lefts, 0)
            project(2, right_u)
            lax.fori_loop(0, nz - 1, send_rights, 0)
            right_in[u, me_z] = right_u[me_z]
            open_gate()

            def take_lefts(k, _):
                take_left(k)

                @pl.when(k >= lag)
                def run():
                    take_left_x(k - lag)

                return _

            lax.fori_loop(0, nz, take_lefts, 0)

            def take_rights(k, _):
                s = source(k)
                wait_right(k, s)
                store_rows(right_mat, 0, s * geo.rows, right_in[1, s].astype(F32))

                @pl.when(k < lag)
                def run_left():
                    take_left_x(nz - lag + k)

                return _

            lax.fori_loop(0, nz, take_rights, 0)

        if u == 0:

            def take_last(k, _):
                take_left_x(k)
                take_right_x(k)
                return _

            lax.fori_loop(nz - lag, nz, take_last, 0)

            for h in range(2):
                total = jnp.zeros((geo.res, geo.cols), F32)
                for x in range(nx):
                    total += lax.dot_general(
                        left_mat[x, h].astype(BF16),
                        right_mat[x, h, : geo.cols, :].astype(BF16),
                        (((1,), (1,)), ((), ())),
                        preferred_element_type=F32,
                    )
                product[h, :, : geo.cols] = total
        else:
            for h in range(2):
                right = right_mat[0, h].astype(BF16)
                for x in range(nx):
                    part = lax.dot_general(
                        left_mat[x, h].astype(BF16),
                        right,
                        (((0,), (0,)), ((), ())),
                        preferred_element_type=F32,
                    )
                    product[h, geo.cols * x : geo.cols * (x + 1), :] = part[: geo.cols, :]

        def send(k, _):
            send_back(k)
            return _

        lax.fori_loop(0, nz, send, 0)

        def take_back(k, _):
            s = far_first(k)
            slot = back_in.at[u, s]
            copy_z(slot, slot, sent_sem.at[4, u], back_sem.at[u, s], s).wait_recv()
            copy_c(slot, back_other.at[u, s], sent_sem.at[6, u], other_sem.at[u, s]).start()
            triangle[me_c, s] = back_in[u, s].astype(F32)
            return _

        copy_c(
            back_u.at[me_z], back_other.at[u, me_z], sent_sem.at[6, u], other_sem.at[u, me_z]
        ).start()
        triangle[me_c, me_z] = back_u[me_z].astype(F32)
        lax.fori_loop(0, nz - 1, take_back, 0)

        def take_other(k, _):
            slot = back_other.at[u, k]
            copy_c(slot, slot, sent_sem.at[6, u], other_sem.at[u, k]).wait_recv()
            triangle[other_c, k] = back_other[u, k].astype(F32)
            return _

        lax.fori_loop(0, nz, take_other, 0)

        at = wide + 2 + u
        gain_out = jnp.concatenate([z_all[0, c, :, at : at + 1] for c in range(2)], axis=0)
        for i in reversed(range(geo.extra)):
            s = chunks[i]
            values = jnp.concatenate(
                [triangle[c, k, :, s] for c in range(2) for k in range(nz)], axis=0
            )
            tn = normed(values, gain_out)
            change = jnp.dot(out_weight_ref[u], tn, preferred_element_type=F32)
            value = z_all[u, me_c, :, s] + gate[:, s] * change
            if u == 0:
                z_all[1, me_c, :, s] = value
                z_piece(1, i).start()
            else:
                lane = lax.broadcasted_iota(jnp.int32, (half, LANES), 1)
                row = jnp.zeros((half, LANES), F32)
                for q in range(geo.pieces):
                    block = lane_block(value, q)
                    out_ref[i * geo.pieces + q] = block[:, : geo.cols]
                    low = geo.spare * q
                    moved = pltpu.roll(block, (low - geo.cols) % LANES, 1)
                    row = jnp.where((lane >= low) & (lane < low + geo.spare), moved, row)
                out_ref[geo.blocks + i] = row[:, : geo.cols]

    any_sem = z_sem.at[0, 0]
    for u in range(2):
        many = left_out.at[u, pl.ds(0, nz - 1)]
        copy_z(many, many, sent_sem.at[0, u], any_sem, me_z).wait_send()
        copy_z(many, many, sent_sem.at[1, u], any_sem, me_z).wait_send()
        copy_z(many, many, sent_sem.at[4, u], any_sem, me_z).wait_send()
        for k in range(1, nx):
            all_slots = left_out.at[u]
            copy_x(all_slots, all_slots, sent_sem.at[2, u], any_sem, me_x).wait_send()
        every = left_out.at[u]
        copy_c(every, every, sent_sem.at[6, u], any_sem).wait_send()
    away = left_out.at[0, pl.ds(0, nz - geo.near)]
    copy_x(away, away, sent_sem.at[3, 0], any_sem, me_x).wait_send()
    for u in range(2):
        part = z_all.at[u, me_c, :, : wide + (LANES if u == 0 else 0)]
        copy_c(part, part, sent_sem.at[5, u], any_sem).wait_send()


def per_device(
    geo, pair, residue_mask, norm_in_gain, proj_weight, gate_weight, norm_out_gain, out_weight
):
    half = pair.shape[0]
    full = 2 * half
    nz, nx = geo.nz, geo.nx
    vmem = pltpu.VMEM
    message = (2, geo.width)
    dma = pltpu.SemaphoreType.DMA
    hbm = pl.BlockSpec(memory_space=pl.ANY)
    pair = jnp.swapaxes(pair, 0, 1)
    proj_weight = jnp.swapaxes(proj_weight, 2, 3)
    gate_weight = jnp.swapaxes(gate_weight, 1, 2)
    out_weight = jnp.swapaxes(out_weight, 1, 2)
    result = pl.pallas_call(
        functools.partial(kernel, geo, half),
        out_shape=jax.ShapeDtypeStruct(pair.shape, F32),
        in_specs=[
            hbm,
            pl.BlockSpec(memory_space=pltpu.SMEM),
            hbm,
            hbm,
            hbm,
            hbm,
            hbm,
        ],
        out_specs=pl.BlockSpec(memory_space=vmem),
        scratch_shapes=[
            vmem(pair.shape, F32),
            vmem((2, *norm_in_gain.shape), F32),
            vmem(proj_weight.shape, BF16),
            vmem(gate_weight.shape, BF16),
            vmem(out_weight.shape, BF16),
            vmem((1, geo.width), F32),
            vmem((2, 2, half, geo.width + LANES), F32),
            vmem((full, geo.width), BF16),
            vmem((half, geo.width), F32),
            vmem((half, geo.width), F32),
            vmem((2, nz, *message), BF16),
            vmem((2, nz, *message), BF16),
            vmem((2, nx, nz, *message), BF16),
            vmem((2, nz, *message), BF16),
            vmem((nx, geo.near, *message), BF16),
            vmem((nx, 2, geo.res, LANES), F32),
            vmem((nx, 2, geo.res, LANES), F32),
            vmem((2, geo.res, LANES), F32),
            vmem((2, nz, *message), BF16),
            vmem((2, nz, *message), BF16),
            vmem((2, nz, *message), BF16),
            vmem((2, nz, *message), F32),
            dma((2, nx, nz)),
            dma((2, nz)),
            dma((nx, geo.near)),
            dma((2, nz)),
            dma((2, nz)),
            dma((2, geo.extra)),
            dma((7, 2)),
            dma((6,)),
            pltpu.SemaphoreType.REGULAR((nz // 2 + 1,)),
            pltpu.SemaphoreType.REGULAR((nz // 2 + 1,)),
        ],
        compiler_params=pltpu.CompilerParams(
            collective_id=0, has_side_effects=True, vmem_limit_bytes=60 * 1024 * 1024
        ),
        name="triangle_updates",
    )(
        pair,
        residue_mask,
        norm_in_gain,
        proj_weight,
        gate_weight,
        norm_out_gain,
        out_weight,
    )
    return jnp.swapaxes(result, 0, 1)


def solution(mesh):
    def body(pair, *rest):
        geo = Geometry(pair.shape[1], pair.shape[2], mesh.shape["gx"], mesh.shape["gy"])
        return per_device(geo, pair, *rest)

    return jax.shard_map(
        body,
        mesh=mesh,
        in_specs=(
            P(("groups", "gz"), "gx", "gy"),
            P("groups"),
            P(None, "gz"),
            P(None, None, None, "gz"),
            P(None, None, "gz"),
            P(None, "gz"),
            P(None, None, "gz"),
        ),
        out_specs=P(("groups", "gz"), "gx", "gy"),
        check_vma=False,
    )
```

```python
import functools

import jax
import jax.numpy as jnp
from jax import lax
from jax.experimental import pallas as pl
from jax.experimental.pallas import tpu as pltpu
from jax.sharding import PartitionSpec as P

EPSILON = 1e-05
LANES = 128
MESH = pl.DeviceIdType.MESH
F32 = jnp.float32
BF16 = jnp.bfloat16


class Geometry:
    def __init__(self, rows, cols, nz, nx):
        self.rows, self.cols, self.nz, self.nx = rows, cols, nz, nx
        self.spare = LANES - cols
        self.blocks = rows * cols // LANES
        self.extra = rows - self.blocks
        self.pieces = cols // self.spare
        self.width = self.blocks * LANES
        self.res = nz * rows
        self.near = cols // rows
        assert self.blocks * LANES == rows * cols
        assert self.extra * self.pieces == self.blocks and nz % 4 == 0
        assert nz * rows == nx * cols and self.near * rows == cols


def lane_block(v, k):
    return v[:, k * LANES : (k + 1) * LANES]


def rows_of(geo, v):
    lane = lax.broadcasted_iota(jnp.int32, (v.shape[0], LANES), 1)
    rows = [jnp.where(lane < geo.cols, lane_block(v, r), 0.0) for r in range(geo.blocks)]
    for e in range(geo.extra):
        row = jnp.zeros((v.shape[0], LANES), F32)
        for q in range(geo.pieces):
            low = geo.spare * q
            piece = pltpu.roll(lane_block(v, e * geo.pieces + q), (low - geo.cols) % LANES, 1)
            row = jnp.where((lane >= low) & (lane < low + geo.spare), piece, row)
        rows.append(row)
    return rows


def block_of(geo, get_row, k):
    row = get_row(k)
    lane = lax.broadcasted_iota(jnp.int32, row.shape, 1)
    extra, q = divmod(k, geo.pieces)
    piece = pltpu.roll(get_row(geo.blocks + extra), geo.cols - geo.spare * q, 1)
    return jnp.where(lane < geo.cols, row, piece)


def normed(values, gain):
    mean = jnp.mean(values, axis=0, keepdims=True)
    centred = values - mean
    spread = jnp.mean(centred * centred, axis=0, keepdims=True)
    return (centred * lax.rsqrt(spread + EPSILON) * gain).astype(BF16)


def kernel(
    geo,
    half,
    pair_hbm,
    flag_ref,
    gain_in_hbm,
    proj_hbm,
    gate_hbm,
    gain_out_hbm,
    out_hbm,
    out_ref,
    pair_ref,
    gains,
    proj_ref,
    gate_ref,
    out_weight_ref,
    mask_ref,
    z_all,
    zn,
    tmp,
    gate,
    left_out,
    right_out,
    left_all,
    right_in,
    right_all,
    left_mat,
    right_mat,
    product,
    back_out,
    back_in,
    back_other,
    triangle,
    left_sem,
    right_sem,
    right_x_sem,
    back_sem,
    other_sem,
    z_sem,
    sent_sem,
    load_sem,
):
    nz, nx = geo.nz, geo.nx
    me_z = lax.axis_index("gx")
    me_x = lax.axis_index("gy")
    me_c = lax.axis_index("gz")
    other_c = 1 - me_c
    chunk = geo.pieces * LANES
    chunks = [slice(k, k + chunk) for k in range(0, geo.width, chunk)]

    barrier = pltpu.get_barrier_semaphore()

    def signal_z(k, _):
        pl.semaphore_signal(
            barrier, inc=1, device_id={"gx": lax.rem(me_z + 1 + k, nz)}, device_id_type=MESH
        )
        return _

    lax.fori_loop(0, nz - 1, signal_z, 0)
    for k in range(1, nx):
        pl.semaphore_signal(
            barrier, inc=1, device_id={"gy": lax.rem(me_x + k, nx)}, device_id_type=MESH
        )
    pl.semaphore_signal(barrier, inc=1, device_id={"gz": other_c}, device_id_type=MESH)

    def far_first(k):
        m = (k + 1) // 2
        return lax.rem(me_z + nz // 2 + m * (1 - 2 * (k % 2)), nz)

    def team(k):
        return (k + 3) // 4

    def wait_team(k, copy_of, last):
        @pl.when(k == 0)
        def run_first():
            copy_of(left_out.at[0, pl.ds(0, 1)]).wait_recv()

        @pl.when((k % 4 == 1) & (k < nz - 3))
        def run_full():
            copy_of(left_out.at[0, pl.ds(0, 4)]).wait_recv()

        @pl.when(k == nz - 3)
        def run_last():
            copy_of(left_out.at[0, pl.ds(0, last)]).wait_recv()

    def copy_z(src, dst, send, recv, to):
        return pltpu.make_async_remote_copy(
            src_ref=src, dst_ref=dst, send_sem=send, recv_sem=recv, device_id={"gx": to}, device_id_type=MESH
        )

    def copy_x(src, dst, send, recv, to):
        return pltpu.make_async_remote_copy(
            src_ref=src, dst_ref=dst, send_sem=send, recv_sem=recv, device_id={"gy": to}, device_id_type=MESH
        )

    def copy_c(src, dst, send, recv):
        return pltpu.make_async_remote_copy(
            src_ref=src, dst_ref=dst, send_sem=send, recv_sem=recv, device_id={"gz": other_c}, device_id_type=MESH
        )

    def store_rows(mat, lead, base, value):
        for r, row in enumerate(rows_of(geo, value)):
            for h in range(2):
                mat[lead, h, pl.ds(base + r, 1), :] = row[h : h + 1, :]

    lag = 8
    wide = geo.width

    loads = [
        pltpu.make_async_copy(src, dst, load_sem.at[i])
        for i, (src, dst) in enumerate(
            [
                (pair_hbm, pair_ref),
                (gain_in_hbm, gains.at[0]),
                (gain_out_hbm, gains.at[1]),
                (proj_hbm, proj_ref),
                (gate_hbm, gate_ref),
                (out_hbm, out_weight_ref),
            ]
        )
    ]
    for load in loads:
        load.start()
    for load in loads[:3]:
        load.wait()
    for k in range(geo.blocks):
        e, q = divmod(k, geo.pieces)
        low = geo.spare * q
        z_all[0, me_c, :, k * LANES : (k + 1) * LANES] = jnp.concatenate(
            [pair_ref[k], pair_ref[geo.blocks + e, :, low : low + geo.spare]], axis=1
        )
    diagonal = lax.broadcasted_iota(jnp.int32, (half, half), 0) == lax.broadcasted_iota(
        jnp.int32, (half, half), 1
    )
    columns = [
        jnp.sum(jnp.where(diagonal, gains[kind, u : u + 1, :], 0.0), axis=1, keepdims=True)
        for kind in range(2)
        for u in range(2)
    ]
    lane = lax.broadcasted_iota(jnp.int32, (half, LANES), 1)
    last = jnp.zeros((half, LANES), F32)
    for i, column in enumerate(columns):
        last = jnp.where(lane == i, column, last)
    z_all[0, me_c, :, wide:] = last

    near_lane = lax.broadcasted_iota(jnp.int32, (1, LANES), 1)
    near_flags = jnp.zeros((1, LANES), F32)
    for t in range(geo.cols):
        flag = flag_ref[me_x * geo.cols + t].astype(F32)
        near_flags = jnp.where(near_lane == t, flag, near_flags)
    row_flag = [flag_ref[me_z * geo.rows + r].astype(F32) for r in range(geo.rows)]
    for k in range(geo.blocks):
        mask_ref[:, k * LANES : (k + 1) * LANES] = block_of(
            geo, lambda r: near_flags * row_flag[r], k
        )

    for load in loads[3:]:
        load.wait()

    pl.semaphore_wait(barrier, nz - 1 + nx - 1 + 1)

    def z_piece(u, i):
        low = i * chunk
        high = low + chunk + (LANES if u == 0 and i == geo.extra - 1 else 0)
        part = z_all.at[u, me_c, :, low:high]
        return copy_c(part, part, sent_sem.at[5, u], z_sem.at[u, i])

    for i in reversed(range(geo.extra)):
        z_piece(0, i).start()

    for u in range(2):
        left_u, right_u, back_u = left_out.at[u], right_out.at[u], back_out.at[u]

        for i in reversed(range(geo.extra)):
            z_piece(u, i).wait_recv()
            s = chunks[i]
            if i == geo.extra - 1:
                gain_in = jnp.concatenate(
                    [z_all[0, c, :, wide + u : wide + u + 1] for c in range(2)], axis=0
                )
            z = jnp.concatenate([z_all[u, 0, :, s], z_all[u, 1, :, s]], axis=0)
            zn[:, s] = normed(z, gain_in)

        def project(first, out):
            for s in chunks:
                opening, value = (
                    jnp.dot(proj_ref[u, first + i], zn[:, s], preferred_element_type=F32)
                    for i in range(2)
                )
                tmp[:, s] = jax.nn.sigmoid(opening) * value * mask_ref[:, s]
            for k in range(nz):
                out[k] = tmp[2 * k : 2 * k + 2, :].astype(BF16)

        def forward_left(src, s, k):
            for d in range(1, nx):
                copy_x(
                    src,
                    left_all.at[u, me_x, s],
                    sent_sem.at[2, u],
                    left_sem.at[u, me_x, team(k)],
                    lax.rem(me_x + d, nx),
                ).start()

        def forward_right(src, s):
            target = s // geo.near

            @pl.when(target != me_x)
            def run():
                copy_x(
                    src,
                    right_all.at[me_x, s % geo.near],
                    sent_sem.at[3, 0],
                    right_x_sem.at[me_x, s % geo.near],
                    target,
                ).start()

        def send_left():
            def send(k, _):
                to = far_first(k)
                copy_z(
                    left_u.at[to],
                    left_all.at[u, me_x, me_z],
                    sent_sem.at[0, u],
                    left_sem.at[u, me_x, team(k)],
                    to,
                ).start()
                return _

            lax.fori_loop(0, nz - 1, send, 0)
            forward_left(left_u.at[me_z], me_z, nz - 1)
            left_all[u, me_x, me_z] = left_u[me_z]

        def send_right():
            def send(k, _):
                to = far_first(k)
                copy_z(
                    right_u.at[to],
                    right_in.at[u, me_z],
                    sent_sem.at[1, u],
                    right_sem.at[u, team(k)],
                    to,
                ).start()
                return _

            lax.fori_loop(0, nz - 1, send, 0)
            right_in[u, me_z] = right_u[me_z]

        def open_gate():
            for s in chunks:
                gate[:, s] = jax.nn.sigmoid(
                    jnp.dot(gate_ref[u], zn[:, s], preferred_element_type=F32)
                )

        def take_left(k):
            s = far_first(k)
            slot = left_all.at[u, me_x, s]

            wait_team(
                k,
                lambda ref: copy_z(ref, ref, sent_sem.at[0, u], left_sem.at[u, me_x, team(k)], s),
                2,
            )

            @pl.when(k < nz - 1)
            def run():
                forward_left(slot, s, k)

            store_rows(left_mat, me_x, s * geo.rows, left_all[u, me_x, s].astype(F32))

        def take_left_x(k):
            s = far_first(k)
            for d in range(1, nx):
                x = lax.rem(me_x + d, nx)
                wait_team(
                    k,
                    lambda ref: copy_x(ref, ref, sent_sem.at[2, u], left_sem.at[u, x, team(k)], x),
                    3,
                )
                store_rows(left_mat, x, s * geo.rows, left_all[u, x, s].astype(F32))

        def wait_right(k, s):
            wait_team(
                k, lambda ref: copy_z(ref, ref, sent_sem.at[1, u], right_sem.at[u, team(k)], s), 2
            )

        def block_row(base, r):
            return jnp.concatenate([product[h, pl.ds(base + r, 1), :] for h in range(2)], axis=0)

        def send_back(k):
            to = far_first(k)
            base = to * geo.rows
            for b in range(geo.blocks):
                value = block_of(geo, functools.partial(block_row, base), b)
                back_u[to, :, b * LANES : (b + 1) * LANES] = value.astype(BF16)

            @pl.when(k < nz - 1)
            def run():
                copy_z(
                    back_u.at[to], back_in.at[u, me_z], sent_sem.at[4, u], back_sem.at[u, team(k)], to
                ).start()

        project(0, left_u)
        send_left()
        project(2, right_u)
        send_right()
        if u == 0:
            forward_right(right_u.at[me_z], me_z)
        open_gate()

        def take_lefts(k, _):
            take_left(k)

            @pl.when(k >= lag)
            def run():
                take_left_x(k - lag)

            return _

        lax.fori_loop(0, nz, take_lefts, 0)

        def take_right_x(k):
            s = far_first(k)
            at = s % geo.near

            @pl.when(s // geo.near == me_x)
            def run():
                for d in range(1, nx):
                    x = lax.rem(me_x + d, nx)
                    slot = right_all.at[x, at]
                    copy_x(slot, slot, sent_sem.at[3, 0], right_x_sem.at[x, at], x).wait_recv()
                    store_rows(right_mat, x, at * geo.rows, right_all[x, at].astype(F32))

        def take_right(k, _):
            s = far_first(k)
            wait_right(k, s)
            if u == 0:

                @pl.when(k < nz - 1)
                def run():
                    forward_right(right_in.at[0, s], s)

                @pl.when(s // geo.near == me_x)
                def run_own():
                    store_rows(
                        right_mat, me_x, (s % geo.near) * geo.rows, right_in[0, s].astype(F32)
                    )

                @pl.when(k >= lag)
                def run_x():
                    take_right_x(k - lag)

            else:
                store_rows(right_mat, 0, s * geo.rows, right_in[1, s].astype(F32))

            @pl.when(k < lag)
            def run_left():
                take_left_x(nz - lag + k)

            return _

        lax.fori_loop(0, nz, take_right, 0)

        if u == 0:

            def take_last(k, _):
                take_right_x(k)
                return _

            lax.fori_loop(nz - lag, nz, take_last, 0)

            for h in range(2):
                total = jnp.zeros((geo.res, geo.cols), F32)
                for x in range(nx):
                    total += lax.dot_general(
                        left_mat[x, h].astype(BF16),
                        right_mat[x, h, : geo.cols, :].astype(BF16),
                        (((1,), (1,)), ((), ())),
                        preferred_element_type=F32,
                    )
                product[h, :, : geo.cols] = total
        else:
            for h in range(2):
                right = right_mat[0, h].astype(BF16)
                for x in range(nx):
                    part = lax.dot_general(
                        left_mat[x, h].astype(BF16),
                        right,
                        (((0,), (0,)), ((), ())),
                        preferred_element_type=F32,
                    )
                    product[h, geo.cols * x : geo.cols * (x + 1), :] = part[: geo.cols, :]

        def send(k, _):
            send_back(k)
            return _

        lax.fori_loop(0, nz, send, 0)

        def take_back(k, _):
            s = far_first(k)
            slot = back_in.at[u, s]
            wait_team(
                k, lambda ref: copy_z(ref, ref, sent_sem.at[4, u], back_sem.at[u, team(k)], s), 2
            )
            copy_c(slot, back_other.at[u, s], sent_sem.at[6, u], other_sem.at[u, team(k)]).start()
            triangle[me_c, s] = back_in[u, s].astype(F32)
            return _

        copy_c(
            back_u.at[me_z], back_other.at[u, me_z], sent_sem.at[6, u], other_sem.at[u, team(nz - 1)]
        ).start()
        triangle[me_c, me_z] = back_u[me_z].astype(F32)
        lax.fori_loop(0, nz - 1, take_back, 0)

        def take_other(k, _):
            s = far_first(k)
            wait_team(k, lambda ref: copy_c(ref, ref, sent_sem.at[6, u], other_sem.at[u, team(k)]), 3)
            triangle[other_c, s] = back_other[u, s].astype(F32)
            return _

        lax.fori_loop(0, nz, take_other, 0)

        at = wide + 2 + u
        gain_out = jnp.concatenate([z_all[0, c, :, at : at + 1] for c in range(2)], axis=0)
        for i in reversed(range(geo.extra)):
            s = chunks[i]
            values = jnp.concatenate(
                [triangle[c, k, :, s] for c in range(2) for k in range(nz)], axis=0
            )
            tn = normed(values, gain_out)
            change = jnp.dot(out_weight_ref[u], tn, preferred_element_type=F32)
            value = z_all[u, me_c, :, s] + gate[:, s] * change
            if u == 0:
                z_all[1, me_c, :, s] = value
                z_piece(1, i).start()
            else:
                lane = lax.broadcasted_iota(jnp.int32, (half, LANES), 1)
                row = jnp.zeros((half, LANES), F32)
                for q in range(geo.pieces):
                    block = lane_block(value, q)
                    out_ref[i * geo.pieces + q] = block[:, : geo.cols]
                    low = geo.spare * q
                    moved = pltpu.roll(block, (low - geo.cols) % LANES, 1)
                    row = jnp.where((lane >= low) & (lane < low + geo.spare), moved, row)
                out_ref[geo.blocks + i] = row[:, : geo.cols]

    any_sem = z_sem.at[0, 0]
    for u in range(2):
        many = left_out.at[u, pl.ds(0, nz - 1)]
        copy_z(many, many, sent_sem.at[0, u], any_sem, me_z).wait_send()
        copy_z(many, many, sent_sem.at[1, u], any_sem, me_z).wait_send()
        copy_z(many, many, sent_sem.at[4, u], any_sem, me_z).wait_send()
        for k in range(1, nx):
            all_slots = left_out.at[u]
            copy_x(all_slots, all_slots, sent_sem.at[2, u], any_sem, me_x).wait_send()
        every = left_out.at[u]
        copy_c(every, every, sent_sem.at[6, u], any_sem).wait_send()
    away = left_out.at[0, pl.ds(0, nz - geo.near)]
    copy_x(away, away, sent_sem.at[3, 0], any_sem, me_x).wait_send()
    for u in range(2):
        part = z_all.at[u, me_c, :, : wide + (LANES if u == 0 else 0)]
        copy_c(part, part, sent_sem.at[5, u], any_sem).wait_send()


def per_device(
    geo, pair, residue_mask, norm_in_gain, proj_weight, gate_weight, norm_out_gain, out_weight
):
    half = pair.shape[0]
    full = 2 * half
    nz, nx = geo.nz, geo.nx
    vmem = pltpu.VMEM
    message = (2, geo.width)
    dma = pltpu.SemaphoreType.DMA
    hbm = pl.BlockSpec(memory_space=pl.ANY)
    pair = jnp.swapaxes(pair, 0, 1)
    proj_weight = jnp.swapaxes(proj_weight, 2, 3)
    gate_weight = jnp.swapaxes(gate_weight, 1, 2)
    out_weight = jnp.swapaxes(out_weight, 1, 2)
    result = pl.pallas_call(
        functools.partial(kernel, geo, half),
        out_shape=jax.ShapeDtypeStruct(pair.shape, F32),
        in_specs=[
            hbm,
            pl.BlockSpec(memory_space=pltpu.SMEM),
            hbm,
            hbm,
            hbm,
            hbm,
            hbm,
        ],
        out_specs=pl.BlockSpec(memory_space=vmem),
        scratch_shapes=[
            vmem(pair.shape, F32),
            vmem((2, *norm_in_gain.shape), F32),
            vmem(proj_weight.shape, BF16),
            vmem(gate_weight.shape, BF16),
            vmem(out_weight.shape, BF16),
            vmem((1, geo.width), F32),
            vmem((2, 2, half, geo.width + LANES), F32),
            vmem((full, geo.width), BF16),
            vmem((half, geo.width), F32),
            vmem((half, geo.width), F32),
            vmem((2, nz, *message), BF16),
            vmem((2, nz, *message), BF16),
            vmem((2, nx, nz, *message), BF16),
            vmem((2, nz, *message), BF16),
            vmem((nx, geo.near, *message), BF16),
            vmem((nx, 2, geo.res, LANES), F32),
            vmem((nx, 2, geo.res, LANES), F32),
            vmem((2, geo.res, LANES), F32),
            vmem((2, nz, *message), BF16),
            vmem((2, nz, *message), BF16),
            vmem((2, nz, *message), BF16),
            vmem((2, nz, *message), F32),
            dma((2, nx, nz // 4 + 1)),
            dma((2, nz // 4 + 1)),
            dma((nx, geo.near)),
            dma((2, nz // 4 + 1)),
            dma((2, nz // 4 + 1)),
            dma((2, geo.extra)),
            dma((7, 2)),
            dma((6,)),
        ],
        compiler_params=pltpu.CompilerParams(
            collective_id=0, has_side_effects=True, vmem_limit_bytes=60 * 1024 * 1024
        ),
        name="triangle_updates",
    )(
        pair,
        residue_mask,
        norm_in_gain,
        proj_weight,
        gate_weight,
        norm_out_gain,
        out_weight,
    )
    return jnp.swapaxes(result, 0, 1)


def solution(mesh):
    def body(pair, *rest):
        geo = Geometry(pair.shape[1], pair.shape[2], mesh.shape["gx"], mesh.shape["gy"])
        return per_device(geo, pair, *rest)

    return jax.shard_map(
        body,
        mesh=mesh,
        in_specs=(
            P(("groups", "gz"), "gx", "gy"),
            P("groups"),
            P(None, "gz"),
            P(None, None, None, "gz"),
            P(None, None, "gz"),
            P(None, "gz"),
            P(None, None, "gz"),
        ),
        out_specs=P(("groups", "gz"), "gx", "gy"),
        check_vma=False,
    )
```

```python
import functools

import jax
import jax.numpy as jnp
from jax import lax
from jax.experimental import pallas as pl
from jax.experimental.pallas import tpu as pltpu
from jax.sharding import PartitionSpec as P

EPSILON = 1e-05
LANES = 128
MESH = pl.DeviceIdType.MESH
F32 = jnp.float32
BF16 = jnp.bfloat16


class Geometry:
    def __init__(self, rows, cols, nz, nx):
        self.rows, self.cols, self.nz, self.nx = rows, cols, nz, nx
        self.spare = LANES - cols
        self.blocks = rows * cols // LANES
        self.extra = rows - self.blocks
        self.pieces = cols // self.spare
        self.width = self.blocks * LANES
        self.res = nz * rows
        self.near = cols // rows
        assert self.blocks * LANES == rows * cols
        assert self.extra * self.pieces == self.blocks
        assert nz * rows == nx * cols and self.near * rows == cols


def lane_block(v, k):
    return v[:, k * LANES : (k + 1) * LANES]


def rows_of(geo, v):
    lane = lax.broadcasted_iota(jnp.int32, (v.shape[0], LANES), 1)
    rows = [jnp.where(lane < geo.cols, lane_block(v, r), 0.0) for r in range(geo.blocks)]
    for e in range(geo.extra):
        row = jnp.zeros((v.shape[0], LANES), F32)
        for q in range(geo.pieces):
            low = geo.spare * q
            piece = pltpu.roll(lane_block(v, e * geo.pieces + q), (low - geo.cols) % LANES, 1)
            row = jnp.where((lane >= low) & (lane < low + geo.spare), piece, row)
        rows.append(row)
    return rows


def block_of(geo, get_row, k):
    row = get_row(k)
    lane = lax.broadcasted_iota(jnp.int32, row.shape, 1)
    extra, q = divmod(k, geo.pieces)
    piece = pltpu.roll(get_row(geo.blocks + extra), geo.cols - geo.spare * q, 1)
    return jnp.where(lane < geo.cols, row, piece)


def normed(values, gain):
    mean = jnp.mean(values, axis=0, keepdims=True)
    centred = values - mean
    spread = jnp.mean(centred * centred, axis=0, keepdims=True)
    return (centred * lax.rsqrt(spread + EPSILON) * gain).astype(BF16)


def kernel(
    geo,
    half,
    pair_hbm,
    flag_ref,
    proj_hbm,
    gate_hbm,
    out_hbm,
    out_ref,
    pair_ref,
    proj_ref,
    gate_ref,
    out_weight_ref,
    mask_ref,
    z_all,
    zn,
    tmp,
    gate,
    left_out,
    right_out,
    left_all,
    right_in,
    right_all,
    left_mat,
    right_mat,
    product,
    back_out,
    back_in,
    back_other,
    triangle,
    left_sem,
    right_sem,
    right_x_sem,
    back_sem,
    other_sem,
    z_sem,
    sent_sem,
    load_sem,
):
    nz, nx = geo.nz, geo.nx
    me_z = lax.axis_index("gx")
    me_x = lax.axis_index("gy")
    me_c = lax.axis_index("gz")
    other_c = 1 - me_c
    chunk = geo.pieces * LANES
    chunks = [slice(k, k + chunk) for k in range(0, geo.width, chunk)]

    barrier = pltpu.get_barrier_semaphore()

    def signal_z(k, _):
        pl.semaphore_signal(
            barrier, inc=1, device_id={"gx": lax.rem(me_z + 1 + k, nz)}, device_id_type=MESH
        )
        return _

    lax.fori_loop(0, nz - 1, signal_z, 0)
    for k in range(1, nx):
        pl.semaphore_signal(
            barrier, inc=1, device_id={"gy": lax.rem(me_x + k, nx)}, device_id_type=MESH
        )
    pl.semaphore_signal(barrier, inc=1, device_id={"gz": other_c}, device_id_type=MESH)

    def far_first(k):
        m = (k + 1) // 2
        return lax.rem(me_z + nz // 2 + m * (1 - 2 * (k % 2)), nz)

    def copy_z(src, dst, send, recv, to):
        return pltpu.make_async_remote_copy(
            src_ref=src, dst_ref=dst, send_sem=send, recv_sem=recv, device_id={"gx": to}, device_id_type=MESH
        )

    def copy_x(src, dst, send, recv, to):
        return pltpu.make_async_remote_copy(
            src_ref=src, dst_ref=dst, send_sem=send, recv_sem=recv, device_id={"gy": to}, device_id_type=MESH
        )

    def copy_c(src, dst, send, recv):
        return pltpu.make_async_remote_copy(
            src_ref=src, dst_ref=dst, send_sem=send, recv_sem=recv, device_id={"gz": other_c}, device_id_type=MESH
        )

    def store_rows(mat, lead, base, value):
        for r, row in enumerate(rows_of(geo, value)):
            for h in range(2):
                mat[lead, h, pl.ds(base + r, 1), :] = row[h : h + 1, :]

    lag = 8

    loads = [
        pltpu.make_async_copy(src, dst, load_sem.at[i])
        for i, (src, dst) in enumerate(
            [
                (pair_hbm, pair_ref),
                (proj_hbm, proj_ref),
                (gate_hbm, gate_ref),
                (out_hbm, out_weight_ref),
            ]
        )
    ]
    for load in loads:
        load.start()
    for load in loads[:1]:
        load.wait()
    for c in range(2):
        own = slice(c * half, (c + 1) * half)
        for k in range(geo.blocks):
            e, q = divmod(k, geo.pieces)
            low = geo.spare * q
            z_all[0, c, :, k * LANES : (k + 1) * LANES] = jnp.concatenate(
                [pair_ref[k, own, :], pair_ref[geo.blocks + e, own, low : low + geo.spare]], axis=1
            )

    near_lane = lax.broadcasted_iota(jnp.int32, (1, LANES), 1)
    near_flags = jnp.zeros((1, LANES), F32)
    for t in range(geo.cols):
        flag = flag_ref[me_x * geo.cols + t].astype(F32)
        near_flags = jnp.where(near_lane == t, flag, near_flags)
    row_flag = [flag_ref[me_z * geo.rows + r].astype(F32) for r in range(geo.rows)]
    for k in range(geo.blocks):
        mask_ref[:, k * LANES : (k + 1) * LANES] = block_of(
            geo, lambda r: near_flags * row_flag[r], k
        )

    for load in loads[1:]:
        load.wait()

    def z_piece(i):
        part = z_all.at[1, me_c, :, chunks[i]]
        return copy_c(part, part, sent_sem.at[5, 0], z_sem.at[i])

    for u in range(2):
        left_u, right_u, back_u = left_out.at[u], right_out.at[u], back_out.at[u]

        for i in reversed(range(geo.extra)):
            if u == 1:
                z_piece(i).wait_recv()
            s = chunks[i]
            gain_in = pair_ref[geo.rows, :, u : u + 1]
            z = jnp.concatenate([z_all[u, 0, :, s], z_all[u, 1, :, s]], axis=0)
            zn[:, s] = normed(z, gain_in)

        def project(first, out):
            for s in chunks:
                opening, value = (
                    jnp.dot(proj_ref[u, first + i], zn[:, s], preferred_element_type=F32)
                    for i in range(2)
                )
                tmp[:, s] = jax.nn.sigmoid(opening) * value * mask_ref[:, s]
            for k in range(nz):
                out[k] = tmp[2 * k : 2 * k + 2, :].astype(BF16)

        def forward_left(src, s):
            for k in range(1, nx):
                copy_x(
                    src,
                    left_all.at[u, me_x, s],
                    sent_sem.at[2, u],
                    left_sem.at[u, me_x, s],
                    lax.rem(me_x + k, nx),
                ).start()

        def forward_right(src, s):
            target = s // geo.near

            @pl.when(target != me_x)
            def run():
                copy_x(
                    src,
                    right_all.at[me_x, s % geo.near],
                    sent_sem.at[3, 0],
                    right_x_sem.at[me_x, s % geo.near],
                    target,
                ).start()

        def send_left():
            def send(k, _):
                to = far_first(k)
                copy_z(
                    left_u.at[to],
                    left_all.at[u, me_x, me_z],
                    sent_sem.at[0, u],
                    left_sem.at[u, me_x, me_z],
                    to,
                ).start()
                return _

            lax.fori_loop(0, nz - 1, send, 0)
            forward_left(left_u.at[me_z], me_z)
            left_all[u, me_x, me_z] = left_u[me_z]

        def send_right():
            def send(k, _):
                to = far_first(k)
                copy_z(
                    right_u.at[to],
                    right_in.at[u, me_z],
                    sent_sem.at[1, u],
                    right_sem.at[u, me_z],
                    to,
                ).start()
                return _

            lax.fori_loop(0, nz - 1, send, 0)
            right_in[u, me_z] = right_u[me_z]

        def open_gate():
            for s in chunks:
                gate[:, s] = jax.nn.sigmoid(
                    jnp.dot(gate_ref[u], zn[:, s], preferred_element_type=F32)
                )

        def take_left(k):
            s = far_first(k)
            slot = left_all.at[u, me_x, s]

            @pl.when(k < nz - 1)
            def run():
                copy_z(slot, slot, sent_sem.at[0, u], left_sem.at[u, me_x, s], s).wait_recv()
                forward_left(slot, s)

            store_rows(left_mat, me_x, s * geo.rows, left_all[u, me_x, s].astype(F32))

        def take_left_x(k):
            s = far_first(k)
            for d in range(1, nx):
                x = lax.rem(me_x + d, nx)
                slot = left_all.at[u, x, s]
                copy_x(slot, slot, sent_sem.at[2, u], left_sem.at[u, x, s], x).wait_recv()
                store_rows(left_mat, x, s * geo.rows, left_all[u, x, s].astype(F32))

        def wait_right(k, s):
            slot = right_in.at[u, s]

            @pl.when(k < nz - 1)
            def run():
                copy_z(slot, slot, sent_sem.at[1, u], right_sem.at[u, s], s).wait_recv()

        def block_row(base, r):
            return jnp.concatenate([product[h, pl.ds(base + r, 1), :] for h in range(2)], axis=0)

        def send_back(k):
            to = far_first(k)
            base = to * geo.rows
            for b in range(geo.blocks):
                value = block_of(geo, functools.partial(block_row, base), b)
                back_u[to, :, b * LANES : (b + 1) * LANES] = value.astype(BF16)

            @pl.when(k < nz - 1)
            def run():
                copy_z(
                    back_u.at[to], back_in.at[u, me_z], sent_sem.at[4, u], back_sem.at[u, me_z], to
                ).start()

        project(0, left_u)
        if u == 0:
            pl.semaphore_wait(barrier, nz - 1 + nx - 1 + 1)
        send_left()
        project(2, right_u)
        send_right()
        if u == 0:
            forward_right(right_u.at[me_z], me_z)
        open_gate()

        def take_lefts(k, _):
            take_left(k)

            @pl.when(k >= lag)
            def run():
                take_left_x(k - lag)

            return _

        lax.fori_loop(0, nz, take_lefts, 0)

        def take_right_x(k):
            s = far_first(k)
            at = s % geo.near

            @pl.when(s // geo.near == me_x)
            def run():
                for d in range(1, nx):
                    x = lax.rem(me_x + d, nx)
                    slot = right_all.at[x, at]
                    copy_x(slot, slot, sent_sem.at[3, 0], right_x_sem.at[x, at], x).wait_recv()
                    store_rows(right_mat, x, at * geo.rows, right_all[x, at].astype(F32))

        def take_right(k, _):
            s = far_first(k)
            wait_right(k, s)
            if u == 0:

                @pl.when(k < nz - 1)
                def run():
                    forward_right(right_in.at[0, s], s)

                @pl.when(s // geo.near == me_x)
                def run_own():
                    store_rows(
                        right_mat, me_x, (s % geo.near) * geo.rows, right_in[0, s].astype(F32)
                    )

                @pl.when(k >= lag)
                def run_x():
                    take_right_x(k - lag)

            else:
                store_rows(right_mat, 0, s * geo.rows, right_in[1, s].astype(F32))

            @pl.when(k < lag)
            def run_left():
                take_left_x(nz - lag + k)

            return _

        lax.fori_loop(0, nz, take_right, 0)

        if u == 0:

            def take_last(k, _):
                take_right_x(k)
                return _

            lax.fori_loop(nz - lag, nz, take_last, 0)

            for h in range(2):
                total = jnp.zeros((geo.res, geo.cols), F32)
                for x in range(nx):
                    total += lax.dot_general(
                        left_mat[x, h].astype(BF16),
                        right_mat[x, h, : geo.cols, :].astype(BF16),
                        (((1,), (1,)), ((), ())),
                        preferred_element_type=F32,
                    )
                product[h, :, : geo.cols] = total
        else:
            for h in range(2):
                right = right_mat[0, h].astype(BF16)
                for x in range(nx):
                    part = lax.dot_general(
                        left_mat[x, h].astype(BF16),
                        right,
                        (((0,), (0,)), ((), ())),
                        preferred_element_type=F32,
                    )
                    product[h, geo.cols * x : geo.cols * (x + 1), :] = part[: geo.cols, :]

        def send(k, _):
            send_back(k)
            return _

        lax.fori_loop(0, nz, send, 0)

        def take_back(k, _):
            s = far_first(k)
            slot = back_in.at[u, s]
            copy_z(slot, slot, sent_sem.at[4, u], back_sem.at[u, s], s).wait_recv()
            copy_c(slot, back_other.at[u, s], sent_sem.at[6, u], other_sem.at[u]).start()
            triangle[me_c, s] = back_in[u, s].astype(F32)
            return _

        copy_c(
            back_u.at[me_z], back_other.at[u, me_z], sent_sem.at[6, u], other_sem.at[u]
        ).start()
        triangle[me_c, me_z] = back_u[me_z].astype(F32)
        lax.fori_loop(0, nz - 1, take_back, 0)

        all_other = back_other.at[u]
        copy_c(all_other, all_other, sent_sem.at[6, u], other_sem.at[u]).wait_recv()

        def take_other(k, _):
            triangle[other_c, k] = back_other[u, k].astype(F32)
            return _

        lax.fori_loop(0, nz, take_other, 0)

        gain_out = pair_ref[geo.rows, :, 2 + u : 3 + u]
        for i in reversed(range(geo.extra)):
            s = chunks[i]
            values = jnp.concatenate(
                [triangle[c, k, :, s] for c in range(2) for k in range(nz)], axis=0
            )
            tn = normed(values, gain_out)
            change = jnp.dot(out_weight_ref[u], tn, preferred_element_type=F32)
            value = z_all[u, me_c, :, s] + gate[:, s] * change
            if u == 0:
                z_all[1, me_c, :, s] = value
                z_piece(i).start()
            else:
                lane = lax.broadcasted_iota(jnp.int32, (half, LANES), 1)
                row = jnp.zeros((half, LANES), F32)
                for q in range(geo.pieces):
                    block = lane_block(value, q)
                    out_ref[i * geo.pieces + q] = block[:, : geo.cols]
                    low = geo.spare * q
                    moved = pltpu.roll(block, (low - geo.cols) % LANES, 1)
                    row = jnp.where((lane >= low) & (lane < low + geo.spare), moved, row)
                out_ref[geo.blocks + i] = row[:, : geo.cols]

    any_sem = z_sem.at[0]
    for u in range(2):
        many = left_out.at[u, pl.ds(0, nz - 1)]
        copy_z(many, many, sent_sem.at[0, u], any_sem, me_z).wait_send()
        copy_z(many, many, sent_sem.at[1, u], any_sem, me_z).wait_send()
        copy_z(many, many, sent_sem.at[4, u], any_sem, me_z).wait_send()
        for k in range(1, nx):
            all_slots = left_out.at[u]
            copy_x(all_slots, all_slots, sent_sem.at[2, u], any_sem, me_x).wait_send()
        every = left_out.at[u]
        copy_c(every, every, sent_sem.at[6, u], any_sem).wait_send()
    away = left_out.at[0, pl.ds(0, nz - geo.near)]
    copy_x(away, away, sent_sem.at[3, 0], any_sem, me_x).wait_send()
    part = z_all.at[1, me_c]
    copy_c(part, part, sent_sem.at[5, 0], any_sem).wait_send()


def per_device(
    geo, pair, residue_mask, norm_in_gain, proj_weight, gate_weight, norm_out_gain, out_weight
):
    half = pair.shape[0]
    full = 2 * half
    nz, nx = geo.nz, geo.nx
    vmem = pltpu.VMEM
    message = (2, geo.width)
    dma = pltpu.SemaphoreType.DMA
    hbm = pl.BlockSpec(memory_space=pl.ANY)
    pair = jnp.swapaxes(pair, 0, 1)
    gains = jnp.concatenate([norm_in_gain, norm_out_gain], axis=0).T
    gains = jnp.pad(gains, ((0, 0), (0, geo.cols - gains.shape[1])))
    pair = jnp.concatenate([pair, gains[None]], axis=0)
    pair = lax.all_gather(pair, "gz", axis=1, tiled=True)
    proj_weight = jnp.swapaxes(proj_weight, 2, 3)
    gate_weight = jnp.swapaxes(gate_weight, 1, 2)
    out_weight = jnp.swapaxes(out_weight, 1, 2)
    result = pl.pallas_call(
        functools.partial(kernel, geo, half),
        out_shape=jax.ShapeDtypeStruct((geo.rows, half, geo.cols), F32),
        in_specs=[
            hbm,
            pl.BlockSpec(memory_space=pltpu.SMEM),
            hbm,
            hbm,
            hbm,
        ],
        out_specs=pl.BlockSpec(memory_space=vmem),
        scratch_shapes=[
            vmem(pair.shape, F32),
            vmem(proj_weight.shape, BF16),
            vmem(gate_weight.shape, BF16),
            vmem(out_weight.shape, BF16),
            vmem((1, geo.width), F32),
            vmem((2, 2, half, geo.width), F32),
            vmem((full, geo.width), BF16),
            vmem((half, geo.width), F32),
            vmem((half, geo.width), F32),
            vmem((2, nz, *message), BF16),
            vmem((2, nz, *message), BF16),
            vmem((2, nx, nz, *message), BF16),
            vmem((2, nz, *message), BF16),
            vmem((nx, geo.near, *message), BF16),
            vmem((nx, 2, geo.res, LANES), F32),
            vmem((nx, 2, geo.res, LANES), F32),
            vmem((2, geo.res, LANES), F32),
            vmem((2, nz, *message), BF16),
            vmem((2, nz, *message), BF16),
            vmem((2, nz, *message), BF16),
            vmem((2, nz, *message), F32),
            dma((2, nx, nz)),
            dma((2, nz)),
            dma((nx, geo.near)),
            dma((2, nz)),
            dma((2,)),
            dma((geo.extra,)),
            dma((7, 2)),
            dma((4,)),
        ],
        compiler_params=pltpu.CompilerParams(
            collective_id=0, has_side_effects=True, vmem_limit_bytes=60 * 1024 * 1024
        ),
        name="triangle_updates",
    )(
        pair,
        residue_mask,
        proj_weight,
        gate_weight,
        out_weight,
    )
    return jnp.swapaxes(result, 0, 1)


def solution(mesh):
    def body(pair, *rest):
        geo = Geometry(pair.shape[1], pair.shape[2], mesh.shape["gx"], mesh.shape["gy"])
        return per_device(geo, pair, *rest)

    return jax.shard_map(
        body,
        mesh=mesh,
        in_specs=(
            P(("groups", "gz"), "gx", "gy"),
            P("groups"),
            P(None, "gz"),
            P(None, None, None, "gz"),
            P(None, None, "gz"),
            P(None, "gz"),
            P(None, None, "gz"),
        ),
        out_specs=P(("groups", "gz"), "gx", "gy"),
        check_vma=False,
    )
```

```python
import functools

import jax
import jax.numpy as jnp
from jax import lax
from jax.experimental import pallas as pl
from jax.experimental.pallas import tpu as pltpu
from jax.sharding import PartitionSpec as P

EPSILON = 1e-05
LANES = 128
MESH = pl.DeviceIdType.MESH
F32 = jnp.float32
BF16 = jnp.bfloat16


class Geometry:
    def __init__(self, rows, cols, nz, nx):
        self.rows, self.cols, self.nz, self.nx = rows, cols, nz, nx
        self.spare = LANES - cols
        self.blocks = rows * cols // LANES
        self.extra = rows - self.blocks
        self.pieces = cols // self.spare
        self.width = self.blocks * LANES
        self.res = nz * rows
        self.near = cols // rows
        assert self.blocks * LANES == rows * cols
        assert self.extra * self.pieces == self.blocks
        assert nz * rows == nx * cols and self.near * rows == cols


def lane_block(v, k):
    return v[:, k * LANES : (k + 1) * LANES]


def rows_of(geo, v):
    lane = lax.broadcasted_iota(jnp.int32, (v.shape[0], LANES), 1)
    rows = [jnp.where(lane < geo.cols, lane_block(v, r), 0.0) for r in range(geo.blocks)]
    for e in range(geo.extra):
        row = jnp.zeros((v.shape[0], LANES), F32)
        for q in range(geo.pieces):
            low = geo.spare * q
            piece = pltpu.roll(lane_block(v, e * geo.pieces + q), (low - geo.cols) % LANES, 1)
            row = jnp.where((lane >= low) & (lane < low + geo.spare), piece, row)
        rows.append(row)
    return rows


def block_of(geo, get_row, k):
    row = get_row(k)
    lane = lax.broadcasted_iota(jnp.int32, row.shape, 1)
    extra, q = divmod(k, geo.pieces)
    piece = pltpu.roll(get_row(geo.blocks + extra), geo.cols - geo.spare * q, 1)
    return jnp.where(lane < geo.cols, row, piece)


def normed(values, gain):
    mean = jnp.mean(values, axis=0, keepdims=True)
    centred = values - mean
    spread = jnp.mean(centred * centred, axis=0, keepdims=True)
    return (centred * lax.rsqrt(spread + EPSILON) * gain).astype(BF16)


def kernel(
    geo,
    half,
    pair_hbm,
    flag_ref,
    proj_hbm,
    gate_hbm,
    out_hbm,
    out_ref,
    pair_ref,
    proj_ref,
    gate_ref,
    out_weight_ref,
    mask_ref,
    z_all,
    zn,
    tmp,
    gate,
    left_out,
    right_out,
    left_all,
    right_in,
    right_all,
    left_mat,
    right_mat,
    product,
    back_out,
    back_in,
    back_other,
    triangle,
    left_sem,
    right_sem,
    right_x_sem,
    back_sem,
    other_sem,
    z_sem,
    sent_sem,
    load_sem,
):
    nz, nx = geo.nz, geo.nx
    me_z = lax.axis_index("gx")
    me_x = lax.axis_index("gy")
    me_c = lax.axis_index("gz")
    other_c = 1 - me_c
    chunk = geo.pieces * LANES
    chunks = [slice(k, k + chunk) for k in range(0, geo.width, chunk)]

    barrier = pltpu.get_barrier_semaphore()

    def signal_z(k, _):
        pl.semaphore_signal(
            barrier, inc=1, device_id={"gx": lax.rem(me_z + 1 + k, nz)}, device_id_type=MESH
        )
        return _

    lax.fori_loop(0, nz - 1, signal_z, 0)
    for k in range(1, nx):
        pl.semaphore_signal(
            barrier, inc=1, device_id={"gy": lax.rem(me_x + k, nx)}, device_id_type=MESH
        )
    pl.semaphore_signal(barrier, inc=1, device_id={"gz": other_c}, device_id_type=MESH)

    def far_first(k):
        m = (k + 1) // 2
        return lax.rem(me_z + nz // 2 + m * (1 - 2 * (k % 2)), nz)

    def copy_z(src, dst, send, recv, to):
        return pltpu.make_async_remote_copy(
            src_ref=src, dst_ref=dst, send_sem=send, recv_sem=recv, device_id={"gx": to}, device_id_type=MESH
        )

    def copy_x(src, dst, send, recv, to):
        return pltpu.make_async_remote_copy(
            src_ref=src, dst_ref=dst, send_sem=send, recv_sem=recv, device_id={"gy": to}, device_id_type=MESH
        )

    def copy_c(src, dst, send, recv):
        return pltpu.make_async_remote_copy(
            src_ref=src, dst_ref=dst, send_sem=send, recv_sem=recv, device_id={"gz": other_c}, device_id_type=MESH
        )

    def store_rows(mat, lead, base, value):
        for r, row in enumerate(rows_of(geo, value)):
            for h in range(2):
                mat[lead, h, pl.ds(base + r, 1), :] = row[h : h + 1, :]

    group = 4
    lag = 8

    loads = [
        pltpu.make_async_copy(src, dst, load_sem.at[i])
        for i, (src, dst) in enumerate(
            [
                (pair_hbm, pair_ref),
                (proj_hbm, proj_ref),
                (gate_hbm, gate_ref),
                (out_hbm, out_weight_ref),
            ]
        )
    ]
    for load in loads:
        load.start()
    for load in loads[:1]:
        load.wait()
    for c in range(2):
        own = slice(c * half, (c + 1) * half)
        for k in range(geo.blocks):
            e, q = divmod(k, geo.pieces)
            low = geo.spare * q
            z_all[0, c, :, k * LANES : (k + 1) * LANES] = jnp.concatenate(
                [pair_ref[k, own, :], pair_ref[geo.blocks + e, own, low : low + geo.spare]], axis=1
            )

    near_lane = lax.broadcasted_iota(jnp.int32, (1, LANES), 1)
    near_flags = jnp.zeros((1, LANES), F32)
    for t in range(geo.cols):
        flag = flag_ref[me_x * geo.cols + t].astype(F32)
        near_flags = jnp.where(near_lane == t, flag, near_flags)
    row_flag = [flag_ref[me_z * geo.rows + r].astype(F32) for r in range(geo.rows)]
    for k in range(geo.blocks):
        mask_ref[:, k * LANES : (k + 1) * LANES] = block_of(
            geo, lambda r: near_flags * row_flag[r], k
        )

    for load in loads[1:]:
        load.wait()

    def z_piece(i):
        part = z_all.at[1, me_c, :, chunks[i]]
        return copy_c(part, part, sent_sem.at[5, 0], z_sem.at[i])

    for u in range(2):
        left_u, right_u, back_u = left_out.at[u], right_out.at[u], back_out.at[u]

        for i in reversed(range(geo.extra)):
            if u == 1:
                z_piece(i).wait_recv()
            s = chunks[i]
            gain_in = pair_ref[geo.rows, :, u : u + 1]
            z = jnp.concatenate([z_all[u, 0, :, s], z_all[u, 1, :, s]], axis=0)
            zn[:, s] = normed(z, gain_in)

        def project(first, out):
            for s in chunks:
                opening, value = (
                    jnp.dot(proj_ref[u, first + i], zn[:, s], preferred_element_type=F32)
                    for i in range(2)
                )
                tmp[:, s] = jax.nn.sigmoid(opening) * value * mask_ref[:, s]
            for k in range(nz):
                out[k] = tmp[2 * k : 2 * k + 2, :].astype(BF16)

        def forward_left(src, s):
            for k in range(1, nx):
                copy_x(
                    src,
                    left_all.at[u, me_x, s],
                    sent_sem.at[2, u],
                    left_sem.at[u, me_x, s],
                    lax.rem(me_x + k, nx),
                ).start()

        def forward_right(src, s):
            target = s // geo.near

            @pl.when(target != me_x)
            def run():
                copy_x(
                    src,
                    right_all.at[me_x, s % geo.near],
                    sent_sem.at[3, 0],
                    right_x_sem.at[me_x, s % geo.near],
                    target,
                ).start()

        def send_left():
            def send(k, _):
                to = far_first(k)
                copy_z(
                    left_u.at[to],
                    left_all.at[u, me_x, me_z],
                    sent_sem.at[0, u],
                    left_sem.at[u, me_x, me_z],
                    to,
                ).start()
                return _

            lax.fori_loop(0, nz - 1, send, 0)
            forward_left(left_u.at[me_z], me_z)
            left_all[u, me_x, me_z] = left_u[me_z]

        def send_right():
            def send(k, _):
                to = far_first(k)
                copy_z(
                    right_u.at[to],
                    right_in.at[u, me_z],
                    sent_sem.at[1, u],
                    right_sem.at[u, me_z],
                    to,
                ).start()
                return _

            lax.fori_loop(0, nz - 1, send, 0)
            right_in[u, me_z] = right_u[me_z]

        def open_gate():
            for s in chunks:
                gate[:, s] = jax.nn.sigmoid(
                    jnp.dot(gate_ref[u], zn[:, s], preferred_element_type=F32)
                )

        def left_base(k, s):
            return (k if u == 0 else s) * geo.rows

        def take_left(k):
            s = far_first(k)
            slot = left_all.at[u, me_x, s]

            @pl.when(k < nz - 1)
            def run():
                copy_z(slot, slot, sent_sem.at[0, u], left_sem.at[u, me_x, s], s).wait_recv()
                forward_left(slot, s)

            store_rows(left_mat, me_x, left_base(k, s), left_all[u, me_x, s].astype(F32))

        def take_left_x(k):
            s = far_first(k)
            for d in range(1, nx):
                x = lax.rem(me_x + d, nx)
                slot = left_all.at[u, x, s]
                copy_x(slot, slot, sent_sem.at[2, u], left_sem.at[u, x, s], x).wait_recv()
                store_rows(left_mat, x, left_base(k, s), left_all[u, x, s].astype(F32))

        def wait_right(k, s):
            slot = right_in.at[u, s]

            @pl.when(k < nz - 1)
            def run():
                copy_z(slot, slot, sent_sem.at[1, u], right_sem.at[u, s], s).wait_recv()

        def block_row(base, r):
            return jnp.concatenate([product[h, pl.ds(base + r, 1), :] for h in range(2)], axis=0)

        def send_back(k):
            to = far_first(k)
            base = left_base(k, to)
            for b in range(geo.blocks):
                value = block_of(geo, functools.partial(block_row, base), b)
                back_u[to, :, b * LANES : (b + 1) * LANES] = value.astype(BF16)

            @pl.when(k < nz - 1)
            def run():
                copy_z(
                    back_u.at[to], back_in.at[u, me_z], sent_sem.at[4, u], back_sem.at[u, me_z], to
                ).start()

        if u == 0:
            project(2, right_u)
            pl.semaphore_wait(barrier, nz - 1 + nx - 1 + 1)
            send_right()
            forward_right(right_u.at[me_z], me_z)
            project(0, left_u)
            send_left()
            open_gate()

            def take_right(k, _):
                s = far_first(k)
                wait_right(k, s)

                @pl.when(k < nz - 1)
                def run():
                    forward_right(right_in.at[0, s], s)

                @pl.when(s // geo.near == me_x)
                def run_own():
                    store_rows(
                        right_mat, me_x, (s % geo.near) * geo.rows, right_in[0, s].astype(F32)
                    )

                return _

            lax.fori_loop(0, nz, take_right, 0)

            def take_group(g):
                def take(i, _):
                    take_left(g * group + i)
                    return _

                lax.fori_loop(0, group, take, 0)

            take_group(0)

            for d in range(1, nx):
                x = lax.rem(me_x + d, nx)

                def take_right_x(k, _):
                    slot = right_all.at[x, k]
                    copy_x(slot, slot, sent_sem.at[3, 0], right_x_sem.at[x, k], x).wait_recv()
                    store_rows(right_mat, x, k * geo.rows, right_all[x, k].astype(F32))
                    return _

                lax.fori_loop(0, geo.near, take_right_x, 0)
            take_group(1)

            tall = group * geo.rows

            def work(g, _):
                @pl.when(g < nz // group - 2)
                def run():
                    take_group(g + 2)

                def take_x(i, _):
                    take_left_x(g * group + i)
                    return _

                lax.fori_loop(0, group, take_x, 0)
                rows = pl.ds(pl.multiple_of(g * tall, tall), tall)
                for h in range(2):
                    total = jnp.zeros((tall, geo.cols), F32)
                    for x in range(nx):
                        total += lax.dot_general(
                            left_mat[x, h, rows, :].astype(BF16),
                            right_mat[x, h, : geo.cols, :].astype(BF16),
                            (((1,), (1,)), ((), ())),
                            preferred_element_type=F32,
                        )
                    product[h, rows, : geo.cols] = total

                def send(i, _):
                    send_back(g * group + i)
                    return _

                lax.fori_loop(0, group, send, 0)
                return _

            lax.fori_loop(0, nz // group, work, 0)
        else:
            project(0, left_u)
            send_left()
            project(2, right_u)
            send_right()
            open_gate()

            def take_lefts(k, _):
                take_left(k)

                @pl.when(k >= lag)
                def run():
                    take_left_x(k - lag)

                return _

            lax.fori_loop(0, nz, take_lefts, 0)

            def take_right(k, _):
                s = far_first(k)
                wait_right(k, s)
                store_rows(right_mat, 0, s * geo.rows, right_in[1, s].astype(F32))

                @pl.when(k < lag)
                def run():
                    take_left_x(nz - lag + k)

                return _

            lax.fori_loop(0, nz, take_right, 0)

            for h in range(2):
                right = right_mat[0, h].astype(BF16)
                for x in range(nx):
                    part = lax.dot_general(
                        left_mat[x, h].astype(BF16),
                        right,
                        (((0,), (0,)), ((), ())),
                        preferred_element_type=F32,
                    )
                    product[h, geo.cols * x : geo.cols * (x + 1), :] = part[: geo.cols, :]

            def send(k, _):
                send_back(k)
                return _

            lax.fori_loop(0, nz, send, 0)

        def take_back(k, _):
            s = far_first(k)
            slot = back_in.at[u, s]
            copy_z(slot, slot, sent_sem.at[4, u], back_sem.at[u, s], s).wait_recv()
            copy_c(slot, back_other.at[u, s], sent_sem.at[6, u], other_sem.at[u]).start()
            triangle[me_c, s] = back_in[u, s].astype(F32)
            return _

        copy_c(
            back_u.at[me_z], back_other.at[u, me_z], sent_sem.at[6, u], other_sem.at[u]
        ).start()
        triangle[me_c, me_z] = back_u[me_z].astype(F32)
        lax.fori_loop(0, nz - 1, take_back, 0)

        all_other = back_other.at[u]
        copy_c(all_other, all_other, sent_sem.at[6, u], other_sem.at[u]).wait_recv()

        def take_other(k, _):
            triangle[other_c, k] = back_other[u, k].astype(F32)
            return _

        lax.fori_loop(0, nz, take_other, 0)

        gain_out = pair_ref[geo.rows, :, 2 + u : 3 + u]
        for i in reversed(range(geo.extra)):
            s = chunks[i]
            values = jnp.concatenate(
                [triangle[c, k, :, s] for c in range(2) for k in range(nz)], axis=0
            )
            tn = normed(values, gain_out)
            change = jnp.dot(out_weight_ref[u], tn, preferred_element_type=F32)
            value = z_all[u, me_c, :, s] + gate[:, s] * change
            if u == 0:
                z_all[1, me_c, :, s] = value
                z_piece(i).start()
            else:
                lane = lax.broadcasted_iota(jnp.int32, (half, LANES), 1)
                row = jnp.zeros((half, LANES), F32)
                for q in range(geo.pieces):
                    block = lane_block(value, q)
                    out_ref[i * geo.pieces + q] = block[:, : geo.cols]
                    low = geo.spare * q
                    moved = pltpu.roll(block, (low - geo.cols) % LANES, 1)
                    row = jnp.where((lane >= low) & (lane < low + geo.spare), moved, row)
                out_ref[geo.blocks + i] = row[:, : geo.cols]

    any_sem = z_sem.at[0]
    for u in range(2):
        many = left_out.at[u, pl.ds(0, nz - 1)]
        copy_z(many, many, sent_sem.at[0, u], any_sem, me_z).wait_send()
        copy_z(many, many, sent_sem.at[1, u], any_sem, me_z).wait_send()
        copy_z(many, many, sent_sem.at[4, u], any_sem, me_z).wait_send()
        for k in range(1, nx):
            all_slots = left_out.at[u]
            copy_x(all_slots, all_slots, sent_sem.at[2, u], any_sem, me_x).wait_send()
        every = left_out.at[u]
        copy_c(every, every, sent_sem.at[6, u], any_sem).wait_send()
    away = left_out.at[0, pl.ds(0, nz - geo.near)]
    copy_x(away, away, sent_sem.at[3, 0], any_sem, me_x).wait_send()
    part = z_all.at[1, me_c]
    copy_c(part, part, sent_sem.at[5, 0], any_sem).wait_send()


def per_device(
    geo, pair, residue_mask, norm_in_gain, proj_weight, gate_weight, norm_out_gain, out_weight
):
    half = pair.shape[0]
    full = 2 * half
    nz, nx = geo.nz, geo.nx
    vmem = pltpu.VMEM
    message = (2, geo.width)
    dma = pltpu.SemaphoreType.DMA
    hbm = pl.BlockSpec(memory_space=pl.ANY)
    pair = jnp.swapaxes(pair, 0, 1)
    gains = jnp.concatenate([norm_in_gain, norm_out_gain], axis=0).T
    gains = jnp.pad(gains, ((0, 0), (0, geo.cols - gains.shape[1])))
    pair = jnp.concatenate([pair, gains[None]], axis=0)
    pair = lax.all_gather(pair, "gz", axis=1, tiled=True)
    proj_weight = jnp.swapaxes(proj_weight, 2, 3)
    gate_weight = jnp.swapaxes(gate_weight, 1, 2)
    out_weight = jnp.swapaxes(out_weight, 1, 2)
    result = pl.pallas_call(
        functools.partial(kernel, geo, half),
        out_shape=jax.ShapeDtypeStruct((geo.rows, half, geo.cols), F32),
        in_specs=[
            hbm,
            pl.BlockSpec(memory_space=pltpu.SMEM),
            hbm,
            hbm,
            hbm,
        ],
        out_specs=pl.BlockSpec(memory_space=vmem),
        scratch_shapes=[
            vmem(pair.shape, F32),
            vmem(proj_weight.shape, BF16),
            vmem(gate_weight.shape, BF16),
            vmem(out_weight.shape, BF16),
            vmem((1, geo.width), F32),
            vmem((2, 2, half, geo.width), F32),
            vmem((full, geo.width), BF16),
            vmem((half, geo.width), F32),
            vmem((half, geo.width), F32),
            vmem((2, nz, *message), BF16),
            vmem((2, nz, *message), BF16),
            vmem((2, nx, nz, *message), BF16),
            vmem((2, nz, *message), BF16),
            vmem((nx, geo.near, *message), BF16),
            vmem((nx, 2, geo.res, LANES), F32),
            vmem((nx, 2, geo.res, LANES), F32),
            vmem((2, geo.res, LANES), F32),
            vmem((2, nz, *message), BF16),
            vmem((2, nz, *message), BF16),
            vmem((2, nz, *message), BF16),
            vmem((2, nz, *message), F32),
            dma((2, nx, nz)),
            dma((2, nz)),
            dma((nx, geo.near)),
            dma((2, nz)),
            dma((2,)),
            dma((geo.extra,)),
            dma((7, 2)),
            dma((4,)),
        ],
        compiler_params=pltpu.CompilerParams(
            collective_id=0, has_side_effects=True, vmem_limit_bytes=60 * 1024 * 1024
        ),
        name="triangle_updates",
    )(
        pair,
        residue_mask,
        proj_weight,
        gate_weight,
        out_weight,
    )
    return jnp.swapaxes(result, 0, 1)


def solution(mesh):
    def body(pair, *rest):
        geo = Geometry(pair.shape[1], pair.shape[2], mesh.shape["gx"], mesh.shape["gy"])
        return per_device(geo, pair, *rest)

    return jax.shard_map(
        body,
        mesh=mesh,
        in_specs=(
            P(("groups", "gz"), "gx", "gy"),
            P("groups"),
            P(None, "gz"),
            P(None, None, None, "gz"),
            P(None, None, "gz"),
            P(None, "gz"),
            P(None, None, "gz"),
        ),
        out_specs=P(("groups", "gz"), "gx", "gy"),
        check_vma=False,
    )
```

```python
import functools

import jax
import jax.numpy as jnp
from jax import lax
from jax.experimental import pallas as pl
from jax.experimental.pallas import tpu as pltpu
from jax.sharding import PartitionSpec as P

EPSILON = 1e-05
LANES = 128
MESH = pl.DeviceIdType.MESH
F32 = jnp.float32
BF16 = jnp.bfloat16


class Geometry:
    def __init__(self, rows, cols, nz, nx):
        self.rows, self.cols, self.nz, self.nx = rows, cols, nz, nx
        self.spare = LANES - cols
        self.blocks = rows * cols // LANES
        self.extra = rows - self.blocks
        self.pieces = cols // self.spare
        self.width = self.blocks * LANES
        self.res = nz * rows
        self.near = cols // rows
        assert self.blocks * LANES == rows * cols
        assert self.extra * self.pieces == self.blocks
        assert nz * rows == nx * cols and self.near * rows == cols


def lane_block(v, k):
    return v[:, k * LANES : (k + 1) * LANES]


def rows_of(geo, v):
    lane = lax.broadcasted_iota(jnp.int32, (v.shape[0], LANES), 1)
    rows = [jnp.where(lane < geo.cols, lane_block(v, r), 0.0) for r in range(geo.blocks)]
    for e in range(geo.extra):
        row = jnp.zeros((v.shape[0], LANES), F32)
        for q in range(geo.pieces):
            low = geo.spare * q
            piece = pltpu.roll(lane_block(v, e * geo.pieces + q), (low - geo.cols) % LANES, 1)
            row = jnp.where((lane >= low) & (lane < low + geo.spare), piece, row)
        rows.append(row)
    return rows


def block_of(geo, get_row, k):
    row = get_row(k)
    lane = lax.broadcasted_iota(jnp.int32, row.shape, 1)
    extra, q = divmod(k, geo.pieces)
    piece = pltpu.roll(get_row(geo.blocks + extra), geo.cols - geo.spare * q, 1)
    return jnp.where(lane < geo.cols, row, piece)


def normed(values, gain):
    mean = jnp.mean(values, axis=0, keepdims=True)
    centred = values - mean
    spread = jnp.mean(centred * centred, axis=0, keepdims=True)
    return (centred * lax.rsqrt(spread + EPSILON) * gain).astype(BF16)


def kernel(
    geo,
    half,
    pair_hbm,
    flag_ref,
    proj_hbm,
    gate_hbm,
    out_hbm,
    out_ref,
    pair_ref,
    proj_ref,
    gate_ref,
    out_weight_ref,
    mask_ref,
    z_all,
    zn,
    tmp,
    gate,
    left_out,
    right_out,
    left_all,
    right_in,
    right_all,
    left_mat,
    right_mat,
    product,
    back_out,
    back_in,
    back_other,
    triangle,
    left_sem,
    right_sem,
    right_x_sem,
    back_sem,
    other_sem,
    z_sem,
    sent_sem,
    load_sem,
):
    nz, nx = geo.nz, geo.nx
    me_z = lax.axis_index("gx")
    me_x = lax.axis_index("gy")
    me_c = lax.axis_index("gz")
    other_c = 1 - me_c
    chunk = geo.pieces * LANES
    chunks = [slice(k, k + chunk) for k in range(0, geo.width, chunk)]

    barrier = pltpu.get_barrier_semaphore()

    def signal_z(k, _):
        pl.semaphore_signal(
            barrier, inc=1, device_id={"gx": lax.rem(me_z + 1 + k, nz)}, device_id_type=MESH
        )
        return _

    lax.fori_loop(0, nz - 1, signal_z, 0)
    for k in range(1, nx):
        pl.semaphore_signal(
            barrier, inc=1, device_id={"gy": lax.rem(me_x + k, nx)}, device_id_type=MESH
        )
    pl.semaphore_signal(barrier, inc=1, device_id={"gz": other_c}, device_id_type=MESH)

    def far_first(k):
        m = (k + 1) // 2
        return lax.rem(me_z + nz // 2 + m * (1 - 2 * (k % 2)), nz)

    def copy_z(src, dst, send, recv, to):
        return pltpu.make_async_remote_copy(
            src_ref=src, dst_ref=dst, send_sem=send, recv_sem=recv, device_id={"gx": to}, device_id_type=MESH
        )

    def copy_x(src, dst, send, recv, to):
        return pltpu.make_async_remote_copy(
            src_ref=src, dst_ref=dst, send_sem=send, recv_sem=recv, device_id={"gy": to}, device_id_type=MESH
        )

    def copy_c(src, dst, send, recv):
        return pltpu.make_async_remote_copy(
            src_ref=src, dst_ref=dst, send_sem=send, recv_sem=recv, device_id={"gz": other_c}, device_id_type=MESH
        )

    def store_rows(mat, lead, base, value):
        for r, row in enumerate(rows_of(geo, value)):
            for h in range(2):
                mat[lead, h, pl.ds(base + r, 1), :] = row[h : h + 1, :]

    group = 4
    lag = 8

    loads = [
        pltpu.make_async_copy(src, dst, load_sem.at[i])
        for i, (src, dst) in enumerate(
            [
                (pair_hbm, pair_ref),
                (proj_hbm, proj_ref),
                (gate_hbm, gate_ref),
                (out_hbm, out_weight_ref),
            ]
        )
    ]
    for load in loads:
        load.start()
    for load in loads[:1]:
        load.wait()
    for c in range(2):
        own = slice(c * half, (c + 1) * half)
        for k in range(geo.blocks):
            e, q = divmod(k, geo.pieces)
            low = geo.spare * q
            z_all[0, c, :, k * LANES : (k + 1) * LANES] = jnp.concatenate(
                [pair_ref[k, own, :], pair_ref[geo.blocks + e, own, low : low + geo.spare]], axis=1
            )

    near_lane = lax.broadcasted_iota(jnp.int32, (1, LANES), 1)
    near_flags = jnp.zeros((1, LANES), F32)
    for t in range(geo.cols):
        flag = flag_ref[me_x * geo.cols + t].astype(F32)
        near_flags = jnp.where(near_lane == t, flag, near_flags)
    row_flag = [flag_ref[me_z * geo.rows + r].astype(F32) for r in range(geo.rows)]
    for k in range(geo.blocks):
        mask_ref[:, k * LANES : (k + 1) * LANES] = block_of(
            geo, lambda r: near_flags * row_flag[r], k
        )

    for load in loads[1:]:
        load.wait()

    def z_piece(i):
        part = z_all.at[1, me_c, :, chunks[i]]
        return copy_c(part, part, sent_sem.at[5, 0], z_sem.at[i])

    for u in range(2):
        left_u, right_u, back_u = left_out.at[u], right_out.at[u], back_out.at[u]

        for i in reversed(range(geo.extra)):
            if u == 1:
                z_piece(i).wait_recv()
            s = chunks[i]
            gain_in = pair_ref[geo.rows, :, u : u + 1]
            z = jnp.concatenate([z_all[u, 0, :, s], z_all[u, 1, :, s]], axis=0)
            zn[:, s] = normed(z, gain_in)

        def project(first, out):
            for s in chunks:
                opening, value = (
                    jnp.dot(proj_ref[u, first + i], zn[:, s], preferred_element_type=F32)
                    for i in range(2)
                )
                tmp[:, s] = jax.nn.sigmoid(opening) * value * mask_ref[:, s]
            for k in range(nz):
                out[k] = tmp[2 * k : 2 * k + 2, :].astype(BF16)

        def forward_left(src, s):
            for k in range(1, nx):
                copy_x(
                    src,
                    left_all.at[u, me_x, s],
                    sent_sem.at[2, u],
                    left_sem.at[u, me_x, s],
                    lax.rem(me_x + k, nx),
                ).start()

        def forward_right(src, s):
            target = s // geo.near

            @pl.when(target != me_x)
            def run():
                copy_x(
                    src,
                    right_all.at[me_x, s % geo.near],
                    sent_sem.at[3, 0],
                    right_x_sem.at[me_x, s % geo.near],
                    target,
                ).start()

        def send_left():
            def send(k, _):
                to = far_first(k)
                copy_z(
                    left_u.at[to],
                    left_all.at[u, me_x, me_z],
                    sent_sem.at[0, u],
                    left_sem.at[u, me_x, me_z],
                    to,
                ).start()
                return _

            lax.fori_loop(0, nz - 1, send, 0)
            forward_left(left_u.at[me_z], me_z)
            left_all[u, me_x, me_z] = left_u[me_z]

        def send_right():
            def send(k, _):
                to = far_first(k)
                copy_z(
                    right_u.at[to],
                    right_in.at[u, me_z],
                    sent_sem.at[1, u],
                    right_sem.at[u, me_z],
                    to,
                ).start()
                return _

            lax.fori_loop(0, nz - 1, send, 0)
            right_in[u, me_z] = right_u[me_z]

        def open_gate():
            for s in chunks:
                gate[:, s] = jax.nn.sigmoid(
                    jnp.dot(gate_ref[u], zn[:, s], preferred_element_type=F32)
                )

        def left_base(k, s):
            return (k if u == 0 else s) * geo.rows

        def take_left(k):
            s = far_first(k)
            slot = left_all.at[u, me_x, s]

            @pl.when(k < nz - 1)
            def run():
                copy_z(slot, slot, sent_sem.at[0, u], left_sem.at[u, me_x, s], s).wait_recv()
                forward_left(slot, s)

        def take_left_x(k):
            s = far_first(k)
            for d in range(1, nx):
                x = lax.rem(me_x + d, nx)
                slot = left_all.at[u, x, s]
                copy_x(slot, slot, sent_sem.at[2, u], left_sem.at[u, x, s], x).wait_recv()
            value = jnp.concatenate([left_all[u, x, s].astype(F32) for x in range(nx)], axis=0)
            for r, row in enumerate(rows_of(geo, value)):
                at = pl.ds(left_base(k, s) + r, 1)
                for x in range(nx):
                    for h in range(2):
                        left_mat[x, h, at, :] = row[2 * x + h : 2 * x + h + 1, :]

        def wait_right(k, s):
            slot = right_in.at[u, s]

            @pl.when(k < nz - 1)
            def run():
                copy_z(slot, slot, sent_sem.at[1, u], right_sem.at[u, s], s).wait_recv()

        def block_row(base, r):
            return jnp.concatenate([product[h, pl.ds(base + r, 1), :] for h in range(2)], axis=0)

        def send_back(k):
            to = far_first(k)
            base = left_base(k, to)
            for b in range(geo.blocks):
                value = block_of(geo, functools.partial(block_row, base), b)
                back_u[to, :, b * LANES : (b + 1) * LANES] = value.astype(BF16)

            @pl.when(k < nz - 1)
            def run():
                copy_z(
                    back_u.at[to], back_in.at[u, me_z], sent_sem.at[4, u], back_sem.at[u, me_z], to
                ).start()

        if u == 0:
            project(2, right_u)
            pl.semaphore_wait(barrier, nz - 1 + nx - 1 + 1)
            send_right()
            forward_right(right_u.at[me_z], me_z)
            project(0, left_u)
            send_left()
            open_gate()

            def take_right(k, _):
                s = far_first(k)
                wait_right(k, s)

                @pl.when(k < nz - 1)
                def run():
                    forward_right(right_in.at[0, s], s)

                @pl.when(s // geo.near == me_x)
                def run_own():
                    store_rows(
                        right_mat, me_x, (s % geo.near) * geo.rows, right_in[0, s].astype(F32)
                    )

                return _

            lax.fori_loop(0, nz, take_right, 0)

            def take_group(g):
                def take(i, _):
                    take_left(g * group + i)
                    return _

                lax.fori_loop(0, group, take, 0)

            take_group(0)

            for d in range(1, nx):
                x = lax.rem(me_x + d, nx)

                def take_right_x(k, _):
                    slot = right_all.at[x, k]
                    copy_x(slot, slot, sent_sem.at[3, 0], right_x_sem.at[x, k], x).wait_recv()
                    store_rows(right_mat, x, k * geo.rows, right_all[x, k].astype(F32))
                    return _

                lax.fori_loop(0, geo.near, take_right_x, 0)
            take_group(1)

            tall = group * geo.rows

            def work(g, _):
                @pl.when(g < nz // group - 2)
                def run():
                    take_group(g + 2)

                def take_x(i, _):
                    take_left_x(g * group + i)
                    return _

                lax.fori_loop(0, group, take_x, 0)
                rows = pl.ds(pl.multiple_of(g * tall, tall), tall)
                for h in range(2):
                    total = jnp.zeros((tall, geo.cols), F32)
                    for x in range(nx):
                        total += lax.dot_general(
                            left_mat[x, h, rows, :].astype(BF16),
                            right_mat[x, h, : geo.cols, :].astype(BF16),
                            (((1,), (1,)), ((), ())),
                            preferred_element_type=F32,
                        )
                    product[h, rows, : geo.cols] = total

                def send(i, _):
                    send_back(g * group + i)
                    return _

                lax.fori_loop(0, group, send, 0)
                return _

            lax.fori_loop(0, nz // group, work, 0)
        else:
            project(0, left_u)
            send_left()
            project(2, right_u)
            send_right()
            open_gate()

            def take_lefts(k, _):
                take_left(k)

                @pl.when(k >= lag)
                def run():
                    take_left_x(k - lag)

                return _

            lax.fori_loop(0, nz, take_lefts, 0)

            def take_right(k, _):
                s = far_first(k)
                wait_right(k, s)
                store_rows(right_mat, 0, s * geo.rows, right_in[1, s].astype(F32))

                @pl.when(k < lag)
                def run():
                    take_left_x(nz - lag + k)

                return _

            lax.fori_loop(0, nz, take_right, 0)

            for h in range(2):
                right = right_mat[0, h].astype(BF16)
                for x in range(nx):
                    part = lax.dot_general(
                        left_mat[x, h].astype(BF16),
                        right,
                        (((0,), (0,)), ((), ())),
                        preferred_element_type=F32,
                    )
                    product[h, geo.cols * x : geo.cols * (x + 1), :] = part[: geo.cols, :]

            def send(k, _):
                send_back(k)
                return _

            lax.fori_loop(0, nz, send, 0)

        def take_back(k, _):
            s = far_first(k)
            slot = back_in.at[u, s]
            copy_z(slot, slot, sent_sem.at[4, u], back_sem.at[u, s], s).wait_recv()
            copy_c(slot, back_other.at[u, s], sent_sem.at[6, u], other_sem.at[u]).start()
            triangle[me_c, s] = back_in[u, s].astype(F32)
            return _

        copy_c(
            back_u.at[me_z], back_other.at[u, me_z], sent_sem.at[6, u], other_sem.at[u]
        ).start()
        triangle[me_c, me_z] = back_u[me_z].astype(F32)
        lax.fori_loop(0, nz - 1, take_back, 0)

        all_other = back_other.at[u]
        copy_c(all_other, all_other, sent_sem.at[6, u], other_sem.at[u]).wait_recv()

        def take_other(k, _):
            triangle[other_c, k] = back_other[u, k].astype(F32)
            return _

        lax.fori_loop(0, nz, take_other, 0)

        gain_out = pair_ref[geo.rows, :, 2 + u : 3 + u]
        for i in reversed(range(geo.extra)):
            s = chunks[i]
            values = jnp.concatenate(
                [triangle[c, k, :, s] for c in range(2) for k in range(nz)], axis=0
            )
            tn = normed(values, gain_out)
            change = jnp.dot(out_weight_ref[u], tn, preferred_element_type=F32)
            value = z_all[u, me_c, :, s] + gate[:, s] * change
            if u == 0:
                z_all[1, me_c, :, s] = value
                z_piece(i).start()
            else:
                lane = lax.broadcasted_iota(jnp.int32, (half, LANES), 1)
                row = jnp.zeros((half, LANES), F32)
                for q in range(geo.pieces):
                    block = lane_block(value, q)
                    out_ref[i * geo.pieces + q] = block[:, : geo.cols]
                    low = geo.spare * q
                    moved = pltpu.roll(block, (low - geo.cols) % LANES, 1)
                    row = jnp.where((lane >= low) & (lane < low + geo.spare), moved, row)
                out_ref[geo.blocks + i] = row[:, : geo.cols]

    any_sem = z_sem.at[0]
    for u in range(2):
        many = left_out.at[u, pl.ds(0, nz - 1)]
        copy_z(many, many, sent_sem.at[0, u], any_sem, me_z).wait_send()
        copy_z(many, many, sent_sem.at[1, u], any_sem, me_z).wait_send()
        copy_z(many, many, sent_sem.at[4, u], any_sem, me_z).wait_send()
        for k in range(1, nx):
            all_slots = left_out.at[u]
            copy_x(all_slots, all_slots, sent_sem.at[2, u], any_sem, me_x).wait_send()
        every = left_out.at[u]
        copy_c(every, every, sent_sem.at[6, u], any_sem).wait_send()
    away = left_out.at[0, pl.ds(0, nz - geo.near)]
    copy_x(away, away, sent_sem.at[3, 0], any_sem, me_x).wait_send()
    part = z_all.at[1, me_c]
    copy_c(part, part, sent_sem.at[5, 0], any_sem).wait_send()


def per_device(
    geo, pair, residue_mask, norm_in_gain, proj_weight, gate_weight, norm_out_gain, out_weight
):
    half = pair.shape[0]
    full = 2 * half
    nz, nx = geo.nz, geo.nx
    vmem = pltpu.VMEM
    message = (2, geo.width)
    dma = pltpu.SemaphoreType.DMA
    hbm = pl.BlockSpec(memory_space=pl.ANY)
    pair = jnp.swapaxes(pair, 0, 1)
    gains = jnp.concatenate([norm_in_gain, norm_out_gain], axis=0).T
    gains = jnp.pad(gains, ((0, 0), (0, geo.cols - gains.shape[1])))
    pair = jnp.concatenate([pair, gains[None]], axis=0)
    pair = lax.all_gather(pair, "gz", axis=1, tiled=True)
    proj_weight = jnp.swapaxes(proj_weight, 2, 3)
    gate_weight = jnp.swapaxes(gate_weight, 1, 2)
    out_weight = jnp.swapaxes(out_weight, 1, 2)
    result = pl.pallas_call(
        functools.partial(kernel, geo, half),
        out_shape=jax.ShapeDtypeStruct((geo.rows, half, geo.cols), F32),
        in_specs=[
            hbm,
            pl.BlockSpec(memory_space=pltpu.SMEM),
            hbm,
            hbm,
            hbm,
        ],
        out_specs=pl.BlockSpec(memory_space=vmem),
        scratch_shapes=[
            vmem(pair.shape, F32),
            vmem(proj_weight.shape, BF16),
            vmem(gate_weight.shape, BF16),
            vmem(out_weight.shape, BF16),
            vmem((1, geo.width), F32),
            vmem((2, 2, half, geo.width), F32),
            vmem((full, geo.width), BF16),
            vmem((half, geo.width), F32),
            vmem((half, geo.width), F32),
            vmem((2, nz, *message), BF16),
            vmem((2, nz, *message), BF16),
            vmem((2, nx, nz, *message), BF16),
            vmem((2, nz, *message), BF16),
            vmem((nx, geo.near, *message), BF16),
            vmem((nx, 2, geo.res, LANES), F32),
            vmem((nx, 2, geo.res, LANES), F32),
            vmem((2, geo.res, LANES), F32),
            vmem((2, nz, *message), BF16),
            vmem((2, nz, *message), BF16),
            vmem((2, nz, *message), BF16),
            vmem((2, nz, *message), F32),
            dma((2, nx, nz)),
            dma((2, nz)),
            dma((nx, geo.near)),
            dma((2, nz)),
            dma((2,)),
            dma((geo.extra,)),
            dma((7, 2)),
            dma((4,)),
        ],
        compiler_params=pltpu.CompilerParams(
            collective_id=0, has_side_effects=True, vmem_limit_bytes=60 * 1024 * 1024
        ),
        name="triangle_updates",
    )(
        pair,
        residue_mask,
        proj_weight,
        gate_weight,
        out_weight,
    )
    return jnp.swapaxes(result, 0, 1)


def solution(mesh):
    def body(pair, *rest):
        geo = Geometry(pair.shape[1], pair.shape[2], mesh.shape["gx"], mesh.shape["gy"])
        return per_device(geo, pair, *rest)

    return jax.shard_map(
        body,
        mesh=mesh,
        in_specs=(
            P(("groups", "gz"), "gx", "gy"),
            P("groups"),
            P(None, "gz"),
            P(None, None, None, "gz"),
            P(None, None, "gz"),
            P(None, "gz"),
            P(None, None, "gz"),
        ),
        out_specs=P(("groups", "gz"), "gx", "gy"),
        check_vma=False,
    )
```

```python
import functools

import jax
import jax.numpy as jnp
from jax import lax
from jax.experimental import pallas as pl
from jax.experimental.pallas import tpu as pltpu
from jax.sharding import PartitionSpec as P

EPSILON = 1e-05
LANES = 128
MESH = pl.DeviceIdType.MESH
F32 = jnp.float32
BF16 = jnp.bfloat16


class Geometry:
    def __init__(self, rows, cols, nz, nx):
        self.rows, self.cols, self.nz, self.nx = rows, cols, nz, nx
        self.spare = LANES - cols
        self.blocks = rows * cols // LANES
        self.extra = rows - self.blocks
        self.pieces = cols // self.spare
        self.width = self.blocks * LANES
        self.res = nz * rows
        self.near = cols // rows
        assert self.blocks * LANES == rows * cols
        assert self.extra * self.pieces == self.blocks
        assert nz * rows == nx * cols and self.near * rows == cols


def lane_block(v, k):
    return v[:, k * LANES : (k + 1) * LANES]


def rows_of(geo, v):
    lane = lax.broadcasted_iota(jnp.int32, (v.shape[0], LANES), 1)
    rows = [jnp.where(lane < geo.cols, lane_block(v, r), 0.0) for r in range(geo.blocks)]
    for e in range(geo.extra):
        row = jnp.zeros((v.shape[0], LANES), F32)
        for q in range(geo.pieces):
            low = geo.spare * q
            piece = pltpu.roll(lane_block(v, e * geo.pieces + q), (low - geo.cols) % LANES, 1)
            row = jnp.where((lane >= low) & (lane < low + geo.spare), piece, row)
        rows.append(row)
    return rows


def block_of(geo, get_row, k):
    row = get_row(k)
    lane = lax.broadcasted_iota(jnp.int32, row.shape, 1)
    extra, q = divmod(k, geo.pieces)
    piece = pltpu.roll(get_row(geo.blocks + extra), geo.cols - geo.spare * q, 1)
    return jnp.where(lane < geo.cols, row, piece)


def normed(values, gain):
    mean = jnp.mean(values, axis=0, keepdims=True)
    centred = values - mean
    spread = jnp.mean(centred * centred, axis=0, keepdims=True)
    return (centred * lax.rsqrt(spread + EPSILON) * gain).astype(BF16)


def kernel(
    geo,
    half,
    pair_hbm,
    flag_ref,
    proj_hbm,
    gate_hbm,
    out_hbm,
    out_ref,
    pair_ref,
    proj_ref,
    gate_ref,
    out_weight_ref,
    mask_ref,
    z_all,
    zn,
    tmp,
    gate,
    left_out,
    right_out,
    left_all,
    right_in,
    right_all,
    left_mat,
    right_mat,
    product,
    back_out,
    back_in,
    back_other,
    triangle,
    left_sem,
    right_sem,
    right_x_sem,
    back_sem,
    other_sem,
    z_sem,
    sent_sem,
    load_sem,
):
    nz, nx = geo.nz, geo.nx
    me_z = lax.axis_index("gx")
    me_x = lax.axis_index("gy")
    me_c = lax.axis_index("gz")
    other_c = 1 - me_c
    chunk = geo.pieces * LANES
    chunks = [slice(k, k + chunk) for k in range(0, geo.width, chunk)]

    barrier = pltpu.get_barrier_semaphore()

    def far_first(k):
        m = (k + 1) // 2
        return lax.rem(me_z + nz // 2 + m * (1 - 2 * (k % 2)), nz)

    def signal_z(k, _):
        pl.semaphore_signal(barrier, inc=1, device_id={"gx": far_first(k)}, device_id_type=MESH)
        return _

    lax.fori_loop(0, nz - 1, signal_z, 0)
    for k in range(1, nx):
        pl.semaphore_signal(
            barrier, inc=1, device_id={"gy": lax.rem(me_x + k, nx)}, device_id_type=MESH
        )
    pl.semaphore_signal(barrier, inc=1, device_id={"gz": other_c}, device_id_type=MESH)

    def copy_z(src, dst, send, recv, to):
        return pltpu.make_async_remote_copy(
            src_ref=src, dst_ref=dst, send_sem=send, recv_sem=recv, device_id={"gx": to}, device_id_type=MESH
        )

    def copy_x(src, dst, send, recv, to):
        return pltpu.make_async_remote_copy(
            src_ref=src, dst_ref=dst, send_sem=send, recv_sem=recv, device_id={"gy": to}, device_id_type=MESH
        )

    def copy_c(src, dst, send, recv):
        return pltpu.make_async_remote_copy(
            src_ref=src, dst_ref=dst, send_sem=send, recv_sem=recv, device_id={"gz": other_c}, device_id_type=MESH
        )

    def store_rows(mat, lead, base, value):
        for r, row in enumerate(rows_of(geo, value)):
            for h in range(2):
                mat[lead, h, pl.ds(base + r, 1), :] = row[h : h + 1, :]

    group = 4
    lag = 8

    loads = [
        pltpu.make_async_copy(src, dst, load_sem.at[i])
        for i, (src, dst) in enumerate(
            [
                (pair_hbm, pair_ref),
                (proj_hbm, proj_ref),
                (gate_hbm, gate_ref),
                (out_hbm, out_weight_ref),
            ]
        )
    ]
    for load in loads:
        load.start()
    for load in loads[:1]:
        load.wait()
    for c in range(2):
        own = slice(c * half, (c + 1) * half)
        for k in range(geo.blocks):
            e, q = divmod(k, geo.pieces)
            low = geo.spare * q
            z_all[0, c, :, k * LANES : (k + 1) * LANES] = jnp.concatenate(
                [pair_ref[k, own, :], pair_ref[geo.blocks + e, own, low : low + geo.spare]], axis=1
            )

    near_lane = lax.broadcasted_iota(jnp.int32, (1, LANES), 1)
    near_flags = jnp.zeros((1, LANES), F32)
    for t in range(geo.cols):
        flag = flag_ref[me_x * geo.cols + t].astype(F32)
        near_flags = jnp.where(near_lane == t, flag, near_flags)
    row_flag = [flag_ref[me_z * geo.rows + r].astype(F32) for r in range(geo.rows)]
    for k in range(geo.blocks):
        mask_ref[:, k * LANES : (k + 1) * LANES] = block_of(
            geo, lambda r: near_flags * row_flag[r], k
        )

    for load in loads[1:]:
        load.wait()

    def z_piece(i):
        part = z_all.at[1, me_c, :, chunks[i]]
        return copy_c(part, part, sent_sem.at[5, 0], z_sem.at[i])

    for u in range(2):
        left_u, right_u, back_u = left_out.at[u], right_out.at[u], back_out.at[u]

        for i in reversed(range(geo.extra)):
            if u == 1:
                z_piece(i).wait_recv()
            s = chunks[i]
            gain_in = pair_ref[geo.rows, :, u : u + 1]
            z = jnp.concatenate([z_all[u, 0, :, s], z_all[u, 1, :, s]], axis=0)
            zn[:, s] = normed(z, gain_in)

        def project(first, out):
            for s in chunks:
                opening, value = (
                    jnp.dot(proj_ref[u, first + i], zn[:, s], preferred_element_type=F32)
                    for i in range(2)
                )
                tmp[:, s] = jax.nn.sigmoid(opening) * value * mask_ref[:, s]
            for k in range(nz):
                out[k] = tmp[2 * k : 2 * k + 2, :].astype(BF16)

        def forward_left(src, s):
            for k in range(1, nx):
                copy_x(
                    src,
                    left_all.at[u, me_x, s],
                    sent_sem.at[2, u],
                    left_sem.at[u, me_x, s],
                    lax.rem(me_x + k, nx),
                ).start()

        def forward_right(src, s):
            target = s // geo.near

            @pl.when(target != me_x)
            def run():
                copy_x(
                    src,
                    right_all.at[me_x, s % geo.near],
                    sent_sem.at[3, 0],
                    right_x_sem.at[me_x, s % geo.near],
                    target,
                ).start()

        def send_left():
            def send(k, _):
                to = far_first(k)
                copy_z(
                    left_u.at[to],
                    left_all.at[u, me_x, me_z],
                    sent_sem.at[0, u],
                    left_sem.at[u, me_x, me_z],
                    to,
                ).start()
                return _

            lax.fori_loop(0, nz - 1, send, 0)
            forward_left(left_u.at[me_z], me_z)
            left_all[u, me_x, me_z] = left_u[me_z]

        def send_right():
            def send(k, _):
                to = far_first(k)
                copy_z(
                    right_u.at[to],
                    right_in.at[u, me_z],
                    sent_sem.at[1, u],
                    right_sem.at[u, me_z],
                    to,
                ).start()
                return _

            lax.fori_loop(0, nz - 1, send, 0)
            right_in[u, me_z] = right_u[me_z]

        def open_gate():
            for s in chunks:
                gate[:, s] = jax.nn.sigmoid(
                    jnp.dot(gate_ref[u], zn[:, s], preferred_element_type=F32)
                )

        def left_base(k, s):
            return (k if u == 0 else s) * geo.rows

        def take_left(k):
            s = far_first(k)
            slot = left_all.at[u, me_x, s]

            @pl.when(k < nz - 1)
            def run():
                copy_z(slot, slot, sent_sem.at[0, u], left_sem.at[u, me_x, s], s).wait_recv()
                forward_left(slot, s)

            store_rows(left_mat, me_x, left_base(k, s), left_all[u, me_x, s].astype(F32))

        def take_left_x(k):
            s = far_first(k)
            for d in range(1, nx):
                x = lax.rem(me_x + d, nx)
                slot = left_all.at[u, x, s]
                copy_x(slot, slot, sent_sem.at[2, u], left_sem.at[u, x, s], x).wait_recv()
                store_rows(left_mat, x, left_base(k, s), left_all[u, x, s].astype(F32))

        def wait_right(k, s):
            slot = right_in.at[u, s]

            @pl.when(k < nz - 1)
            def run():
                copy_z(slot, slot, sent_sem.at[1, u], right_sem.at[u, s], s).wait_recv()

        def block_row(base, r):
            return jnp.concatenate([product[h, pl.ds(base + r, 1), :] for h in range(2)], axis=0)

        def send_back(k):
            to = far_first(k)
            base = left_base(k, to)
            for b in range(geo.blocks):
                value = block_of(geo, functools.partial(block_row, base), b)
                back_u[to, :, b * LANES : (b + 1) * LANES] = value.astype(BF16)

            @pl.when(k < nz - 1)
            def run():
                copy_z(
                    back_u.at[to], back_in.at[u, me_z], sent_sem.at[4, u], back_sem.at[u, me_z], to
                ).start()

        if u == 0:
            project(2, right_u)
            pl.semaphore_wait(barrier, nz - 1 + nx - 1 + 1)
            send_right()
            forward_right(right_u.at[me_z], me_z)
            project(0, left_u)
            send_left()
            open_gate()

            def take_right(k, _):
                s = far_first(k)
                wait_right(k, s)

                @pl.when(k < nz - 1)
                def run():
                    forward_right(right_in.at[0, s], s)

                @pl.when(s // geo.near == me_x)
                def run_own():
                    store_rows(
                        right_mat, me_x, (s % geo.near) * geo.rows, right_in[0, s].astype(F32)
                    )

                return _

            lax.fori_loop(0, nz, take_right, 0)

            def take_group(g):
                def take(i, _):
                    take_left(g * group + i)
                    return _

                lax.fori_loop(0, group, take, 0)

            take_group(0)

            for d in range(1, nx):
                x = lax.rem(me_x + d, nx)

                def take_right_x(k, _):
                    slot = right_all.at[x, k]
                    copy_x(slot, slot, sent_sem.at[3, 0], right_x_sem.at[x, k], x).wait_recv()
                    store_rows(right_mat, x, k * geo.rows, right_all[x, k].astype(F32))
                    return _

                lax.fori_loop(0, geo.near, take_right_x, 0)
            take_group(1)

            tall = group * geo.rows

            def work(g, _):
                @pl.when(g < nz // group - 2)
                def run():
                    take_group(g + 2)

                def take_x(i, _):
                    take_left_x(g * group + i)
                    return _

                lax.fori_loop(0, group, take_x, 0)
                rows = pl.ds(pl.multiple_of(g * tall, tall), tall)
                for h in range(2):
                    total = jnp.zeros((tall, geo.cols), F32)
                    for x in range(nx):
                        total += lax.dot_general(
                            left_mat[x, h, rows, :].astype(BF16),
                            right_mat[x, h, : geo.cols, :].astype(BF16),
                            (((1,), (1,)), ((), ())),
                            preferred_element_type=F32,
                        )
                    product[h, rows, : geo.cols] = total

                def send(i, _):
                    send_back(g * group + i)
                    return _

                lax.fori_loop(0, group, send, 0)
                return _

            lax.fori_loop(0, nz // group, work, 0)
        else:
            project(0, left_u)
            send_left()
            project(2, right_u)
            send_right()
            open_gate()

            def take_lefts(k, _):
                take_left(k)

                @pl.when(k >= lag)
                def run():
                    take_left_x(k - lag)

                return _

            lax.fori_loop(0, nz, take_lefts, 0)

            def take_right(k, _):
                s = far_first(k)
                wait_right(k, s)
                store_rows(right_mat, 0, s * geo.rows, right_in[1, s].astype(F32))

                @pl.when(k < lag)
                def run():
                    take_left_x(nz - lag + k)

                return _

            lax.fori_loop(0, nz, take_right, 0)

            for h in range(2):
                right = right_mat[0, h].astype(BF16)
                for x in range(nx):
                    part = lax.dot_general(
                        left_mat[x, h].astype(BF16),
                        right,
                        (((0,), (0,)), ((), ())),
                        preferred_element_type=F32,
                    )
                    product[h, geo.cols * x : geo.cols * (x + 1), :] = part[: geo.cols, :]

            def send(k, _):
                send_back(k)
                return _

            lax.fori_loop(0, nz, send, 0)

        def take_back(k, _):
            s = far_first(k)
            slot = back_in.at[u, s]
            copy_z(slot, slot, sent_sem.at[4, u], back_sem.at[u, s], s).wait_recv()
            copy_c(slot, back_other.at[u, s], sent_sem.at[6, u], other_sem.at[u]).start()
            triangle[me_c, s] = back_in[u, s].astype(F32)
            return _

        copy_c(
            back_u.at[me_z], back_other.at[u, me_z], sent_sem.at[6, u], other_sem.at[u]
        ).start()
        triangle[me_c, me_z] = back_u[me_z].astype(F32)
        lax.fori_loop(0, nz - 1, take_back, 0)

        all_other = back_other.at[u]
        copy_c(all_other, all_other, sent_sem.at[6, u], other_sem.at[u]).wait_recv()

        def take_other(k, _):
            triangle[other_c, k] = back_other[u, k].astype(F32)
            return _

        lax.fori_loop(0, nz, take_other, 0)

        gain_out = pair_ref[geo.rows, :, 2 + u : 3 + u]
        for i in reversed(range(geo.extra)):
            s = chunks[i]
            values = jnp.concatenate(
                [triangle[c, k, :, s] for c in range(2) for k in range(nz)], axis=0
            )
            tn = normed(values, gain_out)
            change = jnp.dot(out_weight_ref[u], tn, preferred_element_type=F32)
            value = z_all[u, me_c, :, s] + gate[:, s] * change
            if u == 0:
                z_all[1, me_c, :, s] = value
                z_piece(i).start()
            else:
                lane = lax.broadcasted_iota(jnp.int32, (half, LANES), 1)
                row = jnp.zeros((half, LANES), F32)
                for q in range(geo.pieces):
                    block = lane_block(value, q)
                    out_ref[i * geo.pieces + q] = block[:, : geo.cols]
                    low = geo.spare * q
                    moved = pltpu.roll(block, (low - geo.cols) % LANES, 1)
                    row = jnp.where((lane >= low) & (lane < low + geo.spare), moved, row)
                out_ref[geo.blocks + i] = row[:, : geo.cols]

    any_sem = z_sem.at[0]
    for u in range(2):
        many = left_out.at[u, pl.ds(0, nz - 1)]
        copy_z(many, many, sent_sem.at[0, u], any_sem, me_z).wait_send()
        copy_z(many, many, sent_sem.at[1, u], any_sem, me_z).wait_send()
        copy_z(many, many, sent_sem.at[4, u], any_sem, me_z).wait_send()
        for k in range(1, nx):
            all_slots = left_out.at[u]
            copy_x(all_slots, all_slots, sent_sem.at[2, u], any_sem, me_x).wait_send()
        every = left_out.at[u]
        copy_c(every, every, sent_sem.at[6, u], any_sem).wait_send()
    away = left_out.at[0, pl.ds(0, nz - geo.near)]
    copy_x(away, away, sent_sem.at[3, 0], any_sem, me_x).wait_send()
    part = z_all.at[1, me_c]
    copy_c(part, part, sent_sem.at[5, 0], any_sem).wait_send()


def per_device(
    geo, pair, residue_mask, norm_in_gain, proj_weight, gate_weight, norm_out_gain, out_weight
):
    half = pair.shape[0]
    full = 2 * half
    nz, nx = geo.nz, geo.nx
    vmem = pltpu.VMEM
    message = (2, geo.width)
    dma = pltpu.SemaphoreType.DMA
    hbm = pl.BlockSpec(memory_space=pl.ANY)
    pair = jnp.swapaxes(pair, 0, 1)
    gains = jnp.concatenate([norm_in_gain, norm_out_gain], axis=0).T
    gains = jnp.pad(gains, ((0, 0), (0, geo.cols - gains.shape[1])))
    pair = jnp.concatenate([pair, gains[None]], axis=0)
    pair = lax.all_gather(pair, "gz", axis=1, tiled=True)
    proj_weight = jnp.swapaxes(proj_weight, 2, 3)
    gate_weight = jnp.swapaxes(gate_weight, 1, 2)
    out_weight = jnp.swapaxes(out_weight, 1, 2)
    result = pl.pallas_call(
        functools.partial(kernel, geo, half),
        out_shape=jax.ShapeDtypeStruct((geo.rows, half, geo.cols), F32),
        in_specs=[
            hbm,
            pl.BlockSpec(memory_space=pltpu.SMEM),
            hbm,
            hbm,
            hbm,
        ],
        out_specs=pl.BlockSpec(memory_space=vmem),
        scratch_shapes=[
            vmem(pair.shape, F32),
            vmem(proj_weight.shape, BF16),
            vmem(gate_weight.shape, BF16),
            vmem(out_weight.shape, BF16),
            vmem((1, geo.width), F32),
            vmem((2, 2, half, geo.width), F32),
            vmem((full, geo.width), BF16),
            vmem((half, geo.width), F32),
            vmem((half, geo.width), F32),
            vmem((2, nz, *message), BF16),
            vmem((2, nz, *message), BF16),
            vmem((2, nx, nz, *message), BF16),
            vmem((2, nz, *message), BF16),
            vmem((nx, geo.near, *message), BF16),
            vmem((nx, 2, geo.res, LANES), F32),
            vmem((nx, 2, geo.res, LANES), F32),
            vmem((2, geo.res, LANES), F32),
            vmem((2, nz, *message), BF16),
            vmem((2, nz, *message), BF16),
            vmem((2, nz, *message), BF16),
            vmem((2, nz, *message), F32),
            dma((2, nx, nz)),
            dma((2, nz)),
            dma((nx, geo.near)),
            dma((2, nz)),
            dma((2,)),
            dma((geo.extra,)),
            dma((7, 2)),
            dma((4,)),
        ],
        compiler_params=pltpu.CompilerParams(
            collective_id=0, has_side_effects=True, vmem_limit_bytes=60 * 1024 * 1024
        ),
        name="triangle_updates",
    )(
        pair,
        residue_mask,
        proj_weight,
        gate_weight,
        out_weight,
    )
    return jnp.swapaxes(result, 0, 1)


def solution(mesh):
    def body(pair, *rest):
        geo = Geometry(pair.shape[1], pair.shape[2], mesh.shape["gx"], mesh.shape["gy"])
        return per_device(geo, pair, *rest)

    return jax.shard_map(
        body,
        mesh=mesh,
        in_specs=(
            P(("groups", "gz"), "gx", "gy"),
            P("groups"),
            P(None, "gz"),
            P(None, None, None, "gz"),
            P(None, None, "gz"),
            P(None, "gz"),
            P(None, None, "gz"),
        ),
        out_specs=P(("groups", "gz"), "gx", "gy"),
        check_vma=False,
    )
```
